256 devices in a mesh: gx: 8 (over x, z_lo), gy: 8 (over z_hi, core), gz: 4 (over y).
Axes of the slice: x: 4, y: 4, z: 8 (z_hi: 4, z_lo: 2; z = z_hi * 2 + z_lo), core: 2. Of those that a mesh axis runs over, the one named last changes fastest.
Arguments:
- partials: float32 [32, 128, 128, 512], P('gx', None, 'gy', 'gz'), may hold values from -40 to 40
- code_bits: int32 [32, 128], replicated, may hold values from 0 to 1
- group_map: int32 [32], replicated, may hold values from 0 to 31, each once
- velocity: float32 [128, 128, 512], P('gx', 'gy', 'gz'), may hold values from 1.5 to 4.5
Outputs:
- gradient: float32 [128, 128, 512], P('gx', 'gy', 'gz')
- new_model: float32 [128, 128, 512], P('gx', 'gy', 'gz')
The draws below stay inside these ranges and needn't reach their ends.
Inputs may be any that keep to these rules, and one draw needn't show every extreme that they name: `group_map`: every group of 0 to 31 stands in exactly one slot.
All inputs are finite; a program needn't handle non-finite values.
Results may differ from the reference program's by a relative error of at most 0.0001.
Values sent between devices are 32-bit elements; how exact they have to be, the bound alone decides.
No kernel may reach another device: no remote copies, remote signals or barrier semaphores. Data moves between devices by JAX's collectives and lax.ppermute only.
A program may use at most 64 MiB of HBM per device.

```python
import jax
import jax.numpy as jnp
from jax import lax

G = 32
ITERS = 3
NX = 128
NY = 128
NZ = 512


def draw_partials(key, part):
    first_key = jax.random.fold_in(jax.random.fold_in(key, 17), 0)
    rough = jnp.clip(jax.random.normal(first_key, (G, NX, NY, NZ), jnp.float32), -6.0, 6.0)
    return rough


def set_ends(result, rng, smallest, top_value):
    longest = result.shape.index(max(result.shape))
    spots = []
    for shift in (0, 1):
        where = [jax.random.randint(jax.random.fold_in(rng, axis), (), 0, length) for axis, length in enumerate(result.shape)]
        where[longest] = (where[longest] + shift) % result.shape[longest]
        spots.append(tuple(where))
    return result.at[spots[0]].set(smallest).at[spots[1]].set(top_value)


def block_scale(key, dims, pieces, low, top_value):
    def one(axis_at, parts):
        draws = jax.random.uniform(jax.random.fold_in(jax.random.fold_in(key, 6), axis_at), (parts,), jnp.float32, low / len(pieces), top_value / len(pieces))
        return jnp.repeat(jnp.exp(draws), dims[axis_at] // parts).reshape((-1,) + (1,) * (len(dims) - axis_at - 1))

    loudness = one(*pieces[0])
    for cut in pieces[1:]:
        loudness = loudness * one(*cut)
    return loudness


def setup_inputs(seed: int = 0) -> dict:
    arg_keys = jax.random.split(jax.random.key(seed), 5)
    return {
        "partials": draw_partials(jax.random.fold_in(arg_keys[4], 71), 0),
        "code_bits": set_ends(jax.random.randint(arg_keys[1], (G, NX), 0, 2), jax.random.fold_in(arg_keys[1], 1), 0, 1).astype(jnp.int32),
        "group_map": jax.random.permutation(arg_keys[2], G).astype(jnp.int32),
        "velocity": jnp.clip(1.5 + 3.0 * jax.random.uniform(arg_keys[3], (NX, NY, NZ), jnp.float32) ** block_scale(arg_keys[3], (NX, NY, NZ), ((0, 8), (1, 8), (2, 4)), -0.2, 0.2), 1.5, 4.5),
    }


step_length = 0.5
tv_weight = 0.2
dual_step = 0.28
primal_step = 0.28

def forward_diff(field):
    zeros_x = jnp.zeros((1,) + field.shape[1:], jnp.float32)
    zeros_y = jnp.zeros((field.shape[0], 1, field.shape[2]), jnp.float32)
    zeros_z = jnp.zeros(field.shape[:2] + (1,), jnp.float32)
    diff_x = jnp.concatenate([field[1:] - field[:-1], zeros_x], 0)
    diff_y = jnp.concatenate([field[:, 1:] - field[:, :-1], zeros_y], 1)
    diff_z = jnp.concatenate([field[:, :, 1:] - field[:, :, :-1], zeros_z], 2)
    return jnp.stack([diff_x, diff_y, diff_z])

def divergence(dual_field):
    left_x = jnp.pad(dual_field[0][:-1], ((1, 0), (0, 0), (0, 0)))
    left_y = jnp.pad(dual_field[1][:, :-1], ((0, 0), (1, 0), (0, 0)))
    left_z = jnp.pad(dual_field[2][:, :, :-1], ((0, 0), (0, 0), (1, 0)))
    return dual_field[0] - left_x + (dual_field[1] - left_y) + (dual_field[2] - left_z)

def reference(partials, code_bits, group_map, velocity):
    sign_table = 2.0 * code_bits[group_map].astype(jnp.float32) - 1.0

    def accumulate(index, acc):
        return acc + sign_table[index][:, None, None] * partials[index]
    gradient = lax.fori_loop(0, partials.shape[0], accumulate, jnp.zeros(velocity.shape, jnp.float32))
    mean_square = jnp.sum(gradient * gradient) / gradient.size
    step_scale = step_length / jnp.sqrt(mean_square + 1.0)
    target = velocity - step_scale * gradient
    current = target
    extra = target
    dual_field = jnp.zeros((3,) + target.shape, jnp.float32)
    for iteration in range(ITERS):
        dual_field = dual_field + dual_step * forward_diff(extra)
        magnitude = jnp.sqrt(lax.optimization_barrier(jnp.sum(dual_field * dual_field, axis=0)))
        dual_field = dual_field / jnp.maximum(1.0, magnitude / tv_weight)[None]
        updated = (current + primal_step * divergence(dual_field) + primal_step * target) / (1.0 + primal_step)
        extra = 2.0 * updated - current
        current = updated
    return (gradient, current)
```

```python
import jax
import jax.numpy as jnp
from jax import lax
from jax.experimental import pallas as pl
from jax.experimental.pallas import tpu as pltpu
from jax.sharding import Mesh
from jax.sharding import PartitionSpec as P

ITERS = 3
HALO = ITERS
GX = ("gx_0", "gx_1")
GY = ("gy_0", "gy_1")
XY = GX + GY
ALL = XY + ("gz",)

step_length = 0.5
tv_weight = 0.2
dual_step = 0.28
primal_step = 0.28

VMEM = pl.BlockSpec(memory_space=pltpu.VMEM)
SMEM = pl.BlockSpec(memory_space=pltpu.SMEM)
HBM = pl.BlockSpec(memory_space=pltpu.HBM)
PARAMS = pltpu.CompilerParams(vmem_limit_bytes=16 * 1024 * 1024)
F32 = jnp.float32


def shift(block, axis, distance):
    size = lax.axis_size(axis)
    return lax.ppermute(block, axis, [(i, (i + distance) % size) for i in range(size)])


def struct(*shape):
    return jax.ShapeDtypeStruct(shape, F32)


def presum(partials, code_bits, group_map, base, chunks):
    slots, nx, by, bz = partials.shape
    rows = nx // chunks

    def kernel(base_ref, map_ref, bits_ref, part_ref, out_ref, buf, sems):
        def copy(c):
            part = pl.ds(c * rows, rows)
            return pltpu.make_async_copy(part_ref.at[:, part], buf.at[:, part], sems.at[c])

        for c in range(chunks):
            copy(c).start()
        groups = [map_ref[base_ref[0] + s] for s in range(slots)]
        for c in range(chunks):
            copy(c).wait()

            def row(i, carry):
                x = c * rows + i
                total = None
                for s in range(slots):
                    sign = (2 * bits_ref[groups[s], x] - 1).astype(F32)
                    term = sign * buf[s, x]
                    total = term if total is None else total + term
                out_ref[x] = total
                return carry

            lax.fori_loop(0, rows, row, 0, unroll=4)

    return pl.pallas_call(
        kernel,
        name="presum",
        compiler_params=PARAMS,
        out_shape=struct(nx, by, bz),
        in_specs=[SMEM, SMEM, SMEM, HBM],
        out_specs=VMEM,
        scratch_shapes=[pltpu.VMEM(partials.shape, F32), pltpu.SemaphoreType.DMA((chunks,))],
    )(base, group_map, code_bits, pltpu.with_memory_space_constraint(partials, pltpu.HBM))


def reduce_pack(parts, velocity, members):
    bx, by, bz = velocity.shape

    def kernel(part_ref, v_ref, g_ref, first_ref, last_ref, square_ref):
        squares = jnp.zeros((by, bz), F32)
        for i in range(bx):
            total = part_ref[i]
            for m in range(1, members):
                total = total + part_ref[m * bx + i]
            g_ref[i] = total
            squares = squares + total * total
            if i < HALO:
                first_ref[i] = total
                first_ref[HALO + i] = v_ref[i]
            if i >= bx - HALO:
                last_ref[i - bx + HALO] = total
                last_ref[i - bx + 2 * HALO] = v_ref[i]
        square_ref[...] = jnp.broadcast_to(jnp.sum(squares, axis=0, keepdims=True), (8, bz))

    edge = struct(2 * HALO, by, bz)
    return pl.pallas_call(
        kernel,
        name="reduce_pack",
        compiler_params=PARAMS,
        out_shape=(struct(bx, by, bz), edge, edge, struct(8, bz)),
        in_specs=[VMEM, VMEM],
        out_specs=(VMEM,) * 4,
    )(parts, velocity)


def plane_of(main_ref, before_ref, after_ref, field, p, bx):
    if p < HALO:
        return before_ref[field * HALO + p]
    if p < HALO + bx:
        return main_ref[p - HALO]
    return after_ref[field * HALO + p - HALO - bx]


def sublane(shape):
    return lax.broadcasted_iota(jnp.int32, shape, len(shape) - 2)


def lane(shape):
    return lax.broadcasted_iota(jnp.int32, shape, len(shape) - 1)


def pack_y(gradient, velocity, before_x, after_x):
    bx, by, bz = velocity.shape
    pairs = (bx + 2 * HALO) // 2

    def kernel(g_ref, v_ref, before_ref, after_ref, first_ref, last_ref):
        low = sublane((8, bz)) < 4
        for field, main in enumerate((g_ref, v_ref)):
            for q in range(pairs):
                even = plane_of(main, before_ref, after_ref, field, 2 * q, bx)
                odd = plane_of(main, before_ref, after_ref, field, 2 * q + 1, bx)
                first_ref[field * pairs + q] = jnp.where(low, even[:8], pltpu.roll(odd[:8], 4, 0))
                last_ref[field * pairs + q] = jnp.where(
                    low, pltpu.roll(even[by - 8 :], 4, 0), odd[by - 8 :]
                )

    edge = struct(2 * pairs, 8, bz)
    return pl.pallas_call(
        kernel,
        name="pack_y",
        compiler_params=PARAMS,
        out_shape=(edge, edge),
        in_specs=[VMEM] * 4,
        out_specs=(VMEM,) * 2,
    )(gradient, velocity, before_x, after_x)


def rows_of(before_ref, after_ref, field, p, pairs):
    after = after_ref[field * pairs + p // 2]
    before = before_ref[field * pairs + p // 2]
    low = sublane(after.shape) < 4
    if p % 2 == 0:
        return jnp.where(low, after, pltpu.roll(before, 4, 0))
    return jnp.where(low, pltpu.roll(after, 4, 0), before)


def pack_z(gradient, velocity, before_x, after_x, before_y, after_y, squares):
    bx, by, bz = velocity.shape
    planes = bx + 2 * HALO
    pairs = planes // 2
    groups = bz // 4
    tall = by + 8

    def kernel(g_ref, v_ref, bx_ref, ax_ref, by_ref, ay_ref, sq_ref, first_ref, last_ref, sum_ref):
        group = lane((tall, bz)) // 4
        for field, main in enumerate((g_ref, v_ref)):
            first = jnp.zeros((tall, bz), F32)
            last = jnp.zeros((tall, bz), F32)
            for p in range(planes):
                own = plane_of(main, bx_ref, ax_ref, field, p, bx)
                extra = rows_of(by_ref, ay_ref, field, p, pairs)
                plane = jnp.concatenate([own, extra], 0)
                turned = pltpu.roll(plane, 4 * p, 1) if p else plane
                first = jnp.where(group == p, turned, first)
                last = jnp.where(group == (p - 1) % groups, turned, last)
            first_ref[pl.ds(field * tall, tall)] = first
            last_ref[pl.ds(field * tall, tall)] = last
        total = jnp.broadcast_to(jnp.sum(sq_ref[...], axis=0), (8, bz))
        first_ref[pl.ds(2 * tall, 8)] = total
        last_ref[pl.ds(2 * tall, 8)] = total
        sum_ref[...] = total

    edge = struct(2 * tall + 8, bz)
    return pl.pallas_call(
        kernel,
        name="pack_z",
        compiler_params=PARAMS,
        out_shape=(edge, edge, struct(8, bz)),
        in_specs=[VMEM] * 7,
        out_specs=(VMEM,) * 3,
    )(gradient, velocity, before_x, after_x, before_y, after_y, squares)


def proximal(device, gradient, velocity, halos, sums, sizes):
    bx, by, bz = velocity.shape
    planes = bx + 2 * HALO
    pairs = planes // 2
    tall = by + 8
    wide = 2 * bz
    size_x, size_y, size_z = sizes
    cells = size_x * bx * size_y * by * size_z * bz

    def kernel(
        dev_ref,
        g_ref,
        v_ref,
        bx_ref,
        ax_ref,
        by_ref,
        ay_ref,
        bz_ref,
        az_ref,
        own_ref,
        far_ref,
        gradient_ref,
        model_ref,
        target,
        current,
        extra,
        dual_x,
        dual_y,
        dual_z,
        model,
        sems,
    ):
        gradient_copy = pltpu.make_async_copy(g_ref, gradient_ref, sems.at[0])
        gradient_copy.start()
        dev = dev_ref[0]
        pos_z = dev % size_z
        pos_y = (dev // size_z) % size_y
        pos_x = dev // (size_z * size_y)

        total = own_ref[0:1] + far_ref[0:1]
        total = total + bz_ref[2 * tall : 2 * tall + 1] + az_ref[2 * tall : 2 * tall + 1]
        total = jnp.sum(total, axis=1, keepdims=True)
        scale = step_length * lax.rsqrt(total / cells + 1.0)
        scale = jnp.broadcast_to(scale, (1, bz))

        side_lane = lane((tall, bz)) < bz // 2
        before_z = bz_ref[pl.ds(tall, tall)] - scale * bz_ref[pl.ds(0, tall)]
        after_z = az_ref[pl.ds(tall, tall)] - scale * az_ref[pl.ds(0, tall)]
        for p in range(planes):
            own = plane_of(v_ref, bx_ref, ax_ref, 1, p, bx) - scale * plane_of(
                g_ref, bx_ref, ax_ref, 0, p, bx
            )
            rows = rows_of(by_ref, ay_ref, 1, p, pairs) - scale * rows_of(
                by_ref, ay_ref, 0, p, pairs
            )
            back = (bz - 4 * p) % bz
            after = pltpu.roll(after_z, back, 1) if back else after_z
            before = pltpu.roll(before_z, back, 1) if back else before_z
            target[p, pl.ds(0, by), pl.ds(0, bz)] = own
            target[p, pl.ds(by, 8), pl.ds(0, bz)] = rows
            target[p, :, pl.ds(bz, bz)] = jnp.where(side_lane, after, before)

        def factor(index, limit):
            return jnp.where((index >= 0) & (index < limit - 1), dual_step, 0.0).astype(F32)

        row = sublane((tall, 1))
        row = jnp.where(row < by + 4, row, row - tall) + pos_y * by
        factor_y = factor(row, size_y * by)
        col = lane((1, wide))
        col = jnp.where(col < bz + bz // 2, col, col - wide) + pos_z * bz
        factor_z = factor(col, size_z * bz)
        shrink = 1.0 / (1.0 + primal_step)
        gain = primal_step / (1.0 + primal_step)

        for iteration in range(ITERS):
            first = iteration == 0
            final = iteration == ITERS - 1
            here_ref = target if first else extra
            ahead = here_ref[iteration]
            before_x = None
            for p in range(iteration, planes - 1 - iteration):
                here = ahead
                ahead = here_ref[p + 1]
                index = pos_x * bx + (p - HALO)
                factor_x = factor(index, size_x * bx)
                dx = factor_x * (ahead - here)
                dy = factor_y * (pltpu.roll(here, tall - 1, 0) - here)
                dz = factor_z * (pltpu.roll(here, wide - 1, 1) - here)
                if not first:
                    dx = dual_x[p] + dx
                    dy = dual_y[p] + dy
                    dz = dual_z[p] + dz
                norm = dx * dx + dy * dy + dz * dz
                ratio = jnp.minimum(1.0, tv_weight * lax.rsqrt(norm))
                dx = dx * ratio
                dy = dy * ratio
                dz = dz * ratio
                if not final:
                    dual_x[p] = dx
                    dual_y[p] = dy
                    dual_z[p] = dz
                if p > iteration:
                    if final:
                        spread = dx[:by, :bz] - before_x
                        spread += dy[:by, :bz] - pltpu.roll(dy[:, :bz], 1, 0)[:by]
                        spread += dz[:by, :bz] - pltpu.roll(dz[:by], 1, 1)[:, :bz]
                        goal = target[p, pl.ds(0, by), pl.ds(0, bz)]
                        old = current[p, pl.ds(0, by), pl.ds(0, bz)]
                        model[p - HALO] = shrink * old + gain * (spread + goal)
                    else:
                        spread = dx - before_x
                        spread += dy - pltpu.roll(dy, 1, 0)
                        spread += dz - pltpu.roll(dz, 1, 1)
                        if first:
                            new = here + gain * spread
                            old = here
                        else:
                            old = current[p]
                            new = shrink * old + gain * (spread + target[p])
                        current[p] = new
                        extra[p] = 2.0 * new - old
                before_x = dx[:by, :bz] if final else dx
        model_copy = pltpu.make_async_copy(model, model_ref, sems.at[1])
        model_copy.start()
        gradient_copy.wait()
        model_copy.wait()

    field = pltpu.VMEM((planes, tall, wide), F32)
    return pl.pallas_call(
        kernel,
        name="proximal",
        compiler_params=PARAMS,
        out_shape=(struct(bx, by, bz),) * 2,
        in_specs=[SMEM] + [VMEM] * 10,
        out_specs=(HBM,) * 2,
        scratch_shapes=[field] * 6 + [pltpu.VMEM((bx, by, bz), F32), pltpu.SemaphoreType.DMA((2,))],
    )(device, gradient, velocity, *halos, *sums)


def shards(partials, code_bits, group_map, velocity):
    bx, by, bz = velocity.shape
    size_x, size_y, size_z = (lax.axis_size(axis) for axis in (GX, GY, "gz"))
    base = (lax.axis_index(GX) * partials.shape[0]).astype(jnp.int32).reshape(1)
    device = lax.axis_index(ALL).astype(jnp.int32).reshape(1)

    local = presum(partials, code_bits, group_map, base, 8)
    parts = lax.all_to_all(local, GX, split_axis=0, concat_axis=0, tiled=True)
    gradient, first_x, last_x, squares = reduce_pack(parts, velocity, size_x)

    after_x = shift(first_x, GX, -1)
    before_x = shift(last_x, GX, 1)
    table = jnp.broadcast_to(squares[:1][None], (size_x * size_y, 1, bz))
    table = lax.all_to_all(table, XY, split_axis=0, concat_axis=0, tiled=True)

    first_y, last_y = pack_y(gradient, velocity, before_x, after_x)
    after_y = shift(first_y, GY, -1)
    before_y = shift(last_y, GY, 1)

    first_z, last_z, own = pack_z(
        gradient, velocity, before_x, after_x, before_y, after_y, table
    )
    after_z = shift(first_z, "gz", -1)
    before_z = shift(last_z, "gz", 1)
    far = shift(own, "gz", 2)

    return proximal(
        device,
        gradient,
        velocity,
        (before_x, after_x, before_y, after_y, before_z, after_z),
        (own, far),
        (size_x, size_y, size_z),
    )


def solution(mesh):
    torus = Mesh(
        mesh.devices.reshape(4, 2, 4, 2, mesh.shape["gz"]), ("gx_0", "gx_1", "gy_0", "gy_1", "gz")
    )
    placed = (P(GX, None, GY, "gz"), P(), P(), P(GX, GY, "gz"))
    return jax.shard_map(
        shards,
        mesh=torus,
        in_specs=placed,
        out_specs=(P(GX, GY, "gz"), P(GX, GY, "gz")),
        check_vma=False,
    )
```

```python
import jax
import jax.numpy as jnp
from jax import lax
from jax.experimental import pallas as pl
from jax.experimental.pallas import tpu as pltpu
from jax.sharding import Mesh
from jax.sharding import PartitionSpec as P

ITERS = 3
HALO = ITERS
GX = ("gx_0", "gx_1")
GY = ("gy_0", "gy_1")
XY = GX + GY
ALL = XY + ("gz",)

step_length = 0.5
tv_weight = 0.2
dual_step = 0.28
primal_step = 0.28

VMEM = pl.BlockSpec(memory_space=pltpu.VMEM)
SMEM = pl.BlockSpec(memory_space=pltpu.SMEM)
HBM = pl.BlockSpec(memory_space=pltpu.HBM)
PARAMS = pltpu.CompilerParams(vmem_limit_bytes=16 * 1024 * 1024)
F32 = jnp.float32


def shift(block, axis, distance):
    size = lax.axis_size(axis)
    return lax.ppermute(block, axis, [(i, (i + distance) % size) for i in range(size)])


def struct(*shape):
    return jax.ShapeDtypeStruct(shape, F32)


def in_hbm(array):
    return pltpu.with_memory_space_constraint(array, pltpu.HBM)


def presum(partials, code_bits, group_map, base, chunks):
    slots, nx, by, bz = partials.shape
    rows = nx // chunks

    def kernel(base_ref, map_hbm, bits_hbm, part_ref, out_ref, buf, map_ref, bits_ref, sems):
        map_copy = pltpu.make_async_copy(map_hbm, map_ref, sems.at[chunks])
        bits_copy = pltpu.make_async_copy(bits_hbm, bits_ref, sems.at[chunks + 1])
        map_copy.start()
        bits_copy.start()

        def copy(c):
            part = pl.ds(c * rows, rows)
            return pltpu.make_async_copy(part_ref.at[:, part], buf.at[:, part], sems.at[c])

        for c in range(chunks):
            copy(c).start()
        map_copy.wait()
        bits_copy.wait()
        groups = [map_ref[base_ref[0] + s] for s in range(slots)]
        for c in range(chunks):
            copy(c).wait()

            def row(i, carry):
                x = c * rows + i
                total = None
                for s in range(slots):
                    sign = (2 * bits_ref[groups[s], x] - 1).astype(F32)
                    term = sign * buf[s, x]
                    total = term if total is None else total + term
                out_ref[x] = total
                return carry

            lax.fori_loop(0, rows, row, 0, unroll=4)

    return pl.pallas_call(
        kernel,
        name="presum",
        compiler_params=PARAMS,
        out_shape=struct(nx, by, bz),
        in_specs=[SMEM, HBM, HBM, HBM],
        out_specs=VMEM,
        scratch_shapes=[
            pltpu.VMEM(partials.shape, F32),
            pltpu.SMEM(group_map.shape, jnp.int32),
            pltpu.SMEM(code_bits.shape, jnp.int32),
            pltpu.SemaphoreType.DMA((chunks + 2,)),
        ],
    )(base, in_hbm(group_map), in_hbm(code_bits), in_hbm(partials))


def reduce_pack(parts, velocity, members):
    bx, by, bz = velocity.shape

    def kernel(part_ref, v_ref, g_ref, first_ref, last_ref, square_ref):
        squares = jnp.zeros((by, bz), F32)
        for i in range(bx):
            total = part_ref[i]
            for m in range(1, members):
                total = total + part_ref[m * bx + i]
            g_ref[i] = total
            squares = squares + total * total
            if i < HALO:
                first_ref[i] = total
                first_ref[HALO + i] = v_ref[i]
            if i >= bx - HALO:
                last_ref[i - bx + HALO] = total
                last_ref[i - bx + 2 * HALO] = v_ref[i]
        square_ref[...] = jnp.broadcast_to(jnp.sum(squares, axis=0, keepdims=True), (8, bz))

    edge = struct(2 * HALO, by, bz)
    return pl.pallas_call(
        kernel,
        name="reduce_pack",
        compiler_params=PARAMS,
        out_shape=(struct(bx, by, bz), edge, edge, struct(8, bz)),
        in_specs=[VMEM, VMEM],
        out_specs=(VMEM,) * 4,
    )(parts, velocity)


def plane_of(main_ref, before_ref, after_ref, field, p, bx):
    if p < HALO:
        return before_ref[field * HALO + p]
    if p < HALO + bx:
        return main_ref[p - HALO]
    return after_ref[field * HALO + p - HALO - bx]


def sublane(shape):
    return lax.broadcasted_iota(jnp.int32, shape, len(shape) - 2)


def lane(shape):
    return lax.broadcasted_iota(jnp.int32, shape, len(shape) - 1)


def pack_y(gradient, velocity, before_x, after_x):
    bx, by, bz = velocity.shape
    pairs = (bx + 2 * HALO) // 2

    def kernel(g_ref, v_ref, before_ref, after_ref, first_ref, last_ref):
        low = sublane((8, bz)) < 4
        for field, main in enumerate((g_ref, v_ref)):
            for q in range(pairs):
                even = plane_of(main, before_ref, after_ref, field, 2 * q, bx)
                odd = plane_of(main, before_ref, after_ref, field, 2 * q + 1, bx)
                first_ref[field * pairs + q] = jnp.where(low, even[:8], pltpu.roll(odd[:8], 4, 0))
                last_ref[field * pairs + q] = jnp.where(
                    low, pltpu.roll(even[by - 8 :], 4, 0), odd[by - 8 :]
                )

    edge = struct(2 * pairs, 8, bz)
    return pl.pallas_call(
        kernel,
        name="pack_y",
        compiler_params=PARAMS,
        out_shape=(edge, edge),
        in_specs=[VMEM] * 4,
        out_specs=(VMEM,) * 2,
    )(gradient, velocity, before_x, after_x)


def rows_of(before_ref, after_ref, field, p, pairs):
    after = after_ref[field * pairs + p // 2]
    before = before_ref[field * pairs + p // 2]
    low = sublane(after.shape) < 4
    if p % 2 == 0:
        return jnp.where(low, after, pltpu.roll(before, 4, 0))
    return jnp.where(low, pltpu.roll(after, 4, 0), before)


def pack_z(gradient, velocity, before_x, after_x, before_y, after_y, squares):
    bx, by, bz = velocity.shape
    planes = bx + 2 * HALO
    pairs = planes // 2
    groups = bz // 4
    tall = by + 8

    def kernel(g_ref, v_ref, bx_ref, ax_ref, by_ref, ay_ref, sq_ref, first_ref, last_ref, sum_ref):
        group = lane((tall, bz)) // 4
        for field, main in enumerate((g_ref, v_ref)):
            first = jnp.zeros((tall, bz), F32)
            last = jnp.zeros((tall, bz), F32)
            for p in range(planes):
                own = plane_of(main, bx_ref, ax_ref, field, p, bx)
                extra = rows_of(by_ref, ay_ref, field, p, pairs)
                plane = jnp.concatenate([own, extra], 0)
                turned = pltpu.roll(plane, 4 * p, 1) if p else plane
                first = jnp.where(group == p, turned, first)
                last = jnp.where(group == (p - 1) % groups, turned, last)
            first_ref[pl.ds(field * tall, tall)] = first
            last_ref[pl.ds(field * tall, tall)] = last
        total = jnp.broadcast_to(jnp.sum(sq_ref[...], axis=0), (8, bz))
        first_ref[pl.ds(2 * tall, 8)] = total
        last_ref[pl.ds(2 * tall, 8)] = total
        sum_ref[...] = total

    edge = struct(2 * tall + 8, bz)
    return pl.pallas_call(
        kernel,
        name="pack_z",
        compiler_params=PARAMS,
        out_shape=(edge, edge, struct(8, bz)),
        in_specs=[VMEM] * 7,
        out_specs=(VMEM,) * 3,
    )(gradient, velocity, before_x, after_x, before_y, after_y, squares)


def proximal(device, gradient, velocity, halos, sums, sizes):
    bx, by, bz = velocity.shape
    planes = bx + 2 * HALO
    pairs = planes // 2
    tall = by + 8
    wide = 2 * bz
    size_x, size_y, size_z = sizes
    cells = size_x * bx * size_y * by * size_z * bz

    def kernel(
        dev_ref,
        g_ref,
        v_ref,
        bx_ref,
        ax_ref,
        by_ref,
        ay_ref,
        bz_ref,
        az_ref,
        own_ref,
        far_ref,
        gradient_ref,
        model_ref,
        target,
        current,
        extra,
        dual_x,
        dual_y,
        dual_z,
        model,
        sems,
    ):
        gradient_copy = pltpu.make_async_copy(g_ref, gradient_ref, sems.at[0])
        gradient_copy.start()
        dev = dev_ref[0]
        pos_z = dev % size_z
        pos_y = (dev // size_z) % size_y
        pos_x = dev // (size_z * size_y)

        total = own_ref[0:1] + far_ref[0:1]
        total = total + bz_ref[2 * tall : 2 * tall + 1] + az_ref[2 * tall : 2 * tall + 1]
        total = jnp.sum(total, axis=1, keepdims=True)
        scale = step_length * lax.rsqrt(total / cells + 1.0)
        scale = jnp.broadcast_to(scale, (1, bz))

        side_lane = lane((tall, bz)) < bz // 2
        before_z = bz_ref[pl.ds(tall, tall)] - scale * bz_ref[pl.ds(0, tall)]
        after_z = az_ref[pl.ds(tall, tall)] - scale * az_ref[pl.ds(0, tall)]
        for p in range(planes):
            own = plane_of(v_ref, bx_ref, ax_ref, 1, p, bx) - scale * plane_of(
                g_ref, bx_ref, ax_ref, 0, p, bx
            )
            rows = rows_of(by_ref, ay_ref, 1, p, pairs) - scale * rows_of(
                by_ref, ay_ref, 0, p, pairs
            )
            back = (bz - 4 * p) % bz
            after = pltpu.roll(after_z, back, 1) if back else after_z
            before = pltpu.roll(before_z, back, 1) if back else before_z
            target[p, pl.ds(0, by), pl.ds(0, bz)] = own
            target[p, pl.ds(by, 8), pl.ds(0, bz)] = rows
            target[p, :, pl.ds(bz, bz)] = jnp.where(side_lane, after, before)

        def factor(index, limit):
            return jnp.where((index >= 0) & (index < limit - 1), dual_step, 0.0).astype(F32)

        row = sublane((tall, 1))
        row = jnp.where(row < by + 4, row, row - tall) + pos_y * by
        factor_y = factor(row, size_y * by)
        col = lane((1, wide))
        col = jnp.where(col < bz + bz // 2, col, col - wide) + pos_z * bz
        factor_z = factor(col, size_z * bz)
        shrink = 1.0 / (1.0 + primal_step)
        gain = primal_step / (1.0 + primal_step)

        for iteration in range(ITERS):
            first = iteration == 0
            final = iteration == ITERS - 1
            here_ref = target if first else extra
            ahead = here_ref[iteration]
            before_x = None
            for p in range(iteration, planes - 1 - iteration):
                here = ahead
                ahead = here_ref[p + 1]
                index = pos_x * bx + (p - HALO)
                factor_x = factor(index, size_x * bx)
                dx = factor_x * (ahead - here)
                dy = factor_y * (pltpu.roll(here, tall - 1, 0) - here)
                dz = factor_z * (pltpu.roll(here, wide - 1, 1) - here)
                if not first:
                    dx = dual_x[p] + dx
                    dy = dual_y[p] + dy
                    dz = dual_z[p] + dz
                norm = dx * dx + dy * dy + dz * dz
                ratio = jnp.minimum(1.0, tv_weight * lax.rsqrt(norm))
                dx = dx * ratio
                dy = dy * ratio
                dz = dz * ratio
                if not final:
                    dual_x[p] = dx
                    dual_y[p] = dy
                    dual_z[p] = dz
                if p > iteration:
                    if final:
                        spread = dx[:by, :bz] - before_x
                        spread += dy[:by, :bz] - pltpu.roll(dy[:, :bz], 1, 0)[:by]
                        spread += dz[:by, :bz] - pltpu.roll(dz[:by], 1, 1)[:, :bz]
                        goal = target[p, pl.ds(0, by), pl.ds(0, bz)]
                        old = current[p, pl.ds(0, by), pl.ds(0, bz)]
                        model[p - HALO] = shrink * old + gain * (spread + goal)
                    else:
                        spread = dx - before_x
                        spread += dy - pltpu.roll(dy, 1, 0)
                        spread += dz - pltpu.roll(dz, 1, 1)
                        if first:
                            new = here + gain * spread
                            old = here
                        else:
                            old = current[p]
                            new = shrink * old + gain * (spread + target[p])
                        current[p] = new
                        extra[p] = 2.0 * new - old
                before_x = dx[:by, :bz] if final else dx
        model_copy = pltpu.make_async_copy(model, model_ref, sems.at[1])
        model_copy.start()
        gradient_copy.wait()
        model_copy.wait()

    field = pltpu.VMEM((planes, tall, wide), F32)
    return pl.pallas_call(
        kernel,
        name="proximal",
        compiler_params=PARAMS,
        out_shape=(struct(bx, by, bz),) * 2,
        in_specs=[SMEM] + [VMEM] * 10,
        out_specs=(HBM,) * 2,
        scratch_shapes=[field] * 6 + [pltpu.VMEM((bx, by, bz), F32), pltpu.SemaphoreType.DMA((2,))],
    )(device, gradient, velocity, *halos, *sums)


def shards(partials, code_bits, group_map, velocity):
    _, _, bz = velocity.shape
    size_x, size_y, size_z = (lax.axis_size(axis) for axis in (GX, GY, "gz"))
    base = (lax.axis_index(GX) * partials.shape[0]).astype(jnp.int32).reshape(1)
    device = lax.axis_index(ALL).astype(jnp.int32).reshape(1)

    local = presum(partials, code_bits, group_map, base, 8)
    parts = lax.all_to_all(local, GX, split_axis=0, concat_axis=0, tiled=True)
    gradient, first_x, last_x, squares = reduce_pack(parts, velocity, size_x)

    after_x = shift(first_x, GX, -1)
    before_x = shift(last_x, GX, 1)
    table = jnp.broadcast_to(squares[:1][None], (size_x * size_y, 1, bz))
    table = lax.all_to_all(table, XY, split_axis=0, concat_axis=0, tiled=True)

    first_y, last_y = pack_y(gradient, velocity, before_x, after_x)
    after_y = shift(first_y, GY, -1)
    before_y = shift(last_y, GY, 1)

    first_z, last_z, own = pack_z(gradient, velocity, before_x, after_x, before_y, after_y, table)
    after_z = shift(first_z, "gz", -1)
    before_z = shift(last_z, "gz", 1)
    far = shift(own, "gz", 2)
    return proximal(
        device,
        gradient,
        velocity,
        (before_x, after_x, before_y, after_y, before_z, after_z),
        (own, far),
        (size_x, size_y, size_z),
    )


def solution(mesh):
    torus = Mesh(
        mesh.devices.reshape(4, 2, 4, 2, mesh.shape["gz"]), ("gx_0", "gx_1", "gy_0", "gy_1", "gz")
    )
    placed = (P(GX, None, GY, "gz"), P(), P(), P(GX, GY, "gz"))
    return jax.shard_map(
        shards,
        mesh=torus,
        in_specs=placed,
        out_specs=(P(GX, GY, "gz"), P(GX, GY, "gz")),
        check_vma=False,
    )
```

```python
import jax
import jax.numpy as jnp
from jax import lax
from jax.experimental import pallas as pl
from jax.experimental.pallas import tpu as pltpu
from jax.sharding import Mesh
from jax.sharding import PartitionSpec as P

ITERS = 3
HALO = ITERS
GX = ("gx_0", "gx_1")
GY = ("gy_0", "gy_1")
ALL = GX + GY + ("gz",)

step_length = 0.5
tv_weight = 0.2
dual_step = 0.28
primal_step = 0.28

VMEM = pl.BlockSpec(memory_space=pltpu.VMEM)
SMEM = pl.BlockSpec(memory_space=pltpu.SMEM)
HBM = pl.BlockSpec(memory_space=pltpu.HBM)
PARAMS = pltpu.CompilerParams(vmem_limit_bytes=16 * 1024 * 1024)
F32 = jnp.float32


def shift(block, axis, distance):
    size = lax.axis_size(axis)
    return lax.ppermute(block, axis, [(i, (i + distance) % size) for i in range(size)])


def struct(*shape):
    return jax.ShapeDtypeStruct(shape, F32)


def in_hbm(array):
    return pltpu.with_memory_space_constraint(array, pltpu.HBM)


def presum(partials, code_bits, group_map, base, chunks):
    slots, nx, by, bz = partials.shape
    rows = nx // chunks

    def kernel(base_ref, map_hbm, bits_hbm, part_ref, out_ref, buf, map_ref, bits_ref, sems):
        map_copy = pltpu.make_async_copy(map_hbm, map_ref, sems.at[chunks])
        bits_copy = pltpu.make_async_copy(bits_hbm, bits_ref, sems.at[chunks + 1])
        map_copy.start()
        bits_copy.start()

        def copy(c):
            part = pl.ds(c * rows, rows)
            return pltpu.make_async_copy(part_ref.at[:, part], buf.at[:, part], sems.at[c])

        for c in range(chunks):
            copy(c).start()
        map_copy.wait()
        bits_copy.wait()
        groups = [map_ref[base_ref[0] + s] for s in range(slots)]
        for c in range(chunks):
            copy(c).wait()

            def row(i, carry):
                x = c * rows + i
                total = None
                for s in range(slots):
                    sign = (2 * bits_ref[groups[s], x] - 1).astype(F32)
                    term = sign * buf[s, x]
                    total = term if total is None else total + term
                out_ref[x] = total
                return carry

            lax.fori_loop(0, rows, row, 0, unroll=4)

    return pl.pallas_call(
        kernel,
        name="presum",
        compiler_params=PARAMS,
        out_shape=struct(nx, by, bz),
        in_specs=[SMEM, HBM, HBM, HBM],
        out_specs=VMEM,
        scratch_shapes=[
            pltpu.VMEM(partials.shape, F32),
            pltpu.SMEM(group_map.shape, jnp.int32),
            pltpu.SMEM(code_bits.shape, jnp.int32),
            pltpu.SemaphoreType.DMA((chunks + 2,)),
        ],
    )(base, in_hbm(group_map), in_hbm(code_bits), in_hbm(partials))


def reduce_pack(parts, velocity, members):
    bx, by, bz = velocity.shape

    def kernel(part_ref, v_ref, g_ref, first_ref, last_ref, square_ref):
        squares = jnp.zeros((by, bz), F32)
        for i in range(bx):
            total = part_ref[i]
            for m in range(1, members):
                total = total + part_ref[m * bx + i]
            g_ref[i] = total
            squares = squares + total * total
            if i < HALO:
                first_ref[i] = total
                first_ref[HALO + i] = v_ref[i]
            if i >= bx - HALO:
                last_ref[i - bx + HALO] = total
                last_ref[i - bx + 2 * HALO] = v_ref[i]
        square_ref[...] = jnp.broadcast_to(jnp.sum(squares, axis=0, keepdims=True), (8, bz))

    edge = struct(2 * HALO, by, bz)
    return pl.pallas_call(
        kernel,
        name="reduce_pack",
        compiler_params=PARAMS,
        out_shape=(struct(bx, by, bz), edge, edge, struct(8, bz)),
        in_specs=[VMEM, VMEM],
        out_specs=(VMEM,) * 4,
    )(parts, velocity)


def plane_of(main_ref, before_ref, after_ref, field, p, bx):
    if p < HALO:
        return before_ref[field * HALO + p]
    if p < HALO + bx:
        return main_ref[p - HALO]
    return after_ref[field * HALO + p - HALO - bx]


def sublane(shape):
    return lax.broadcasted_iota(jnp.int32, shape, len(shape) - 2)


def lane(shape):
    return lax.broadcasted_iota(jnp.int32, shape, len(shape) - 1)


def pack_y(gradient, velocity, before_x, after_x):
    bx, by, bz = velocity.shape
    pairs = (bx + 2 * HALO) // 2

    def kernel(g_ref, v_ref, before_ref, after_ref, first_ref, last_ref):
        low = sublane((8, bz)) < 4
        for field, main in enumerate((g_ref, v_ref)):
            for q in range(pairs):
                even = plane_of(main, before_ref, after_ref, field, 2 * q, bx)
                odd = plane_of(main, before_ref, after_ref, field, 2 * q + 1, bx)
                first_ref[field * pairs + q] = jnp.where(low, even[:8], pltpu.roll(odd[:8], 4, 0))
                last_ref[field * pairs + q] = jnp.where(
                    low, pltpu.roll(even[by - 8 :], 4, 0), odd[by - 8 :]
                )

    edge = struct(2 * pairs, 8, bz)
    return pl.pallas_call(
        kernel,
        name="pack_y",
        compiler_params=PARAMS,
        out_shape=(edge, edge),
        in_specs=[VMEM] * 4,
        out_specs=(VMEM,) * 2,
    )(gradient, velocity, before_x, after_x)


def rows_of(before_ref, after_ref, field, p, pairs):
    after = after_ref[field * pairs + p // 2]
    before = before_ref[field * pairs + p // 2]
    low = sublane(after.shape) < 4
    if p % 2 == 0:
        return jnp.where(low, after, pltpu.roll(before, 4, 0))
    return jnp.where(low, pltpu.roll(after, 4, 0), before)


def pack_z(gradient, velocity, before_x, after_x, before_y, after_y):
    bx, by, bz = velocity.shape
    planes = bx + 2 * HALO
    pairs = planes // 2
    groups = bz // 4
    tall = by + 8

    def kernel(g_ref, v_ref, bx_ref, ax_ref, by_ref, ay_ref, first_ref, last_ref):
        group = lane((tall, bz)) // 4
        for field, main in enumerate((g_ref, v_ref)):
            first = jnp.zeros((tall, bz), F32)
            last = jnp.zeros((tall, bz), F32)
            for p in range(planes):
                own = plane_of(main, bx_ref, ax_ref, field, p, bx)
                extra = rows_of(by_ref, ay_ref, field, p, pairs)
                plane = jnp.concatenate([own, extra], 0)
                turned = pltpu.roll(plane, 4 * p, 1) if p else plane
                first = jnp.where(group == p, turned, first)
                last = jnp.where(group == (p - 1) % groups, turned, last)
            first_ref[pl.ds(field * tall, tall)] = first
            last_ref[pl.ds(field * tall, tall)] = last

    edge = struct(2 * tall, bz)
    return pl.pallas_call(
        kernel,
        name="pack_z",
        compiler_params=PARAMS,
        out_shape=(edge, edge),
        in_specs=[VMEM] * 6,
        out_specs=(VMEM,) * 2,
    )(gradient, velocity, before_x, after_x, before_y, after_y)


def proximal(device, gradient, velocity, halos, squares, sizes):
    bx, by, bz = velocity.shape
    planes = bx + 2 * HALO
    pairs = planes // 2
    tall = by + 8
    wide = 2 * bz
    size_x, size_y, size_z = sizes
    cells = size_x * bx * size_y * by * size_z * bz

    def kernel(
        dev_ref,
        g_ref,
        v_ref,
        bx_ref,
        ax_ref,
        by_ref,
        ay_ref,
        bz_ref,
        az_ref,
        sq_ref,
        gradient_ref,
        model_ref,
        target,
        current,
        extra,
        dual_x,
        dual_y,
        dual_z,
        model,
        sems,
    ):
        gradient_copy = pltpu.make_async_copy(g_ref, gradient_ref, sems.at[0])
        gradient_copy.start()
        dev = dev_ref[0]
        pos_z = dev % size_z
        pos_y = (dev // size_z) % size_y
        pos_x = dev // (size_z * size_y)

        total = jnp.sum(jnp.sum(sq_ref[...], axis=0), axis=1, keepdims=True)
        scale = step_length * lax.rsqrt(total / cells + 1.0)
        scale = jnp.broadcast_to(scale, (1, bz))

        side_lane = lane((tall, bz)) < bz // 2
        before_z = bz_ref[pl.ds(tall, tall)] - scale * bz_ref[pl.ds(0, tall)]
        after_z = az_ref[pl.ds(tall, tall)] - scale * az_ref[pl.ds(0, tall)]
        for p in range(planes):
            own = plane_of(v_ref, bx_ref, ax_ref, 1, p, bx) - scale * plane_of(
                g_ref, bx_ref, ax_ref, 0, p, bx
            )
            rows = rows_of(by_ref, ay_ref, 1, p, pairs) - scale * rows_of(
                by_ref, ay_ref, 0, p, pairs
            )
            back = (bz - 4 * p) % bz
            after = pltpu.roll(after_z, back, 1) if back else after_z
            before = pltpu.roll(before_z, back, 1) if back else before_z
            target[p, pl.ds(0, by), pl.ds(0, bz)] = own
            target[p, pl.ds(by, 8), pl.ds(0, bz)] = rows
            target[p, :, pl.ds(bz, bz)] = jnp.where(side_lane, after, before)

        def factor(index, limit):
            return jnp.where((index >= 0) & (index < limit - 1), dual_step, 0.0).astype(F32)

        row = sublane((tall, 1))
        row = jnp.where(row < by + 4, row, row - tall) + pos_y * by
        factor_y = factor(row, size_y * by)
        col = lane((1, wide))
        col = jnp.where(col < bz + bz // 2, col, col - wide) + pos_z * bz
        factor_z = factor(col, size_z * bz)
        shrink = 1.0 / (1.0 + primal_step)
        gain = primal_step / (1.0 + primal_step)

        for iteration in range(ITERS):
            first = iteration == 0
            final = iteration == ITERS - 1
            here_ref = target if first else extra
            ahead = here_ref[iteration]
            before_x = None
            for p in range(iteration, planes - 1 - iteration):
                here = ahead
                ahead = here_ref[p + 1]
                index = pos_x * bx + (p - HALO)
                factor_x = factor(index, size_x * bx)
                dx = factor_x * (ahead - here)
                dy = factor_y * (pltpu.roll(here, tall - 1, 0) - here)
                dz = factor_z * (pltpu.roll(here, wide - 1, 1) - here)
                if not first:
                    dx = dual_x[p] + dx
                    dy = dual_y[p] + dy
                    dz = dual_z[p] + dz
                norm = dx * dx + dy * dy + dz * dz
                ratio = jnp.minimum(1.0, tv_weight * lax.rsqrt(norm))
                dx = dx * ratio
                dy = dy * ratio
                dz = dz * ratio
                if not final:
                    dual_x[p] = dx
                    dual_y[p] = dy
                    dual_z[p] = dz
                if p > iteration:
                    if final:
                        spread = dx[:by, :bz] - before_x
                        spread += dy[:by, :bz] - pltpu.roll(dy[:, :bz], 1, 0)[:by]
                        spread += dz[:by, :bz] - pltpu.roll(dz[:by], 1, 1)[:, :bz]
                        goal = target[p, pl.ds(0, by), pl.ds(0, bz)]
                        old = current[p, pl.ds(0, by), pl.ds(0, bz)]
                        model[p - HALO] = shrink * old + gain * (spread + goal)
                    else:
                        spread = dx - before_x
                        spread += dy - pltpu.roll(dy, 1, 0)
                        spread += dz - pltpu.roll(dz, 1, 1)
                        if first:
                            new = here + gain * spread
                            old = here
                        else:
                            old = current[p]
                            new = shrink * old + gain * (spread + target[p])
                        current[p] = new
                        extra[p] = 2.0 * new - old
                before_x = dx[:by, :bz] if final else dx
        model_copy = pltpu.make_async_copy(model, model_ref, sems.at[1])
        model_copy.start()
        gradient_copy.wait()
        model_copy.wait()

    field = pltpu.VMEM((planes, tall, wide), F32)
    return pl.pallas_call(
        kernel,
        name="proximal",
        compiler_params=PARAMS,
        out_shape=(struct(bx, by, bz),) * 2,
        in_specs=[SMEM] + [VMEM] * 9,
        out_specs=(HBM,) * 2,
        scratch_shapes=[field] * 6 + [pltpu.VMEM((bx, by, bz), F32), pltpu.SemaphoreType.DMA((2,))],
    )(device, gradient, velocity, *halos, squares)


def shards(partials, code_bits, group_map, velocity):
    _, _, bz = velocity.shape
    size_x, size_y, size_z = (lax.axis_size(axis) for axis in (GX, GY, "gz"))
    base = (lax.axis_index(GX) * partials.shape[0]).astype(jnp.int32).reshape(1)
    device = lax.axis_index(ALL).astype(jnp.int32).reshape(1)

    local = presum(partials, code_bits, group_map, base, 8)
    parts = lax.all_to_all(local, GX, split_axis=0, concat_axis=0, tiled=True)
    gradient, first_x, last_x, squares = reduce_pack(parts, velocity, size_x)

    after_x = shift(first_x, GX, -1)
    before_x = shift(last_x, GX, 1)
    table = jnp.broadcast_to(squares[:1][None], (size_x * size_y * size_z, 1, bz))
    table = lax.all_to_all(table, ALL, split_axis=0, concat_axis=0, tiled=True)

    first_y, last_y = pack_y(gradient, velocity, before_x, after_x)
    after_y = shift(first_y, GY, -1)
    before_y = shift(last_y, GY, 1)

    first_z, last_z = pack_z(gradient, velocity, before_x, after_x, before_y, after_y)
    after_z = shift(first_z, "gz", -1)
    before_z = shift(last_z, "gz", 1)

    return proximal(
        device,
        gradient,
        velocity,
        (before_x, after_x, before_y, after_y, before_z, after_z),
        table,
        (size_x, size_y, size_z),
    )


def solution(mesh):
    torus = Mesh(
        mesh.devices.reshape(4, 2, 4, 2, mesh.shape["gz"]), ("gx_0", "gx_1", "gy_0", "gy_1", "gz")
    )
    placed = (P(GX, None, GY, "gz"), P(), P(), P(GX, GY, "gz"))
    return jax.shard_map(
        shards,
        mesh=torus,
        in_specs=placed,
        out_specs=(P(GX, GY, "gz"), P(GX, GY, "gz")),
        check_vma=False,
    )
```

```python
import jax
import jax.numpy as jnp
from jax import lax
from jax.experimental import pallas as pl
from jax.experimental.pallas import tpu as pltpu
from jax.sharding import Mesh
from jax.sharding import PartitionSpec as P

ITERS = 3
HALO = ITERS
GX = ("gx_0", "gx_1")
GY = ("gy_0", "gy_1")
ALL = GX + GY + ("gz",)
REST = GX[:1] + GY + ("gz",)

step_length = 0.5
tv_weight = 0.2
dual_step = 0.28
primal_step = 0.28

VMEM = pl.BlockSpec(memory_space=pltpu.VMEM)
SMEM = pl.BlockSpec(memory_space=pltpu.SMEM)
HBM = pl.BlockSpec(memory_space=pltpu.HBM)
PARAMS = pltpu.CompilerParams(vmem_limit_bytes=16 * 1024 * 1024)
F32 = jnp.float32


def shift(block, axis, distance):
    size = lax.axis_size(axis)
    return lax.ppermute(block, axis, [(i, (i + distance) % size) for i in range(size)])


def struct(*shape):
    return jax.ShapeDtypeStruct(shape, F32)


def in_hbm(array):
    return pltpu.with_memory_space_constraint(array, pltpu.HBM)


def presum(partials, code_bits, group_map, base, chunks):
    slots, nx, by, bz = partials.shape
    rows = nx // chunks

    def kernel(base_ref, map_hbm, bits_hbm, part_ref, out_ref, buf, map_ref, bits_ref, sems):
        map_copy = pltpu.make_async_copy(map_hbm, map_ref, sems.at[chunks])
        bits_copy = pltpu.make_async_copy(bits_hbm, bits_ref, sems.at[chunks + 1])
        map_copy.start()
        bits_copy.start()

        def copy(c):
            part = pl.ds(c * rows, rows)
            return pltpu.make_async_copy(part_ref.at[:, part], buf.at[:, part], sems.at[c])

        for c in range(chunks):
            copy(c).start()
        map_copy.wait()
        bits_copy.wait()
        groups = [map_ref[base_ref[0] + s] for s in range(slots)]
        for c in range(chunks):
            copy(c).wait()

            def row(i, carry):
                x = c * rows + i
                total = None
                for s in range(slots):
                    sign = (2 * bits_ref[groups[s], x] - 1).astype(F32)
                    term = sign * buf[s, x]
                    total = term if total is None else total + term
                out_ref[x] = total
                return carry

            lax.fori_loop(0, rows, row, 0, unroll=4)

    return pl.pallas_call(
        kernel,
        name="presum",
        compiler_params=PARAMS,
        out_shape=struct(nx, by, bz),
        in_specs=[SMEM, HBM, HBM, HBM],
        out_specs=VMEM,
        scratch_shapes=[
            pltpu.VMEM(partials.shape, F32),
            pltpu.SMEM(group_map.shape, jnp.int32),
            pltpu.SMEM(code_bits.shape, jnp.int32),
            pltpu.SemaphoreType.DMA((chunks + 2,)),
        ],
    )(base, in_hbm(group_map), in_hbm(code_bits), in_hbm(partials))


def reduce_pack(parts, velocity, members):
    bx, by, bz = velocity.shape

    def kernel(part_ref, v_ref, g_ref, first_ref, last_ref, square_ref):
        squares = jnp.zeros((by, bz), F32)
        for i in range(bx):
            total = part_ref[i]
            for m in range(1, members):
                total = total + part_ref[m * bx + i]
            g_ref[i] = total
            squares = squares + total * total
            if i < HALO:
                first_ref[pl.ds(i * by, by)] = total
                first_ref[pl.ds((HALO + i) * by, by)] = v_ref[i]
            if i >= bx - HALO:
                last_ref[pl.ds((i - bx + HALO) * by, by)] = total
                last_ref[pl.ds((i - bx + 2 * HALO) * by, by)] = v_ref[i]
        row = jnp.broadcast_to(jnp.sum(squares, axis=0, keepdims=True), (8, bz))
        square_ref[...] = row
        first_ref[pl.ds(2 * HALO * by, 8)] = row
        last_ref[pl.ds(2 * HALO * by, 8)] = row

    edge = struct(2 * HALO * by + 8, bz)
    return pl.pallas_call(
        kernel,
        name="reduce_pack",
        compiler_params=PARAMS,
        out_shape=(struct(bx, by, bz), edge, edge, struct(8, bz)),
        in_specs=[VMEM, VMEM],
        out_specs=(VMEM,) * 4,
    )(parts, velocity)


def plane_of(main_ref, before_ref, after_ref, field, p):
    bx, by, _ = main_ref.shape
    if p < HALO:
        return before_ref[pl.ds((field * HALO + p) * by, by)]
    if p < HALO + bx:
        return main_ref[p - HALO]
    return after_ref[pl.ds((field * HALO + p - HALO - bx) * by, by)]


def sublane(shape):
    return lax.broadcasted_iota(jnp.int32, shape, len(shape) - 2)


def lane(shape):
    return lax.broadcasted_iota(jnp.int32, shape, len(shape) - 1)


def pack_y(device, gradient, velocity, before_x, after_x, squares, sizes):
    bx, by, bz = velocity.shape
    pairs = (bx + 2 * HALO) // 2
    size_x, size_y, size_z = sizes
    receivers = size_x // 2 * size_y * size_z

    def kernel(
        dev_ref, g_ref, v_ref, before_ref, after_ref, sq_ref, first_ref, last_ref, table_ref
    ):
        even_x = (dev_ref[0] // (size_y * size_z)) % 2 == 0
        where = pl.ds(2 * HALO * by, 8)
        row = sq_ref[...] + jnp.where(even_x, after_ref[where], before_ref[where])
        table_ref[...] = jnp.broadcast_to(row[:1][None], table_ref.shape)
        low = sublane((8, bz)) < 4
        for field, main in enumerate((g_ref, v_ref)):
            for q in range(pairs):
                even = plane_of(main, before_ref, after_ref, field, 2 * q)
                odd = plane_of(main, before_ref, after_ref, field, 2 * q + 1)
                first_ref[field * pairs + q] = jnp.where(low, even[:8], pltpu.roll(odd[:8], 4, 0))
                last_ref[field * pairs + q] = jnp.where(
                    low, pltpu.roll(even[by - 8 :], 4, 0), odd[by - 8 :]
                )

    edge = struct(2 * pairs, 8, bz)
    return pl.pallas_call(
        kernel,
        name="pack_y",
        compiler_params=PARAMS,
        out_shape=(edge, edge, struct(receivers, 1, bz)),
        in_specs=[SMEM] + [VMEM] * 5,
        out_specs=(VMEM,) * 3,
    )(device, gradient, velocity, before_x, after_x, squares)


def rows_of(before_ref, after_ref, field, p, pairs):
    after = after_ref[field * pairs + p // 2]
    before = before_ref[field * pairs + p // 2]
    low = sublane(after.shape) < 4
    if p % 2 == 0:
        return jnp.where(low, after, pltpu.roll(before, 4, 0))
    return jnp.where(low, pltpu.roll(after, 4, 0), before)


def pack_z(gradient, velocity, before_x, after_x, before_y, after_y):
    bx, by, bz = velocity.shape
    planes = bx + 2 * HALO
    pairs = planes // 2
    groups = bz // 4
    tall = by + 8

    def kernel(g_ref, v_ref, bx_ref, ax_ref, by_ref, ay_ref, first_ref, last_ref):
        group = lane((tall, bz)) // 4
        for field, main in enumerate((g_ref, v_ref)):
            first = jnp.zeros((tall, bz), F32)
            last = jnp.zeros((tall, bz), F32)
            for p in range(planes):
                own = plane_of(main, bx_ref, ax_ref, field, p)
                extra = rows_of(by_ref, ay_ref, field, p, pairs)
                plane = jnp.concatenate([own, extra], 0)
                turned = pltpu.roll(plane, 4 * p, 1) if p else plane
                first = jnp.where(group == p, turned, first)
                last = jnp.where(group == (p - 1) % groups, turned, last)
            first_ref[pl.ds(field * tall, tall)] = first
            last_ref[pl.ds(field * tall, tall)] = last

    edge = struct(2 * tall, bz)
    return pl.pallas_call(
        kernel,
        name="pack_z",
        compiler_params=PARAMS,
        out_shape=(edge, edge),
        in_specs=[VMEM] * 6,
        out_specs=(VMEM,) * 2,
    )(gradient, velocity, before_x, after_x, before_y, after_y)


def proximal(device, gradient, velocity, halos, squares, sizes):
    bx, by, bz = velocity.shape
    planes = bx + 2 * HALO
    pairs = planes // 2
    tall = by + 8
    wide = 2 * bz
    size_x, size_y, size_z = sizes
    cells = size_x * bx * size_y * by * size_z * bz

    def kernel(
        dev_ref,
        g_ref,
        v_ref,
        bx_ref,
        ax_ref,
        by_ref,
        ay_ref,
        bz_ref,
        az_ref,
        sq_ref,
        gradient_ref,
        model_ref,
        target,
        current,
        extra,
        dual_x,
        dual_y,
        dual_z,
        model,
        sems,
    ):
        gradient_copy = pltpu.make_async_copy(g_ref, gradient_ref, sems.at[0])
        gradient_copy.start()
        dev = dev_ref[0]
        pos_z = dev % size_z
        pos_y = (dev // size_z) % size_y
        pos_x = dev // (size_z * size_y)

        total = jnp.sum(jnp.sum(sq_ref[...], axis=0), axis=1, keepdims=True)
        scale = step_length * lax.rsqrt(total / cells + 1.0)
        scale = jnp.broadcast_to(scale, (1, bz))

        side_lane = lane((tall, bz)) < bz // 2
        before_z = bz_ref[pl.ds(tall, tall)] - scale * bz_ref[pl.ds(0, tall)]
        after_z = az_ref[pl.ds(tall, tall)] - scale * az_ref[pl.ds(0, tall)]
        for p in range(planes):
            own = plane_of(v_ref, bx_ref, ax_ref, 1, p) - scale * plane_of(g_ref, bx_ref, ax_ref, 0, p)
            rows = rows_of(by_ref, ay_ref, 1, p, pairs) - scale * rows_of(
                by_ref, ay_ref, 0, p, pairs
            )
            back = (bz - 4 * p) % bz
            after = pltpu.roll(after_z, back, 1) if back else after_z
            before = pltpu.roll(before_z, back, 1) if back else before_z
            target[p, pl.ds(0, by), pl.ds(0, bz)] = own
            target[p, pl.ds(by, 8), pl.ds(0, bz)] = rows
            target[p, :, pl.ds(bz, bz)] = jnp.where(side_lane, after, before)

        def factor(index, limit):
            return jnp.where((index >= 0) & (index < limit - 1), dual_step, 0.0).astype(F32)

        row = sublane((tall, 1))
        row = jnp.where(row < by + 4, row, row - tall) + pos_y * by
        factor_y = factor(row, size_y * by)
        col = lane((1, wide))
        col = jnp.where(col < bz + bz // 2, col, col - wide) + pos_z * bz
        factor_z = factor(col, size_z * bz)
        shrink = 1.0 / (1.0 + primal_step)
        gain = primal_step / (1.0 + primal_step)

        for iteration in range(ITERS):
            first = iteration == 0
            final = iteration == ITERS - 1
            here_ref = target if first else extra
            ahead = here_ref[iteration]
            before_x = None
            for p in range(iteration, planes - 1 - iteration):
                here = ahead
                ahead = here_ref[p + 1]
                index = pos_x * bx + (p - HALO)
                factor_x = factor(index, size_x * bx)
                dx = factor_x * (ahead - here)
                dy = factor_y * (pltpu.roll(here, tall - 1, 0) - here)
                dz = factor_z * (pltpu.roll(here, wide - 1, 1) - here)
                if not first:
                    dx = dual_x[p] + dx
                    dy = dual_y[p] + dy
                    dz = dual_z[p] + dz
                norm = dx * dx + dy * dy + dz * dz
                ratio = jnp.minimum(1.0, tv_weight * lax.rsqrt(norm))
                dx = dx * ratio
                dy = dy * ratio
                dz = dz * ratio
                if not final:
                    dual_x[p] = dx
                    dual_y[p] = dy
                    dual_z[p] = dz
                if p > iteration:
                    if final:
                        spread = dx[:by, :bz] - before_x
                        spread += dy[:by, :bz] - pltpu.roll(dy[:, :bz], 1, 0)[:by]
                        spread += dz[:by, :bz] - pltpu.roll(dz[:by], 1, 1)[:, :bz]
                        goal = target[p, pl.ds(0, by), pl.ds(0, bz)]
                        old = current[p, pl.ds(0, by), pl.ds(0, bz)]
                        model[p - HALO] = shrink * old + gain * (spread + goal)
                    else:
                        spread = dx - before_x
                        spread += dy - pltpu.roll(dy, 1, 0)
                        spread += dz - pltpu.roll(dz, 1, 1)
                        if first:
                            new = here + gain * spread
                            old = here
                        else:
                            old = current[p]
                            new = shrink * old + gain * (spread + target[p])
                        current[p] = new
                        extra[p] = 2.0 * new - old
                before_x = dx[:by, :bz] if final else dx
        model_copy = pltpu.make_async_copy(model, model_ref, sems.at[1])
        model_copy.start()
        gradient_copy.wait()
        model_copy.wait()

    field = pltpu.VMEM((planes, tall, wide), F32)
    return pl.pallas_call(
        kernel,
        name="proximal",
        compiler_params=PARAMS,
        out_shape=(struct(bx, by, bz),) * 2,
        in_specs=[SMEM] + [VMEM] * 9,
        out_specs=(HBM,) * 2,
        scratch_shapes=[field] * 6 + [pltpu.VMEM((bx, by, bz), F32), pltpu.SemaphoreType.DMA((2,))],
    )(device, gradient, velocity, *halos, squares)


def shards(partials, code_bits, group_map, velocity):
    sizes = tuple(lax.axis_size(axis) for axis in (GX, GY, "gz"))
    base = (lax.axis_index(GX) * partials.shape[0]).astype(jnp.int32).reshape(1)
    device = lax.axis_index(ALL).astype(jnp.int32).reshape(1)

    local = presum(partials, code_bits, group_map, base, 8)
    parts = lax.all_to_all(local, GX, split_axis=0, concat_axis=0, tiled=True)
    gradient, first_x, last_x, squares = reduce_pack(parts, velocity, sizes[0])

    after_x = shift(first_x, GX, -1)
    before_x = shift(last_x, GX, 1)
    first_y, last_y, table = pack_y(device, gradient, velocity, before_x, after_x, squares, sizes)
    after_y = shift(first_y, GY, -1)
    before_y = shift(last_y, GY, 1)
    table = lax.all_to_all(table, REST, split_axis=0, concat_axis=0, tiled=True)

    first_z, last_z = pack_z(gradient, velocity, before_x, after_x, before_y, after_y)
    after_z = shift(first_z, "gz", -1)
    before_z = shift(last_z, "gz", 1)

    return proximal(
        device,
        gradient,
        velocity,
        (before_x, after_x, before_y, after_y, before_z, after_z),
        table,
        sizes,
    )


def solution(mesh):
    torus = Mesh(
        mesh.devices.reshape(4, 2, 4, 2, mesh.shape["gz"]), ("gx_0", "gx_1", "gy_0", "gy_1", "gz")
    )
    placed = (P(GX, None, GY, "gz"), P(), P(), P(GX, GY, "gz"))
    return jax.shard_map(
        shards,
        mesh=torus,
        in_specs=placed,
        out_specs=(P(GX, GY, "gz"), P(GX, GY, "gz")),
        check_vma=False,
    )
```

```python
import jax
import jax.numpy as jnp
from jax import lax
from jax.experimental import pallas as pl
from jax.experimental.pallas import tpu as pltpu
from jax.sharding import Mesh
from jax.sharding import PartitionSpec as P

ITERS = 3
HALO = ITERS
GX = ("gx_0", "gx_1")
GY = ("gy_0", "gy_1")
ALL = GX + GY + ("gz",)
XZ = GX + ("gz",)

step_length = 0.5
tv_weight = 0.2
dual_step = 0.28
primal_step = 0.28

VMEM = pl.BlockSpec(memory_space=pltpu.VMEM)
SMEM = pl.BlockSpec(memory_space=pltpu.SMEM)
HBM = pl.BlockSpec(memory_space=pltpu.HBM)
PARAMS = pltpu.CompilerParams(vmem_limit_bytes=16 * 1024 * 1024)
F32 = jnp.float32


def shift(block, axis, distance):
    devices = range(lax.axis_size(axis))
    return lax.ppermute(block, axis, [(i, i + distance) for i in devices if i + distance in devices])


def turn(block, axis, distance):
    size = lax.axis_size(axis)
    return lax.ppermute(block, axis, [(i, (i + distance) % size) for i in range(size)])


def struct(*shape):
    return jax.ShapeDtypeStruct(shape, F32)


def in_hbm(array):
    return pltpu.with_memory_space_constraint(array, pltpu.HBM)


def presum(partials, code_bits, group_map, base, chunks):
    slots, nx, by, bz = partials.shape
    rows = nx // chunks

    def kernel(base_ref, map_hbm, bits_hbm, part_ref, out_ref, buf, map_ref, bits_ref, sems):
        map_copy = pltpu.make_async_copy(map_hbm, map_ref, sems.at[chunks])
        bits_copy = pltpu.make_async_copy(bits_hbm, bits_ref, sems.at[chunks + 1])
        map_copy.start()
        bits_copy.start()

        def copy(c):
            part = pl.ds(c * rows, rows)
            return pltpu.make_async_copy(part_ref.at[:, part], buf.at[:, part], sems.at[c])

        for c in range(chunks):
            copy(c).start()
        map_copy.wait()
        bits_copy.wait()
        groups = [map_ref[base_ref[0] + s] for s in range(slots)]
        for c in range(chunks):
            copy(c).wait()

            def row(i, carry):
                x = c * rows + i
                total = None
                for s in range(slots):
                    sign = (2 * bits_ref[groups[s], x] - 1).astype(F32)
                    term = sign * buf[s, x]
                    total = term if total is None else total + term
                out_ref[x] = total
                return carry

            lax.fori_loop(0, rows, row, 0, unroll=4)

    return pl.pallas_call(
        kernel,
        name="presum",
        compiler_params=PARAMS,
        out_shape=struct(nx, by, bz),
        in_specs=[SMEM, HBM, HBM, HBM],
        out_specs=VMEM,
        scratch_shapes=[
            pltpu.VMEM(partials.shape, F32),
            pltpu.SMEM(group_map.shape, jnp.int32),
            pltpu.SMEM(code_bits.shape, jnp.int32),
            pltpu.SemaphoreType.DMA((chunks + 2,)),
        ],
    )(base, in_hbm(group_map), in_hbm(code_bits), in_hbm(partials))


def reduce_pack(parts, velocity, members):
    bx, by, bz = velocity.shape

    def kernel(part_ref, v_ref, g_ref, first_ref, last_ref, square_ref):
        squares = jnp.zeros((by, bz), F32)
        for i in range(bx):
            total = part_ref[i]
            for m in range(1, members):
                total = total + part_ref[m * bx + i]
            g_ref[i] = total
            squares = squares + total * total
            if i < HALO:
                first_ref[i] = total
                first_ref[HALO + i] = v_ref[i]
            if i >= bx - HALO:
                last_ref[i - bx + HALO] = total
                last_ref[i - bx + 2 * HALO] = v_ref[i]
        square_ref[...] = jnp.broadcast_to(jnp.sum(squares, axis=0, keepdims=True), (8, bz))

    edge = struct(2 * HALO, by, bz)
    return pl.pallas_call(
        kernel,
        name="reduce_pack",
        compiler_params=PARAMS,
        out_shape=(struct(bx, by, bz), edge, edge, struct(8, bz)),
        in_specs=[VMEM, VMEM],
        out_specs=(VMEM,) * 4,
    )(parts, velocity)


def plane_of(main_ref, before_ref, after_ref, field, p, bx):
    if p < HALO:
        return before_ref[field * HALO + p]
    if p < HALO + bx:
        return main_ref[p - HALO]
    return after_ref[field * HALO + p - HALO - bx]


def sublane(shape):
    return lax.broadcasted_iota(jnp.int32, shape, len(shape) - 2)


def lane(shape):
    return lax.broadcasted_iota(jnp.int32, shape, len(shape) - 1)


def pack_y(gradient, velocity, before_x, after_x):
    bx, by, bz = velocity.shape
    pairs = (bx + 2 * HALO) // 2

    def kernel(g_ref, v_ref, before_ref, after_ref, first_ref, last_ref):
        low = sublane((8, bz)) < 4
        for field, main in enumerate((g_ref, v_ref)):
            for q in range(pairs):
                even = plane_of(main, before_ref, after_ref, field, 2 * q, bx)
                odd = plane_of(main, before_ref, after_ref, field, 2 * q + 1, bx)
                first_ref[field * pairs + q] = jnp.where(low, even[:8], pltpu.roll(odd[:8], 4, 0))
                last_ref[field * pairs + q] = jnp.where(
                    low, pltpu.roll(even[by - 8 :], 4, 0), odd[by - 8 :]
                )

    edge = struct(2 * pairs, 8, bz)
    return pl.pallas_call(
        kernel,
        name="pack_y",
        compiler_params=PARAMS,
        out_shape=(edge, edge),
        in_specs=[VMEM] * 4,
        out_specs=(VMEM,) * 2,
    )(gradient, velocity, before_x, after_x)


def rows_of(before_ref, after_ref, field, p, pairs):
    after = after_ref[field * pairs + p // 2]
    before = before_ref[field * pairs + p // 2]
    low = sublane(after.shape) < 4
    if p % 2 == 0:
        return jnp.where(low, after, pltpu.roll(before, 4, 0))
    return jnp.where(low, pltpu.roll(after, 4, 0), before)


def pack_z(gradient, velocity, before_x, after_x, before_y, after_y):
    bx, by, bz = velocity.shape
    planes = bx + 2 * HALO
    pairs = planes // 2
    groups = bz // 4
    tall = by + 8

    def kernel(g_ref, v_ref, bx_ref, ax_ref, by_ref, ay_ref, first_ref, last_ref):
        group = lane((tall, bz)) // 4
        for field, main in enumerate((g_ref, v_ref)):
            first = jnp.zeros((tall, bz), F32)
            last = jnp.zeros((tall, bz), F32)
            for p in range(planes):
                own = plane_of(main, bx_ref, ax_ref, field, p, bx)
                extra = rows_of(by_ref, ay_ref, field, p, pairs)
                plane = jnp.concatenate([own, extra], 0)
                turned = pltpu.roll(plane, 4 * p, 1) if p else plane
                first = jnp.where(group == p, turned, first)
                last = jnp.where(group == (p - 1) % groups, turned, last)
            first_ref[pl.ds(field * tall, tall)] = first
            last_ref[pl.ds(field * tall, tall)] = last

    edge = struct(2 * tall, bz)
    return pl.pallas_call(
        kernel,
        name="pack_z",
        compiler_params=PARAMS,
        out_shape=(edge, edge),
        in_specs=[VMEM] * 6,
        out_specs=(VMEM,) * 2,
    )(gradient, velocity, before_x, after_x, before_y, after_y)


def proximal(device, gradient, velocity, halos, sums, sizes):
    bx, by, bz = velocity.shape
    planes = bx + 2 * HALO
    pairs = planes // 2
    tall = by + 8
    wide = 2 * bz
    size_x, size_y, size_z = sizes
    cells = size_x * bx * size_y * by * size_z * bz

    def kernel(
        dev_ref,
        g_ref,
        v_ref,
        bx_ref,
        ax_ref,
        by_ref,
        ay_ref,
        bz_ref,
        az_ref,
        *refs,
    ):
        sum_refs = refs[: len(sums)]
        gradient_ref, model_ref, target, current, extra = refs[len(sums) : len(sums) + 5]
        dual_x, dual_y, dual_z, model, sems = refs[len(sums) + 5 :]
        gradient_copy = pltpu.make_async_copy(g_ref, gradient_ref, sems.at[0])
        gradient_copy.start()
        dev = dev_ref[0]
        pos_z = dev % size_z
        pos_y = (dev // size_z) % size_y
        pos_x = dev // (size_z * size_y)

        total = sum_refs[0][0:1]
        for ref in sum_refs[1:]:
            total = total + ref[0:1]
        total = jnp.sum(total, axis=1, keepdims=True)
        scale = step_length * lax.rsqrt(total / cells + 1.0)
        scale = jnp.broadcast_to(scale, (1, bz))

        side_lane = lane((tall, bz)) < bz // 2
        before_z = bz_ref[pl.ds(tall, tall)] - scale * bz_ref[pl.ds(0, tall)]
        after_z = az_ref[pl.ds(tall, tall)] - scale * az_ref[pl.ds(0, tall)]
        for p in range(planes):
            own = plane_of(v_ref, bx_ref, ax_ref, 1, p, bx) - scale * plane_of(
                g_ref, bx_ref, ax_ref, 0, p, bx
            )
            rows = rows_of(by_ref, ay_ref, 1, p, pairs) - scale * rows_of(
                by_ref, ay_ref, 0, p, pairs
            )
            back = (bz - 4 * p) % bz
            after = pltpu.roll(after_z, back, 1) if back else after_z
            before = pltpu.roll(before_z, back, 1) if back else before_z
            target[p, pl.ds(0, by), pl.ds(0, bz)] = own
            target[p, pl.ds(by, 8), pl.ds(0, bz)] = rows
            target[p, :, pl.ds(bz, bz)] = jnp.where(side_lane, after, before)

        def factor(index, limit):
            return jnp.where((index >= 0) & (index < limit - 1), dual_step, 0.0).astype(F32)

        row = sublane((tall, 1))
        row = jnp.where(row < by + 4, row, row - tall) + pos_y * by
        factor_y = factor(row, size_y * by)
        col = lane((1, wide))
        col = jnp.where(col < bz + bz // 2, col, col - wide) + pos_z * bz
        factor_z = factor(col, size_z * bz)
        shrink = 1.0 / (1.0 + primal_step)
        gain = primal_step / (1.0 + primal_step)

        for iteration in range(ITERS):
            first = iteration == 0
            final = iteration == ITERS - 1
            here_ref = target if first else extra
            ahead = here_ref[iteration]
            before_x = None
            for p in range(iteration, planes - 1 - iteration):
                here = ahead
                ahead = here_ref[p + 1]
                index = pos_x * bx + (p - HALO)
                factor_x = factor(index, size_x * bx)
                dx = factor_x * (ahead - here)
                dy = factor_y * (pltpu.roll(here, tall - 1, 0) - here)
                dz = factor_z * (pltpu.roll(here, wide - 1, 1) - here)
                if not first:
                    dx = dual_x[p] + dx
                    dy = dual_y[p] + dy
                    dz = dual_z[p] + dz
                norm = dx * dx + dy * dy + dz * dz
                ratio = jnp.minimum(1.0, tv_weight * lax.rsqrt(norm))
                dx = dx * ratio
                dy = dy * ratio
                dz = dz * ratio
                if not final:
                    dual_x[p] = dx
                    dual_y[p] = dy
                    dual_z[p] = dz
                if p > iteration:
                    if final:
                        spread = dx[:by, :bz] - before_x
                        spread += dy[:by, :bz] - pltpu.roll(dy[:, :bz], 1, 0)[:by]
                        spread += dz[:by, :bz] - pltpu.roll(dz[:by], 1, 1)[:, :bz]
                        goal = target[p, pl.ds(0, by), pl.ds(0, bz)]
                        old = current[p, pl.ds(0, by), pl.ds(0, bz)]
                        model[p - HALO] = shrink * old + gain * (spread + goal)
                    else:
                        spread = dx - before_x
                        spread += dy - pltpu.roll(dy, 1, 0)
                        spread += dz - pltpu.roll(dz, 1, 1)
                        if first:
                            new = here + gain * spread
                            old = here
                        else:
                            old = current[p]
                            new = shrink * old + gain * (spread + target[p])
                        current[p] = new
                        extra[p] = 2.0 * new - old
                before_x = dx[:by, :bz] if final else dx
        model_copy = pltpu.make_async_copy(model, model_ref, sems.at[1])
        model_copy.start()
        gradient_copy.wait()
        model_copy.wait()

    field = pltpu.VMEM((planes, tall, wide), F32)
    return pl.pallas_call(
        kernel,
        name="proximal",
        compiler_params=PARAMS,
        out_shape=(struct(bx, by, bz),) * 2,
        in_specs=[SMEM] + [VMEM] * (8 + len(sums)),
        out_specs=(HBM,) * 2,
        scratch_shapes=[field] * 6 + [pltpu.VMEM((bx, by, bz), F32), pltpu.SemaphoreType.DMA((2,))],
    )(device, gradient, velocity, *halos, *sums)


def shards(partials, code_bits, group_map, velocity):
    sizes = tuple(lax.axis_size(axis) for axis in (GX, GY, "gz"))
    base = (lax.axis_index(GX) * partials.shape[0]).astype(jnp.int32).reshape(1)
    device = lax.axis_index(ALL).astype(jnp.int32).reshape(1)

    local = presum(partials, code_bits, group_map, base, 8)
    parts = lax.all_to_all(local, GX, split_axis=0, concat_axis=0, tiled=True)
    gradient, first_x, last_x, squares = reduce_pack(parts, velocity, sizes[0])

    after_x = shift(first_x, GX, -1)
    before_x = shift(last_x, GX, 1)
    table = jnp.broadcast_to(squares[:1][None], (sizes[0] * sizes[2], 1, squares.shape[1]))
    table = lax.all_to_all(table, XZ, split_axis=0, concat_axis=0, tiled=True)

    first_y, last_y = pack_y(gradient, velocity, before_x, after_x)
    after_y = shift(first_y, GY, -1)
    before_y = shift(last_y, GY, 1)

    column = jnp.broadcast_to(jnp.sum(table, axis=0), squares.shape)
    for d in range(1, lax.axis_size(GY[1])):
        column = column + turn(column, GY[1], d)
    columns = [turn(column, GY[0], d) for d in range(1, lax.axis_size(GY[0]))]

    first_z, last_z = pack_z(gradient, velocity, before_x, after_x, before_y, after_y)
    after_z = shift(first_z, "gz", -1)
    before_z = shift(last_z, "gz", 1)

    return proximal(
        device,
        gradient,
        velocity,
        (before_x, after_x, before_y, after_y, before_z, after_z),
        [column, *columns],
        sizes,
    )


def solution(mesh):
    torus = Mesh(
        mesh.devices.reshape(4, 2, 4, 2, mesh.shape["gz"]), ("gx_0", "gx_1", "gy_0", "gy_1", "gz")
    )
    placed = (P(GX, None, GY, "gz"), P(), P(), P(GX, GY, "gz"))
    return jax.shard_map(
        shards,
        mesh=torus,
        in_specs=placed,
        out_specs=(P(GX, GY, "gz"), P(GX, GY, "gz")),
        check_vma=False,
    )
```

```python
import jax
import jax.numpy as jnp
from jax import lax
from jax.experimental import pallas as pl
from jax.experimental.pallas import tpu as pltpu
from jax.sharding import Mesh
from jax.sharding import PartitionSpec as P

ITERS = 3
HALO = ITERS
GX = ("gx_0", "gx_1")
GY = ("gy_0", "gy_1")
ALL = GX + GY + ("gz",)
XZ = GX + ("gz",)

step_length = 0.5
tv_weight = 0.2
dual_step = 0.28
primal_step = 0.28

VMEM = pl.BlockSpec(memory_space=pltpu.VMEM)
SMEM = pl.BlockSpec(memory_space=pltpu.SMEM)
HBM = pl.BlockSpec(memory_space=pltpu.HBM)
PARAMS = pltpu.CompilerParams(vmem_limit_bytes=16 * 1024 * 1024)
F32 = jnp.float32


def shift(block, axis, distance):
    size = lax.axis_size(axis)
    return lax.ppermute(block, axis, [(i, (i + distance) % size) for i in range(size)])


def struct(*shape):
    return jax.ShapeDtypeStruct(shape, F32)


def in_hbm(array):
    return pltpu.with_memory_space_constraint(array, pltpu.HBM)


def presum(partials, code_bits, group_map, base, chunks):
    slots, nx, by, bz = partials.shape
    rows = nx // chunks

    def kernel(base_ref, map_hbm, bits_hbm, part_ref, out_ref, buf, map_ref, bits_ref, sems):
        map_copy = pltpu.make_async_copy(map_hbm, map_ref, sems.at[chunks])
        bits_copy = pltpu.make_async_copy(bits_hbm, bits_ref, sems.at[chunks + 1])
        map_copy.start()
        bits_copy.start()

        def copy(c):
            part = pl.ds(c * rows, rows)
            return pltpu.make_async_copy(part_ref.at[:, part], buf.at[:, part], sems.at[c])

        for c in range(chunks):
            copy(c).start()
        map_copy.wait()
        bits_copy.wait()
        groups = [map_ref[base_ref[0] + s] for s in range(slots)]
        for c in range(chunks):
            copy(c).wait()

            def row(i, carry):
                x = c * rows + i
                total = None
                for s in range(slots):
                    sign = (2 * bits_ref[groups[s], x] - 1).astype(F32)
                    term = sign * buf[s, x]
                    total = term if total is None else total + term
                out_ref[x] = total
                return carry

            lax.fori_loop(0, rows, row, 0, unroll=4)

    return pl.pallas_call(
        kernel,
        name="presum",
        compiler_params=PARAMS,
        out_shape=struct(nx, by, bz),
        in_specs=[SMEM, HBM, HBM, HBM],
        out_specs=VMEM,
        scratch_shapes=[
            pltpu.VMEM(partials.shape, F32),
            pltpu.SMEM(group_map.shape, jnp.int32),
            pltpu.SMEM(code_bits.shape, jnp.int32),
            pltpu.SemaphoreType.DMA((chunks + 2,)),
        ],
    )(base, in_hbm(group_map), in_hbm(code_bits), in_hbm(partials))


def reduce_pack(parts, velocity, members):
    bx, by, bz = velocity.shape

    def kernel(part_ref, v_ref, g_ref, first_ref, last_ref, square_ref):
        squares = jnp.zeros((by, bz), F32)
        for i in range(bx):
            total = part_ref[i]
            for m in range(1, members):
                total = total + part_ref[m * bx + i]
            g_ref[i] = total
            squares = squares + total * total
            if i < HALO:
                first_ref[i] = total
                first_ref[HALO + i] = v_ref[i]
            if i >= bx - HALO:
                last_ref[i - bx + HALO] = total
                last_ref[i - bx + 2 * HALO] = v_ref[i]
        square_ref[...] = jnp.broadcast_to(jnp.sum(squares, axis=0, keepdims=True), (8, bz))

    edge = struct(2 * HALO, by, bz)
    return pl.pallas_call(
        kernel,
        name="reduce_pack",
        compiler_params=PARAMS,
        out_shape=(struct(bx, by, bz), edge, edge, struct(8, bz)),
        in_specs=[VMEM, VMEM],
        out_specs=(VMEM,) * 4,
    )(parts, velocity)


def plane_of(main_ref, before_ref, after_ref, field, p, bx):
    if p < HALO:
        return before_ref[field * HALO + p]
    if p < HALO + bx:
        return main_ref[p - HALO]
    return after_ref[field * HALO + p - HALO - bx]


def sublane(shape):
    return lax.broadcasted_iota(jnp.int32, shape, len(shape) - 2)


def lane(shape):
    return lax.broadcasted_iota(jnp.int32, shape, len(shape) - 1)


def pack_y(gradient, velocity, before_x, after_x):
    bx, by, bz = velocity.shape
    pairs = (bx + 2 * HALO) // 2

    def kernel(g_ref, v_ref, before_ref, after_ref, first_ref, last_ref):
        low = sublane((8, bz)) < 4
        for field, main in enumerate((g_ref, v_ref)):
            for q in range(pairs):
                even = plane_of(main, before_ref, after_ref, field, 2 * q, bx)
                odd = plane_of(main, before_ref, after_ref, field, 2 * q + 1, bx)
                first_ref[field * pairs + q] = jnp.where(low, even[:8], pltpu.roll(odd[:8], 4, 0))
                last_ref[field * pairs + q] = jnp.where(
                    low, pltpu.roll(even[by - 8 :], 4, 0), odd[by - 8 :]
                )

    edge = struct(2 * pairs, 8, bz)
    return pl.pallas_call(
        kernel,
        name="pack_y",
        compiler_params=PARAMS,
        out_shape=(edge, edge),
        in_specs=[VMEM] * 4,
        out_specs=(VMEM,) * 2,
    )(gradient, velocity, before_x, after_x)


def rows_of(before_ref, after_ref, field, p, pairs):
    after = after_ref[field * pairs + p // 2]
    before = before_ref[field * pairs + p // 2]
    low = sublane(after.shape) < 4
    if p % 2 == 0:
        return jnp.where(low, after, pltpu.roll(before, 4, 0))
    return jnp.where(low, pltpu.roll(after, 4, 0), before)


def pack_z(gradient, velocity, before_x, after_x, before_y, after_y):
    bx, by, bz = velocity.shape
    planes = bx + 2 * HALO
    pairs = planes // 2
    groups = bz // 4
    tall = by + 8

    def kernel(g_ref, v_ref, bx_ref, ax_ref, by_ref, ay_ref, first_ref, last_ref):
        group = lane((tall, bz)) // 4
        for field, main in enumerate((g_ref, v_ref)):
            first = jnp.zeros((tall, bz), F32)
            last = jnp.zeros((tall, bz), F32)
            for p in range(planes):
                own = plane_of(main, bx_ref, ax_ref, field, p, bx)
                extra = rows_of(by_ref, ay_ref, field, p, pairs)
                plane = jnp.concatenate([own, extra], 0)
                turned = pltpu.roll(plane, 4 * p, 1) if p else plane
                first = jnp.where(group == p, turned, first)
                last = jnp.where(group == (p - 1) % groups, turned, last)
            first_ref[pl.ds(field * tall, tall)] = first
            last_ref[pl.ds(field * tall, tall)] = last

    edge = struct(2 * tall, bz)
    return pl.pallas_call(
        kernel,
        name="pack_z",
        compiler_params=PARAMS,
        out_shape=(edge, edge),
        in_specs=[VMEM] * 6,
        out_specs=(VMEM,) * 2,
    )(gradient, velocity, before_x, after_x, before_y, after_y)


def proximal(device, gradient, velocity, halos, sums, sizes):
    bx, by, bz = velocity.shape
    planes = bx + 2 * HALO
    pairs = planes // 2
    tall = by + 8
    wide = 2 * bz
    size_x, size_y, size_z = sizes
    cells = size_x * bx * size_y * by * size_z * bz

    def kernel(
        dev_ref,
        g_ref,
        v_ref,
        bx_ref,
        ax_ref,
        by_ref,
        ay_ref,
        bz_ref,
        az_ref,
        *refs,
    ):
        sum_refs = refs[: len(sums)]
        gradient_ref, model_ref, target, current, extra = refs[len(sums) : len(sums) + 5]
        dual_x, dual_y, dual_z, model, sems = refs[len(sums) + 5 :]
        gradient_copy = pltpu.make_async_copy(g_ref, gradient_ref, sems.at[0])
        gradient_copy.start()
        dev = dev_ref[0]
        pos_z = dev % size_z
        pos_y = (dev // size_z) % size_y
        pos_x = dev // (size_z * size_y)

        total = sum_refs[0][0:1]
        for ref in sum_refs[1:]:
            total = total + ref[0:1]
        total = jnp.sum(total, axis=1, keepdims=True)
        scale = step_length * lax.rsqrt(total / cells + 1.0)
        scale = jnp.broadcast_to(scale, (1, bz))

        side_lane = lane((tall, bz)) < bz // 2
        before_z = bz_ref[pl.ds(tall, tall)] - scale * bz_ref[pl.ds(0, tall)]
        after_z = az_ref[pl.ds(tall, tall)] - scale * az_ref[pl.ds(0, tall)]
        for p in range(planes):
            own = plane_of(v_ref, bx_ref, ax_ref, 1, p, bx) - scale * plane_of(
                g_ref, bx_ref, ax_ref, 0, p, bx
            )
            rows = rows_of(by_ref, ay_ref, 1, p, pairs) - scale * rows_of(
                by_ref, ay_ref, 0, p, pairs
            )
            back = (bz - 4 * p) % bz
            after = pltpu.roll(after_z, back, 1) if back else after_z
            before = pltpu.roll(before_z, back, 1) if back else before_z
            target[p, pl.ds(0, by), pl.ds(0, bz)] = own
            target[p, pl.ds(by, 8), pl.ds(0, bz)] = rows
            target[p, :, pl.ds(bz, bz)] = jnp.where(side_lane, after, before)

        def factor(index, limit):
            return jnp.where((index >= 0) & (index < limit - 1), dual_step, 0.0).astype(F32)

        row = sublane((tall, 1))
        row = jnp.where(row < by + 4, row, row - tall) + pos_y * by
        factor_y = factor(row, size_y * by)
        col = lane((1, wide))
        col = jnp.where(col < bz + bz // 2, col, col - wide) + pos_z * bz
        factor_z = factor(col, size_z * bz)
        shrink = 1.0 / (1.0 + primal_step)
        gain = primal_step / (1.0 + primal_step)

        for iteration in range(ITERS):
            first = iteration == 0
            final = iteration == ITERS - 1
            here_ref = target if first else extra
            ahead = here_ref[iteration]
            before_x = None
            for p in range(iteration, planes - 1 - iteration):
                here = ahead
                ahead = here_ref[p + 1]
                index = pos_x * bx + (p - HALO)
                factor_x = factor(index, size_x * bx)
                dx = factor_x * (ahead - here)
                dy = factor_y * (pltpu.roll(here, tall - 1, 0) - here)
                dz = factor_z * (pltpu.roll(here, wide - 1, 1) - here)
                if not first:
                    dx = dual_x[p] + dx
                    dy = dual_y[p] + dy
                    dz = dual_z[p] + dz
                norm = dx * dx + dy * dy + dz * dz
                ratio = jnp.minimum(1.0, tv_weight * lax.rsqrt(norm))
                dx = dx * ratio
                dy = dy * ratio
                dz = dz * ratio
                if not final:
                    dual_x[p] = dx
                    dual_y[p] = dy
                    dual_z[p] = dz
                if p > iteration:
                    if final:
                        spread = dx[:by, :bz] - before_x
                        spread += dy[:by, :bz] - pltpu.roll(dy[:, :bz], 1, 0)[:by]
                        spread += dz[:by, :bz] - pltpu.roll(dz[:by], 1, 1)[:, :bz]
                        goal = target[p, pl.ds(0, by), pl.ds(0, bz)]
                        old = current[p, pl.ds(0, by), pl.ds(0, bz)]
                        model[p - HALO] = shrink * old + gain * (spread + goal)
                    else:
                        spread = dx - before_x
                        spread += dy - pltpu.roll(dy, 1, 0)
                        spread += dz - pltpu.roll(dz, 1, 1)
                        if first:
                            new = here + gain * spread
                            old = here
                        else:
                            old = current[p]
                            new = shrink * old + gain * (spread + target[p])
                        current[p] = new
                        extra[p] = 2.0 * new - old
                before_x = dx[:by, :bz] if final else dx
        model_copy = pltpu.make_async_copy(model, model_ref, sems.at[1])
        model_copy.start()
        gradient_copy.wait()
        model_copy.wait()

    field = pltpu.VMEM((planes, tall, wide), F32)
    return pl.pallas_call(
        kernel,
        name="proximal",
        compiler_params=PARAMS,
        out_shape=(struct(bx, by, bz),) * 2,
        in_specs=[SMEM] + [VMEM] * (8 + len(sums)),
        out_specs=(HBM,) * 2,
        scratch_shapes=[field] * 6 + [pltpu.VMEM((bx, by, bz), F32), pltpu.SemaphoreType.DMA((2,))],
    )(device, gradient, velocity, *halos, *sums)


def shards(partials, code_bits, group_map, velocity):
    sizes = tuple(lax.axis_size(axis) for axis in (GX, GY, "gz"))
    base = (lax.axis_index(GX) * partials.shape[0]).astype(jnp.int32).reshape(1)
    device = lax.axis_index(ALL).astype(jnp.int32).reshape(1)

    local = presum(partials, code_bits, group_map, base, 8)
    parts = lax.all_to_all(local, GX, split_axis=0, concat_axis=0, tiled=True)
    gradient, first_x, last_x, squares = reduce_pack(parts, velocity, sizes[0])

    after_x = shift(first_x, GX, -1)
    before_x = shift(last_x, GX, 1)
    table = jnp.broadcast_to(squares[:1][None], (sizes[0] * sizes[2], 1, squares.shape[1]))
    table = lax.all_to_all(table, XZ, split_axis=0, concat_axis=0, tiled=True)

    first_y, last_y = pack_y(gradient, velocity, before_x, after_x)
    after_y = shift(first_y, GY, -1)
    before_y = shift(last_y, GY, 1)

    column = jnp.broadcast_to(jnp.sum(table, axis=0), squares.shape)
    for d in range(1, lax.axis_size(GY[1])):
        column = column + shift(column, GY[1], d)
    columns = [shift(column, GY[0], d) for d in range(1, lax.axis_size(GY[0]))]

    first_z, last_z = pack_z(gradient, velocity, before_x, after_x, before_y, after_y)
    after_z = shift(first_z, "gz", -1)
    before_z = shift(last_z, "gz", 1)

    return proximal(
        device,
        gradient,
        velocity,
        (before_x, after_x, before_y, after_y, before_z, after_z),
        [column, *columns],
        sizes,
    )


def solution(mesh):
    torus = Mesh(
        mesh.devices.reshape(4, 2, 4, 2, mesh.shape["gz"]), ("gx_0", "gx_1", "gy_0", "gy_1", "gz")
    )
    placed = (P(GX, None, GY, "gz"), P(), P(), P(GX, GY, "gz"))
    return jax.shard_map(
        shards,
        mesh=torus,
        in_specs=placed,
        out_specs=(P(GX, GY, "gz"), P(GX, GY, "gz")),
        check_vma=False,
    )
```

```python
import jax
import jax.numpy as jnp
from jax import lax
from jax.experimental import pallas as pl
from jax.experimental.pallas import tpu as pltpu
from jax.sharding import Mesh
from jax.sharding import PartitionSpec as P

ITERS = 3
HALO = ITERS
GX = ("gx_0", "gx_1")
GY = ("gy_0", "gy_1")
ALL = GX + GY + ("gz",)

step_length = 0.5
tv_weight = 0.2
dual_step = 0.28
primal_step = 0.28

VMEM = pl.BlockSpec(memory_space=pltpu.VMEM)
SMEM = pl.BlockSpec(memory_space=pltpu.SMEM)
HBM = pl.BlockSpec(memory_space=pltpu.HBM)
PARAMS = pltpu.CompilerParams(vmem_limit_bytes=16 * 1024 * 1024)
F32 = jnp.float32


def shift(block, axis, distance):
    size = lax.axis_size(axis)
    return lax.ppermute(block, axis, [(i, (i + distance) % size) for i in range(size)])


def struct(*shape):
    return jax.ShapeDtypeStruct(shape, F32)


def in_hbm(array):
    return pltpu.with_memory_space_constraint(array, pltpu.HBM)


def presum(partials, code_bits, group_map, base, blocks, segments):
    slots, nx, by, bz = partials.shape
    length = nx // blocks
    span = sum(count for _, count in segments)
    pieces = len(segments)

    def kernel(base_ref, map_hbm, bits_hbm, part_ref, out_ref, buf, map_ref, bits_ref, sems):
        map_copy = pltpu.make_async_copy(map_hbm, map_ref, sems.at[blocks * pieces])
        bits_copy = pltpu.make_async_copy(bits_hbm, bits_ref, sems.at[blocks * pieces + 1])
        map_copy.start()
        bits_copy.start()

        def copy(d, k):
            first, count = segments[k]
            at = sum(c for _, c in segments[:k])
            return pltpu.make_async_copy(
                part_ref.at[:, pl.ds(d * length + first, count)],
                buf.at[:, pl.ds(d * span + at, count)],
                sems.at[d * pieces + k],
            )

        for d in range(blocks):
            for k in range(pieces):
                copy(d, k).start()
        map_copy.wait()
        bits_copy.wait()
        groups = [map_ref[base_ref[0] + s] for s in range(slots)]

        def block(d, carry):
            row = d * span
            for k, (first, count) in enumerate(segments):
                copy(d, k).wait()
                for i in range(count):
                    total = None
                    for s in range(slots):
                        bit = bits_ref[groups[s], d * length + first + i]
                        term = (2 * bit - 1).astype(F32) * buf[s, row]
                        total = term if total is None else total + term
                    out_ref[row] = total
                    row = row + 1
            return carry

        lax.fori_loop(0, blocks, block, 0)

    return pl.pallas_call(
        kernel,
        compiler_params=PARAMS,
        out_shape=struct(blocks * span, by, bz),
        in_specs=[SMEM, HBM, HBM, HBM],
        out_specs=VMEM,
        scratch_shapes=[
            pltpu.VMEM((slots, blocks * span, by, bz), F32),
            pltpu.SMEM(group_map.shape, jnp.int32),
            pltpu.SMEM(code_bits.shape, jnp.int32),
            pltpu.SemaphoreType.DMA((blocks * pieces + 2,)),
        ],
    )(base, in_hbm(group_map), in_hbm(code_bits), in_hbm(partials))


def member_sum(part_ref, i, span, members):
    total = part_ref[i]
    for m in range(1, members):
        total = total + part_ref[m * span + i]
    return total


def reduce_edges(parts, velocity, members):
    bx, by, bz = velocity.shape

    def kernel(part_ref, v_ref, first_ref, last_ref):
        for i in range(HALO):
            first_ref[i] = member_sum(part_ref, i, 2 * HALO, members)
            first_ref[HALO + i] = v_ref[i]
            last_ref[i] = member_sum(part_ref, HALO + i, 2 * HALO, members)
            last_ref[HALO + i] = v_ref[bx - HALO + i]

    edge = struct(2 * HALO, by, bz)
    return pl.pallas_call(
        kernel,
        name="reduce_edges",
        compiler_params=PARAMS,
        out_shape=(edge, edge),
        in_specs=[VMEM, VMEM],
        out_specs=(VMEM,) * 2,
    )(parts, velocity)


def reduce_rest(parts, first_x, last_x, members):
    _, by, bz = parts.shape
    inner = parts.shape[0] // members
    bx = inner + 2 * HALO

    def kernel(part_ref, first_ref, last_ref, g_ref, square_ref):
        squares = jnp.zeros((by, bz), F32)
        for i in range(bx):
            if i < HALO:
                total = first_ref[i]
            elif i < bx - HALO:
                total = member_sum(part_ref, i - HALO, inner, members)
            else:
                total = last_ref[i - bx + HALO]
            g_ref[i] = total
            squares = squares + total * total
        square_ref[...] = jnp.broadcast_to(jnp.sum(squares, axis=0, keepdims=True), (8, bz))

    return pl.pallas_call(
        kernel,
        name="reduce_rest",
        compiler_params=PARAMS,
        out_shape=(struct(bx, by, bz), struct(8, bz)),
        in_specs=[VMEM] * 3,
        out_specs=(VMEM,) * 2,
    )(parts, first_x, last_x)


def plane_of(main_ref, before_ref, after_ref, field, p, bx):
    if p < HALO:
        return before_ref[field * HALO + p]
    if p < HALO + bx:
        return main_ref[p - HALO]
    return after_ref[field * HALO + p - HALO - bx]


def sublane(shape):
    return lax.broadcasted_iota(jnp.int32, shape, len(shape) - 2)


def lane(shape):
    return lax.broadcasted_iota(jnp.int32, shape, len(shape) - 1)


def pack_y(gradient, velocity, before_x, after_x):
    bx, by, bz = velocity.shape
    pairs = (bx + 2 * HALO) // 2

    def kernel(g_ref, v_ref, before_ref, after_ref, first_ref, last_ref):
        low = sublane((8, bz)) < 4
        for field, main in enumerate((g_ref, v_ref)):
            for q in range(pairs):
                even = plane_of(main, before_ref, after_ref, field, 2 * q, bx)
                odd = plane_of(main, before_ref, after_ref, field, 2 * q + 1, bx)
                first_ref[field * pairs + q] = jnp.where(low, even[:8], pltpu.roll(odd[:8], 4, 0))
                last_ref[field * pairs + q] = jnp.where(
                    low, pltpu.roll(even[by - 8 :], 4, 0), odd[by - 8 :]
                )

    edge = struct(2 * pairs, 8, bz)
    return pl.pallas_call(
        kernel,
        name="pack_y",
        compiler_params=PARAMS,
        out_shape=(edge, edge),
        in_specs=[VMEM] * 4,
        out_specs=(VMEM,) * 2,
    )(gradient, velocity, before_x, after_x)


def rows_of(before_ref, after_ref, field, p, pairs):
    after = after_ref[field * pairs + p // 2]
    before = before_ref[field * pairs + p // 2]
    low = sublane(after.shape) < 4
    if p % 2 == 0:
        return jnp.where(low, after, pltpu.roll(before, 4, 0))
    return jnp.where(low, pltpu.roll(after, 4, 0), before)


def pack_z(gradient, velocity, before_x, after_x, before_y, after_y):
    bx, by, bz = velocity.shape
    planes = bx + 2 * HALO
    pairs = planes // 2
    groups = bz // 4
    tall = by + 8

    def kernel(g_ref, v_ref, bx_ref, ax_ref, by_ref, ay_ref, first_ref, last_ref):
        group = lane((tall, bz)) // 4
        for field, main in enumerate((g_ref, v_ref)):
            first = jnp.zeros((tall, bz), F32)
            last = jnp.zeros((tall, bz), F32)
            for p in range(planes):
                own = plane_of(main, bx_ref, ax_ref, field, p, bx)
                extra = rows_of(by_ref, ay_ref, field, p, pairs)
                plane = jnp.concatenate([own, extra], 0)
                turned = pltpu.roll(plane, 4 * p, 1) if p else plane
                first = jnp.where(group == p, turned, first)
                last = jnp.where(group == (p - 1) % groups, turned, last)
            first_ref[pl.ds(field * tall, tall)] = first
            last_ref[pl.ds(field * tall, tall)] = last

    edge = struct(2 * tall, bz)
    return pl.pallas_call(
        kernel,
        name="pack_z",
        compiler_params=PARAMS,
        out_shape=(edge, edge),
        in_specs=[VMEM] * 6,
        out_specs=(VMEM,) * 2,
    )(gradient, velocity, before_x, after_x, before_y, after_y)


def proximal(device, gradient, velocity, halos, squares, sizes):
    bx, by, bz = velocity.shape
    planes = bx + 2 * HALO
    pairs = planes // 2
    tall = by + 8
    wide = 2 * bz
    size_x, size_y, size_z = sizes
    cells = size_x * bx * size_y * by * size_z * bz

    def kernel(
        dev_ref,
        g_ref,
        v_ref,
        bx_ref,
        ax_ref,
        by_ref,
        ay_ref,
        bz_ref,
        az_ref,
        sq_ref,
        gradient_ref,
        model_ref,
        target,
        current,
        extra,
        dual_x,
        dual_y,
        dual_z,
        model,
        sems,
    ):
        gradient_copy = pltpu.make_async_copy(g_ref, gradient_ref, sems.at[0])
        gradient_copy.start()
        dev = dev_ref[0]
        pos_z = dev % size_z
        pos_y = (dev // size_z) % size_y
        pos_x = dev // (size_z * size_y)

        total = jnp.sum(jnp.sum(sq_ref[...], axis=0), axis=1, keepdims=True)
        scale = step_length * lax.rsqrt(total / cells + 1.0)
        scale = jnp.broadcast_to(scale, (1, bz))

        side_lane = lane((tall, bz)) < bz // 2
        before_z = bz_ref[pl.ds(tall, tall)] - scale * bz_ref[pl.ds(0, tall)]
        after_z = az_ref[pl.ds(tall, tall)] - scale * az_ref[pl.ds(0, tall)]
        for p in range(planes):
            own = plane_of(v_ref, bx_ref, ax_ref, 1, p, bx) - scale * plane_of(
                g_ref, bx_ref, ax_ref, 0, p, bx
            )
            rows = rows_of(by_ref, ay_ref, 1, p, pairs) - scale * rows_of(
                by_ref, ay_ref, 0, p, pairs
            )
            back = (bz - 4 * p) % bz
            after = pltpu.roll(after_z, back, 1) if back else after_z
            before = pltpu.roll(before_z, back, 1) if back else before_z
            target[p, pl.ds(0, by), pl.ds(0, bz)] = own
            target[p, pl.ds(by, 8), pl.ds(0, bz)] = rows
            target[p, :, pl.ds(bz, bz)] = jnp.where(side_lane, after, before)

        def factor(index, limit):
            return jnp.where((index >= 0) & (index < limit - 1), dual_step, 0.0).astype(F32)

        row = sublane((tall, 1))
        row = jnp.where(row < by + 4, row, row - tall) + pos_y * by
        factor_y = factor(row, size_y * by)
        col = lane((1, wide))
        col = jnp.where(col < bz + bz // 2, col, col - wide) + pos_z * bz
        factor_z = factor(col, size_z * bz)
        shrink = 1.0 / (1.0 + primal_step)
        gain = primal_step / (1.0 + primal_step)

        for iteration in range(ITERS):
            first = iteration == 0
            final = iteration == ITERS - 1
            here_ref = target if first else extra
            ahead = here_ref[iteration]
            before_x = None
            for p in range(iteration, planes - 1 - iteration):
                here = ahead
                ahead = here_ref[p + 1]
                index = pos_x * bx + (p - HALO)
                factor_x = factor(index, size_x * bx)
                dx = factor_x * (ahead - here)
                dy = factor_y * (pltpu.roll(here, tall - 1, 0) - here)
                dz = factor_z * (pltpu.roll(here, wide - 1, 1) - here)
                if not first:
                    dx = dual_x[p] + dx
                    dy = dual_y[p] + dy
                    dz = dual_z[p] + dz
                norm = dx * dx + dy * dy + dz * dz
                ratio = jnp.minimum(1.0, tv_weight * lax.rsqrt(norm))
                dx = dx * ratio
                dy = dy * ratio
                dz = dz * ratio
                if not final:
                    dual_x[p] = dx
                    dual_y[p] = dy
                    dual_z[p] = dz
                if p > iteration:
                    if final:
                        spread = dx[:by, :bz] - before_x
                        spread += dy[:by, :bz] - pltpu.roll(dy[:, :bz], 1, 0)[:by]
                        spread += dz[:by, :bz] - pltpu.roll(dz[:by], 1, 1)[:, :bz]
                        goal = target[p, pl.ds(0, by), pl.ds(0, bz)]
                        old = current[p, pl.ds(0, by), pl.ds(0, bz)]
                        model[p - HALO] = shrink * old + gain * (spread + goal)
                    else:
                        spread = dx - before_x
                        spread += dy - pltpu.roll(dy, 1, 0)
                        spread += dz - pltpu.roll(dz, 1, 1)
                        if first:
                            new = here + gain * spread
                            old = here
                        else:
                            old = current[p]
                            new = shrink * old + gain * (spread + target[p])
                        current[p] = new
                        extra[p] = 2.0 * new - old
                before_x = dx[:by, :bz] if final else dx
        model_copy = pltpu.make_async_copy(model, model_ref, sems.at[1])
        model_copy.start()
        gradient_copy.wait()
        model_copy.wait()

    field = pltpu.VMEM((planes, tall, wide), F32)
    return pl.pallas_call(
        kernel,
        name="proximal",
        compiler_params=PARAMS,
        out_shape=(struct(bx, by, bz),) * 2,
        in_specs=[SMEM] + [VMEM] * 9,
        out_specs=(HBM,) * 2,
        scratch_shapes=[field] * 6 + [pltpu.VMEM((bx, by, bz), F32), pltpu.SemaphoreType.DMA((2,))],
    )(device, gradient, velocity, *halos, squares)


def shards(partials, code_bits, group_map, velocity):
    bx, _, bz = velocity.shape
    size_x, size_y, size_z = (lax.axis_size(axis) for axis in (GX, GY, "gz"))
    base = (lax.axis_index(GX) * partials.shape[0]).astype(jnp.int32).reshape(1)
    device = lax.axis_index(ALL).astype(jnp.int32).reshape(1)

    bx = velocity.shape[0]
    edge_layers = ((0, HALO), (bx - HALO, HALO))
    inner_layers = ((HALO, bx - 2 * HALO),)
    outer = presum(partials, code_bits, group_map, base, size_x, edge_layers)
    outer = lax.all_to_all(outer, GX, split_axis=0, concat_axis=0, tiled=True)
    inner = presum(partials, code_bits, group_map, base, size_x, inner_layers)
    inner = lax.all_to_all(inner, GX, split_axis=0, concat_axis=0, tiled=True)
    first_x, last_x = reduce_edges(outer, velocity, size_x)
    after_x = shift(first_x, GX, -1)
    before_x = shift(last_x, GX, 1)
    gradient, squares = reduce_rest(inner, first_x, last_x, size_x)
    first_y, last_y = pack_y(gradient, velocity, before_x, after_x)
    after_y = shift(first_y, GY, -1)
    before_y = shift(last_y, GY, 1)

    table = jnp.broadcast_to(squares[:1][None], (size_x * size_y * size_z, 1, bz))
    table = lax.all_to_all(table, ALL, split_axis=0, concat_axis=0, tiled=True)

    first_z, last_z = pack_z(gradient, velocity, before_x, after_x, before_y, after_y)
    after_z = shift(first_z, "gz", -1)
    before_z = shift(last_z, "gz", 1)

    return proximal(
        device,
        gradient,
        velocity,
        (before_x, after_x, before_y, after_y, before_z, after_z),
        table,
        (size_x, size_y, size_z),
    )


def solution(mesh):
    torus = Mesh(
        mesh.devices.reshape(4, 2, 4, 2, mesh.shape["gz"]), ("gx_0", "gx_1", "gy_0", "gy_1", "gz")
    )
    placed = (P(GX, None, GY, "gz"), P(), P(), P(GX, GY, "gz"))
    return jax.shard_map(
        shards,
        mesh=torus,
        in_specs=placed,
        out_specs=(P(GX, GY, "gz"), P(GX, GY, "gz")),
        check_vma=False,
    )
```

```python
import jax
import jax.numpy as jnp
from jax import lax
from jax.experimental import pallas as pl
from jax.experimental.pallas import tpu as pltpu
from jax.sharding import Mesh
from jax.sharding import PartitionSpec as P

ITERS = 3
HALO = ITERS
GX = ("gx_0", "gx_1")
GY = ("gy_0", "gy_1")
ALL = GX + GY + ("gz",)
XZ = GX + ("gz",)

step_length = 0.5
tv_weight = 0.2
dual_step = 0.28
primal_step = 0.28

VMEM = pl.BlockSpec(memory_space=pltpu.VMEM)
SMEM = pl.BlockSpec(memory_space=pltpu.SMEM)
HBM = pl.BlockSpec(memory_space=pltpu.HBM)
PARAMS = pltpu.CompilerParams(vmem_limit_bytes=16 * 1024 * 1024)
F32 = jnp.float32


def swap(blocks, axis):
    size = lax.axis_size(axis)
    pairs = [(i, i ^ 1) for i in range(size)]
    others = [(i, ((i + 1) ^ 1) - 1) for i in range(size)]
    others = [(i, j % size) for i, j in others]
    return lax.ppermute(blocks[0], axis, pairs), lax.ppermute(blocks[1], axis, others)


def struct(*shape):
    return jax.ShapeDtypeStruct(shape, F32)


def in_hbm(array):
    return pltpu.with_memory_space_constraint(array, pltpu.HBM)


def presum(device, partials, code_bits, group_map, sizes, chunks):
    slots, nx, by, bz = partials.shape
    rows = nx // chunks

    def kernel(dev_ref, map_hbm, bits_hbm, part_ref, out_ref, buf, map_ref, bits_ref, sems):
        map_copy = pltpu.make_async_copy(map_hbm, map_ref, sems.at[chunks])
        bits_copy = pltpu.make_async_copy(bits_hbm, bits_ref, sems.at[chunks + 1])
        map_copy.start()
        bits_copy.start()

        def copy(c):
            part = pl.ds(c * rows, rows)
            return pltpu.make_async_copy(part_ref.at[:, part], buf.at[:, part], sems.at[c])

        for c in range(chunks):
            copy(c).start()
        map_copy.wait()
        bits_copy.wait()
        base = position(dev_ref, sizes)[0] * slots
        groups = [map_ref[base + s] for s in range(slots)]
        for c in range(chunks):
            copy(c).wait()

            def row(i, carry):
                x = c * rows + i
                total = None
                for s in range(slots):
                    sign = (2 * bits_ref[groups[s], x] - 1).astype(F32)
                    term = sign * buf[s, x]
                    total = term if total is None else total + term
                out_ref[x] = total
                return carry

            lax.fori_loop(0, rows, row, 0, unroll=4)

    return pl.pallas_call(
        kernel,
        name="presum",
        compiler_params=PARAMS,
        out_shape=struct(nx, by, bz),
        in_specs=[SMEM, HBM, HBM, HBM],
        out_specs=VMEM,
        scratch_shapes=[
            pltpu.VMEM(partials.shape, F32),
            pltpu.SMEM(group_map.shape, jnp.int32),
            pltpu.SMEM(code_bits.shape, jnp.int32),
            pltpu.SemaphoreType.DMA((chunks + 2,)),
        ],
    )(device, in_hbm(group_map), in_hbm(code_bits), in_hbm(partials))


def position(dev_ref, sizes):
    _, size_y, size_z = sizes
    dev = dev_ref[0]
    return dev // (size_y * size_z), (dev // size_z) % size_y, dev % size_z


def is_even(index):
    return index % 2 == 0


def reduce_pack(device, parts, velocity, sizes):
    bx, by, bz = velocity.shape
    members = sizes[0]

    def kernel(dev_ref, part_ref, v_ref, g_ref, near_ref, other_ref, square_ref):
        even = is_even(position(dev_ref, sizes)[0])
        squares = jnp.zeros((by, bz), F32)
        for i in range(bx):
            total = part_ref[i]
            for m in range(1, members):
                total = total + part_ref[m * bx + i]
            g_ref[i] = total
            squares = squares + total * total
        for i in range(HALO):
            for k, ref in enumerate((g_ref, v_ref)):
                first, last = ref[i], ref[bx - HALO + i]
                near_ref[k * HALO + i] = jnp.where(even, last, first)
                other_ref[k * HALO + i] = jnp.where(even, first, last)
        square_ref[...] = jnp.broadcast_to(jnp.sum(squares, axis=0, keepdims=True), (8, bz))

    edge = struct(2 * HALO, by, bz)
    return pl.pallas_call(
        kernel,
        name="reduce_pack",
        compiler_params=PARAMS,
        out_shape=(struct(bx, by, bz), edge, edge, struct(8, bz)),
        in_specs=[SMEM, VMEM, VMEM],
        out_specs=(VMEM,) * 4,
    )(device, parts, velocity)


def plane_of(main_ref, near_ref, other_ref, even, field, p):
    bx = main_ref.shape[0]
    if p < HALO:
        at = field * HALO + p
        return jnp.where(even, other_ref[at], near_ref[at])
    if p < HALO + bx:
        return main_ref[p - HALO]
    at = field * HALO + p - HALO - bx
    return jnp.where(even, near_ref[at], other_ref[at])


def sublane(shape):
    return lax.broadcasted_iota(jnp.int32, shape, len(shape) - 2)


def lane(shape):
    return lax.broadcasted_iota(jnp.int32, shape, len(shape) - 1)


def pack_y(device, gradient, velocity, halo_x, sizes):
    bx, by, bz = velocity.shape
    pairs = (bx + 2 * HALO) // 2

    def kernel(dev_ref, g_ref, v_ref, nx_ref, ox_ref, near_ref, other_ref):
        even_x, even_y = (is_even(i) for i in position(dev_ref, sizes)[:2])
        low = sublane((8, bz)) < 4
        for field, main in enumerate((g_ref, v_ref)):
            for q in range(pairs):
                left = plane_of(main, nx_ref, ox_ref, even_x, field, 2 * q)
                right = plane_of(main, nx_ref, ox_ref, even_x, field, 2 * q + 1)
                first = jnp.where(low, left[:8], pltpu.roll(right[:8], 4, 0))
                last = jnp.where(low, pltpu.roll(left[by - 8 :], 4, 0), right[by - 8 :])
                near_ref[field * pairs + q] = jnp.where(even_y, last, first)
                other_ref[field * pairs + q] = jnp.where(even_y, first, last)

    edge = struct(2 * pairs, 8, bz)
    return pl.pallas_call(
        kernel,
        name="pack_y",
        compiler_params=PARAMS,
        out_shape=(edge, edge),
        in_specs=[SMEM] + [VMEM] * 4,
        out_specs=(VMEM,) * 2,
    )(device, gradient, velocity, *halo_x)


def rows_of(near_ref, other_ref, even, field, p, pairs):
    near = near_ref[field * pairs + p // 2]
    other = other_ref[field * pairs + p // 2]
    low = sublane(near.shape) < 4
    after = jnp.where(even, near, other)
    before = jnp.where(even, other, near)
    if p % 2 == 0:
        return jnp.where(low, after, pltpu.roll(before, 4, 0))
    return jnp.where(low, pltpu.roll(after, 4, 0), before)


def pack_z(device, gradient, velocity, halo_x, halo_y, sizes):
    bx, by, bz = velocity.shape
    planes = bx + 2 * HALO
    pairs = planes // 2
    groups = bz // 4
    tall = by + 8

    def kernel(dev_ref, g_ref, v_ref, nx_ref, ox_ref, ny_ref, oy_ref, near_ref, other_ref):
        even_x, even_y, even_z = (is_even(i) for i in position(dev_ref, sizes))
        group = lane((tall, bz)) // 4
        for field, main in enumerate((g_ref, v_ref)):
            first = jnp.zeros((tall, bz), F32)
            last = jnp.zeros((tall, bz), F32)
            for p in range(planes):
                own = plane_of(main, nx_ref, ox_ref, even_x, field, p)
                extra = rows_of(ny_ref, oy_ref, even_y, field, p, pairs)
                plane = jnp.concatenate([own, extra], 0)
                turned = pltpu.roll(plane, 4 * p, 1) if p else plane
                first = jnp.where(group == p, turned, first)
                last = jnp.where(group == (p - 1) % groups, turned, last)
            near_ref[pl.ds(field * tall, tall)] = jnp.where(even_z, last, first)
            other_ref[pl.ds(field * tall, tall)] = jnp.where(even_z, first, last)

    edge = struct(2 * tall, bz)
    return pl.pallas_call(
        kernel,
        name="pack_z",
        compiler_params=PARAMS,
        out_shape=(edge, edge),
        in_specs=[SMEM] + [VMEM] * 6,
        out_specs=(VMEM,) * 2,
    )(device, gradient, velocity, *halo_x, *halo_y)


def proximal(device, gradient, velocity, halos, squares, sizes):
    bx, by, bz = velocity.shape
    planes = bx + 2 * HALO
    pairs = planes // 2
    tall = by + 8
    wide = 2 * bz
    size_x, size_y, size_z = sizes
    cells = size_x * bx * size_y * by * size_z * bz

    def kernel(
        dev_ref,
        g_ref,
        v_ref,
        nx_ref,
        ox_ref,
        ny_ref,
        oy_ref,
        nz_ref,
        oz_ref,
        sq_ref,
        gradient_ref,
        model_ref,
        target,
        current,
        extra,
        dual_x,
        dual_y,
        dual_z,
        model,
        sems,
    ):
        gradient_copy = pltpu.make_async_copy(g_ref, gradient_ref, sems.at[0])
        gradient_copy.start()
        pos_x, pos_y, pos_z = position(dev_ref, sizes)
        even_x, even_y, even_z = (is_even(i) for i in (pos_x, pos_y, pos_z))

        total = jnp.sum(jnp.sum(sq_ref[...], axis=0), axis=1, keepdims=True)
        scale = step_length * lax.rsqrt(total / cells + 1.0)
        scale = jnp.broadcast_to(scale, (1, bz))

        side_lane = lane((tall, bz)) < bz // 2
        near_z = nz_ref[pl.ds(tall, tall)] - scale * nz_ref[pl.ds(0, tall)]
        other_z = oz_ref[pl.ds(tall, tall)] - scale * oz_ref[pl.ds(0, tall)]
        before_z = jnp.where(even_z, other_z, near_z)
        after_z = jnp.where(even_z, near_z, other_z)
        for p in range(planes):
            own, rows = (
                [
                    plane_of(main, nx_ref, ox_ref, even_x, field, p),
                    rows_of(ny_ref, oy_ref, even_y, field, p, pairs),
                ]
                for field, main in ((1, v_ref), (0, g_ref))
            )
            own, rows = (own[0] - scale * rows[0], own[1] - scale * rows[1])
            back = (bz - 4 * p) % bz
            after = pltpu.roll(after_z, back, 1) if back else after_z
            before = pltpu.roll(before_z, back, 1) if back else before_z
            target[p, pl.ds(0, by), pl.ds(0, bz)] = own
            target[p, pl.ds(by, 8), pl.ds(0, bz)] = rows
            target[p, :, pl.ds(bz, bz)] = jnp.where(side_lane, after, before)

        def factor(index, limit):
            return jnp.where((index >= 0) & (index < limit - 1), dual_step, 0.0).astype(F32)

        row = sublane((tall, 1))
        row = jnp.where(row < by + 4, row, row - tall) + pos_y * by
        factor_y = factor(row, size_y * by)
        col = lane((1, wide))
        col = jnp.where(col < bz + bz // 2, col, col - wide) + pos_z * bz
        factor_z = factor(col, size_z * bz)
        shrink = 1.0 / (1.0 + primal_step)
        gain = primal_step / (1.0 + primal_step)

        for iteration in range(ITERS):
            first = iteration == 0
            final = iteration == ITERS - 1
            here_ref = target if first else extra
            ahead = here_ref[iteration]
            before_x = None
            for p in range(iteration, planes - 1 - iteration):
                here = ahead
                ahead = here_ref[p + 1]
                index = pos_x * bx + (p - HALO)
                factor_x = factor(index, size_x * bx)
                dx = factor_x * (ahead - here)
                dy = factor_y * (pltpu.roll(here, tall - 1, 0) - here)
                dz = factor_z * (pltpu.roll(here, wide - 1, 1) - here)
                if not first:
                    dx = dual_x[p] + dx
                    dy = dual_y[p] + dy
                    dz = dual_z[p] + dz
                norm = dx * dx + dy * dy + dz * dz
                ratio = jnp.minimum(1.0, tv_weight * lax.rsqrt(norm))
                dx = dx * ratio
                dy = dy * ratio
                dz = dz * ratio
                if not final:
                    dual_x[p] = dx
                    dual_y[p] = dy
                    dual_z[p] = dz
                if p > iteration:
                    if final:
                        spread = dx[:by, :bz] - before_x
                        spread += dy[:by, :bz] - pltpu.roll(dy[:, :bz], 1, 0)[:by]
                        spread += dz[:by, :bz] - pltpu.roll(dz[:by], 1, 1)[:, :bz]
                        goal = target[p, pl.ds(0, by), pl.ds(0, bz)]
                        old = current[p, pl.ds(0, by), pl.ds(0, bz)]
                        model[p - HALO] = shrink * old + gain * (spread + goal)
                    else:
                        spread = dx - before_x
                        spread += dy - pltpu.roll(dy, 1, 0)
                        spread += dz - pltpu.roll(dz, 1, 1)
                        if first:
                            new = here + gain * spread
                            old = here
                        else:
                            old = current[p]
                            new = shrink * old + gain * (spread + target[p])
                        current[p] = new
                        extra[p] = 2.0 * new - old
                before_x = dx[:by, :bz] if final else dx
        model_copy = pltpu.make_async_copy(model, model_ref, sems.at[1])
        model_copy.start()
        gradient_copy.wait()
        model_copy.wait()

    field = pltpu.VMEM((planes, tall, wide), F32)
    return pl.pallas_call(
        kernel,
        name="proximal",
        compiler_params=PARAMS,
        out_shape=(struct(bx, by, bz),) * 2,
        in_specs=[SMEM] + [VMEM] * 9,
        out_specs=(HBM,) * 2,
        scratch_shapes=[field] * 6 + [pltpu.VMEM((bx, by, bz), F32), pltpu.SemaphoreType.DMA((2,))],
    )(device, gradient, velocity, *halos, squares)


def shards(partials, code_bits, group_map, velocity):
    sizes = tuple(lax.axis_size(axis) for axis in (GX, GY, "gz"))
    device = lax.axis_index(ALL).astype(jnp.int32).reshape(1)

    local = presum(device, partials, code_bits, group_map, sizes, 8)
    parts = lax.all_to_all(local, GX, split_axis=0, concat_axis=0, tiled=True)
    gradient, *send_x, squares = reduce_pack(device, parts, velocity, sizes)
    halo_x = swap(send_x, GX)
    table = jnp.broadcast_to(squares[:1][None], (sizes[0] * sizes[2], 1, squares.shape[1]))
    table = lax.all_to_all(table, XZ, split_axis=0, concat_axis=0, tiled=True)
    send_y = pack_y(device, gradient, velocity, halo_x, sizes)
    halo_y = swap(send_y, GY)
    table = jnp.broadcast_to(jnp.sum(table, axis=0, keepdims=True), (sizes[1], 1, squares.shape[1]))
    table = lax.all_to_all(table, GY, split_axis=0, concat_axis=0, tiled=True)
    send_z = pack_z(device, gradient, velocity, halo_x, halo_y, sizes)
    halo_z = swap(send_z, "gz")
    halos = (*halo_x, *halo_y, *halo_z)
    return proximal(device, gradient, velocity, halos, table, sizes)


def solution(mesh):
    torus = Mesh(
        mesh.devices.reshape(4, 2, 4, 2, mesh.shape["gz"]), ("gx_0", "gx_1", "gy_0", "gy_1", "gz")
    )
    placed = (P(GX, None, GY, "gz"), P(), P(), P(GX, GY, "gz"))
    return jax.shard_map(
        shards,
        mesh=torus,
        in_specs=placed,
        out_specs=(P(GX, GY, "gz"), P(GX, GY, "gz")),
        check_vma=False,
    )
```

```python
import jax
import jax.numpy as jnp
from jax import lax
from jax.experimental import pallas as pl
from jax.experimental.pallas import tpu as pltpu
from jax.sharding import Mesh
from jax.sharding import PartitionSpec as P

ITERS = 3
HALO = ITERS
GX = ("gx_0", "gx_1")
GY = ("gy_0", "gy_1")
ALL = GX + GY + ("gz",)

step_length = 0.5
tv_weight = 0.2
dual_step = 0.28
primal_step = 0.28

VMEM = pl.BlockSpec(memory_space=pltpu.VMEM)
SMEM = pl.BlockSpec(memory_space=pltpu.SMEM)
HBM = pl.BlockSpec(memory_space=pltpu.HBM)
PARAMS = pltpu.CompilerParams(vmem_limit_bytes=16 * 1024 * 1024)
F32 = jnp.float32


def swap(blocks, axis):
    size = lax.axis_size(axis)
    pairs = [(i, i ^ 1) for i in range(size)]
    others = [(i, min(max(((i + 1) ^ 1) - 1, 0), size - 1)) for i in range(size)]
    return lax.ppermute(blocks[0], axis, pairs), lax.ppermute(blocks[1], axis, others)


def struct(*shape):
    return jax.ShapeDtypeStruct(shape, F32)


def in_hbm(array):
    return pltpu.with_memory_space_constraint(array, pltpu.HBM)


def presum(device, partials, code_bits, group_map, sizes, chunks):
    slots, nx, by, bz = partials.shape
    rows = nx // chunks

    def kernel(dev_ref, map_hbm, bits_hbm, part_ref, out_ref, buf, map_ref, bits_ref, sems):
        map_copy = pltpu.make_async_copy(map_hbm, map_ref, sems.at[chunks])
        bits_copy = pltpu.make_async_copy(bits_hbm, bits_ref, sems.at[chunks + 1])
        map_copy.start()
        bits_copy.start()

        def copy(c):
            part = pl.ds(c * rows, rows)
            return pltpu.make_async_copy(part_ref.at[:, part], buf.at[:, part], sems.at[c])

        for c in range(chunks):
            copy(c).start()
        map_copy.wait()
        bits_copy.wait()
        base = position(dev_ref, sizes)[0] * slots
        groups = [map_ref[base + s] for s in range(slots)]
        for c in range(chunks):
            copy(c).wait()

            def row(i, carry):
                x = c * rows + i
                total = None
                for s in range(slots):
                    sign = (2 * bits_ref[groups[s], x] - 1).astype(F32)
                    term = sign * buf[s, x]
                    total = term if total is None else total + term
                out_ref[x] = total
                return carry

            lax.fori_loop(0, rows, row, 0, unroll=4)

    return pl.pallas_call(
        kernel,
        name="presum",
        compiler_params=PARAMS,
        out_shape=struct(nx, by, bz),
        in_specs=[SMEM, HBM, HBM, HBM],
        out_specs=VMEM,
        scratch_shapes=[
            pltpu.VMEM(partials.shape, F32),
            pltpu.SMEM(group_map.shape, jnp.int32),
            pltpu.SMEM(code_bits.shape, jnp.int32),
            pltpu.SemaphoreType.DMA((chunks + 2,)),
        ],
    )(device, in_hbm(group_map), in_hbm(code_bits), in_hbm(partials))


def position(dev_ref, sizes):
    _, size_y, size_z = sizes
    dev = dev_ref[0]
    return dev // (size_y * size_z), (dev // size_z) % size_y, dev % size_z


def is_even(index):
    return index % 2 == 0


def reduce_pack(device, parts, velocity, sizes):
    bx, by, bz = velocity.shape
    members = sizes[0]

    def kernel(dev_ref, part_ref, v_ref, g_ref, near_ref, other_ref, square_ref):
        even = is_even(position(dev_ref, sizes)[0])
        squares = jnp.zeros((by, bz), F32)
        for i in range(bx):
            total = part_ref[i]
            for m in range(1, members):
                total = total + part_ref[m * bx + i]
            g_ref[i] = total
            squares = squares + total * total
        for i in range(HALO):
            for k, ref in enumerate((g_ref, v_ref)):
                first, last = ref[i], ref[bx - HALO + i]
                near_ref[k * HALO + i] = jnp.where(even, last, first)
                other_ref[k * HALO + i] = jnp.where(even, first, last)
        square_ref[...] = jnp.broadcast_to(jnp.sum(squares, axis=0, keepdims=True), (8, bz))

    edge = struct(2 * HALO, by, bz)
    return pl.pallas_call(
        kernel,
        name="reduce_pack",
        compiler_params=PARAMS,
        out_shape=(struct(bx, by, bz), edge, edge, struct(8, bz)),
        in_specs=[SMEM, VMEM, VMEM],
        out_specs=(VMEM,) * 4,
    )(device, parts, velocity)


def plane_of(main_ref, near_ref, other_ref, even, field, p):
    bx = main_ref.shape[0]
    if p < HALO:
        at = field * HALO + p
        return jnp.where(even, other_ref[at], near_ref[at])
    if p < HALO + bx:
        return main_ref[p - HALO]
    at = field * HALO + p - HALO - bx
    return jnp.where(even, near_ref[at], other_ref[at])


def sublane(shape):
    return lax.broadcasted_iota(jnp.int32, shape, len(shape) - 2)


def lane(shape):
    return lax.broadcasted_iota(jnp.int32, shape, len(shape) - 1)


def pack_y(device, gradient, velocity, halo_x, sizes):
    bx, by, bz = velocity.shape
    pairs = (bx + 2 * HALO) // 2

    def kernel(dev_ref, g_ref, v_ref, nx_ref, ox_ref, near_ref, other_ref):
        even_x, even_y = (is_even(i) for i in position(dev_ref, sizes)[:2])
        low = sublane((8, bz)) < 4
        for field, main in enumerate((g_ref, v_ref)):
            for q in range(pairs):
                left = plane_of(main, nx_ref, ox_ref, even_x, field, 2 * q)
                right = plane_of(main, nx_ref, ox_ref, even_x, field, 2 * q + 1)
                first = jnp.where(low, left[:8], pltpu.roll(right[:8], 4, 0))
                last = jnp.where(low, pltpu.roll(left[by - 8 :], 4, 0), right[by - 8 :])
                near_ref[field * pairs + q] = jnp.where(even_y, last, first)
                other_ref[field * pairs + q] = jnp.where(even_y, first, last)

    edge = struct(2 * pairs, 8, bz)
    return pl.pallas_call(
        kernel,
        name="pack_y",
        compiler_params=PARAMS,
        out_shape=(edge, edge),
        in_specs=[SMEM] + [VMEM] * 4,
        out_specs=(VMEM,) * 2,
    )(device, gradient, velocity, *halo_x)


def rows_of(near_ref, other_ref, even, field, p, pairs):
    near = near_ref[field * pairs + p // 2]
    other = other_ref[field * pairs + p // 2]
    low = sublane(near.shape) < 4
    after = jnp.where(even, near, other)
    before = jnp.where(even, other, near)
    if p % 2 == 0:
        return jnp.where(low, after, pltpu.roll(before, 4, 0))
    return jnp.where(low, pltpu.roll(after, 4, 0), before)


def pack_z(device, gradient, velocity, halo_x, halo_y, sizes):
    bx, by, bz = velocity.shape
    planes = bx + 2 * HALO
    pairs = planes // 2
    groups = bz // 4
    tall = by + 8

    def kernel(dev_ref, g_ref, v_ref, nx_ref, ox_ref, ny_ref, oy_ref, near_ref, other_ref):
        even_x, even_y, even_z = (is_even(i) for i in position(dev_ref, sizes))
        group = lane((tall, bz)) // 4
        for field, main in enumerate((g_ref, v_ref)):
            first = jnp.zeros((tall, bz), F32)
            last = jnp.zeros((tall, bz), F32)
            for p in range(planes):
                own = plane_of(main, nx_ref, ox_ref, even_x, field, p)
                extra = rows_of(ny_ref, oy_ref, even_y, field, p, pairs)
                plane = jnp.concatenate([own, extra], 0)
                turned = pltpu.roll(plane, 4 * p, 1) if p else plane
                first = jnp.where(group == p, turned, first)
                last = jnp.where(group == (p - 1) % groups, turned, last)
            near_ref[pl.ds(field * tall, tall)] = jnp.where(even_z, last, first)
            other_ref[pl.ds(field * tall, tall)] = jnp.where(even_z, first, last)

    edge = struct(2 * tall, bz)
    return pl.pallas_call(
        kernel,
        name="pack_z",
        compiler_params=PARAMS,
        out_shape=(edge, edge),
        in_specs=[SMEM] + [VMEM] * 6,
        out_specs=(VMEM,) * 2,
    )(device, gradient, velocity, *halo_x, *halo_y)


def proximal(device, gradient, velocity, halos, squares, sizes):
    bx, by, bz = velocity.shape
    planes = bx + 2 * HALO
    pairs = planes // 2
    tall = by + 8
    wide = 2 * bz
    size_x, size_y, size_z = sizes
    cells = size_x * bx * size_y * by * size_z * bz

    def kernel(
        dev_ref,
        g_ref,
        v_ref,
        nx_ref,
        ox_ref,
        ny_ref,
        oy_ref,
        nz_ref,
        oz_ref,
        sq_ref,
        gradient_ref,
        model_ref,
        target,
        current,
        extra,
        dual_x,
        dual_y,
        dual_z,
        model,
        sems,
    ):
        gradient_copy = pltpu.make_async_copy(g_ref, gradient_ref, sems.at[0])
        gradient_copy.start()
        pos_x, pos_y, pos_z = position(dev_ref, sizes)
        even_x, even_y, even_z = (is_even(i) for i in (pos_x, pos_y, pos_z))

        total = jnp.sum(jnp.sum(sq_ref[...], axis=0), axis=1, keepdims=True)
        scale = step_length * lax.rsqrt(total / cells + 1.0)
        scale = jnp.broadcast_to(scale, (1, bz))

        side_lane = lane((tall, bz)) < bz // 2
        near_z = nz_ref[pl.ds(tall, tall)] - scale * nz_ref[pl.ds(0, tall)]
        other_z = oz_ref[pl.ds(tall, tall)] - scale * oz_ref[pl.ds(0, tall)]
        before_z = jnp.where(even_z, other_z, near_z)
        after_z = jnp.where(even_z, near_z, other_z)
        for p in range(planes):
            own, rows = (
                [
                    plane_of(main, nx_ref, ox_ref, even_x, field, p),
                    rows_of(ny_ref, oy_ref, even_y, field, p, pairs),
                ]
                for field, main in ((1, v_ref), (0, g_ref))
            )
            own, rows = (own[0] - scale * rows[0], own[1] - scale * rows[1])
            back = (bz - 4 * p) % bz
            after = pltpu.roll(after_z, back, 1) if back else after_z
            before = pltpu.roll(before_z, back, 1) if back else before_z
            target[p, pl.ds(0, by), pl.ds(0, bz)] = own
            target[p, pl.ds(by, 8), pl.ds(0, bz)] = rows
            target[p, :, pl.ds(bz, bz)] = jnp.where(side_lane, after, before)

        def factor(index, limit):
            return jnp.where((index >= 0) & (index < limit - 1), dual_step, 0.0).astype(F32)

        row = sublane((tall, 1))
        row = jnp.where(row < by + 4, row, row - tall) + pos_y * by
        factor_y = factor(row, size_y * by)
        col = lane((1, wide))
        col = jnp.where(col < bz + bz // 2, col, col - wide) + pos_z * bz
        factor_z = factor(col, size_z * bz)
        shrink = 1.0 / (1.0 + primal_step)
        gain = primal_step / (1.0 + primal_step)

        for iteration in range(ITERS):
            first = iteration == 0
            final = iteration == ITERS - 1
            here_ref = target if first else extra
            ahead = here_ref[iteration]
            before_x = None
            for p in range(iteration, planes - 1 - iteration):
                here = ahead
                ahead = here_ref[p + 1]
                index = pos_x * bx + (p - HALO)
                factor_x = factor(index, size_x * bx)
                dx = factor_x * (ahead - here)
                dy = factor_y * (pltpu.roll(here, tall - 1, 0) - here)
                dz = factor_z * (pltpu.roll(here, wide - 1, 1) - here)
                if not first:
                    dx = dual_x[p] + dx
                    dy = dual_y[p] + dy
                    dz = dual_z[p] + dz
                norm = dx * dx + dy * dy + dz * dz
                ratio = jnp.minimum(1.0, tv_weight * lax.rsqrt(norm))
                dx = dx * ratio
                dy = dy * ratio
                dz = dz * ratio
                if not final:
                    dual_x[p] = dx
                    dual_y[p] = dy
                    dual_z[p] = dz
                if p > iteration:
                    if final:
                        spread = dx[:by, :bz] - before_x
                        spread += dy[:by, :bz] - pltpu.roll(dy[:, :bz], 1, 0)[:by]
                        spread += dz[:by, :bz] - pltpu.roll(dz[:by], 1, 1)[:, :bz]
                        goal = target[p, pl.ds(0, by), pl.ds(0, bz)]
                        old = current[p, pl.ds(0, by), pl.ds(0, bz)]
                        model[p - HALO] = shrink * old + gain * (spread + goal)
                    else:
                        spread = dx - before_x
                        spread += dy - pltpu.roll(dy, 1, 0)
                        spread += dz - pltpu.roll(dz, 1, 1)
                        if first:
                            new = here + gain * spread
                            old = here
                        else:
                            old = current[p]
                            new = shrink * old + gain * (spread + target[p])
                        current[p] = new
                        extra[p] = 2.0 * new - old
                before_x = dx[:by, :bz] if final else dx
        model_copy = pltpu.make_async_copy(model, model_ref, sems.at[1])
        model_copy.start()
        gradient_copy.wait()
        model_copy.wait()

    field = pltpu.VMEM((planes, tall, wide), F32)
    return pl.pallas_call(
        kernel,
        name="proximal",
        compiler_params=PARAMS,
        out_shape=(struct(bx, by, bz),) * 2,
        in_specs=[SMEM] + [VMEM] * 9,
        out_specs=(HBM,) * 2,
        scratch_shapes=[field] * 6 + [pltpu.VMEM((bx, by, bz), F32), pltpu.SemaphoreType.DMA((2,))],
    )(device, gradient, velocity, *halos, squares)


def shards(partials, code_bits, group_map, velocity):
    sizes = tuple(lax.axis_size(axis) for axis in (GX, GY, "gz"))
    device = lax.axis_index(ALL).astype(jnp.int32).reshape(1)

    local = presum(device, partials, code_bits, group_map, sizes, 8)
    parts = lax.all_to_all(local, GX, split_axis=0, concat_axis=0, tiled=True)
    gradient, *send_x, squares = reduce_pack(device, parts, velocity, sizes)
    halo_x = swap(send_x, GX)
    table = jnp.broadcast_to(
        squares[:1][None], (sizes[0] * sizes[1] * sizes[2], 1, squares.shape[1])
    )
    table = lax.all_to_all(table, ALL, split_axis=0, concat_axis=0, tiled=True)
    send_y = pack_y(device, gradient, velocity, halo_x, sizes)
    halo_y = swap(send_y, GY)
    send_z = pack_z(device, gradient, velocity, halo_x, halo_y, sizes)
    halo_z = swap(send_z, "gz")
    halos = (*halo_x, *halo_y, *halo_z)
    return proximal(device, gradient, velocity, halos, table, sizes)


def solution(mesh):
    torus = Mesh(
        mesh.devices.reshape(4, 2, 4, 2, mesh.shape["gz"]), ("gx_0", "gx_1", "gy_0", "gy_1", "gz")
    )
    placed = (P(GX, None, GY, "gz"), P(), P(), P(GX, GY, "gz"))
    return jax.shard_map(
        shards,
        mesh=torus,
        in_specs=placed,
        out_specs=(P(GX, GY, "gz"), P(GX, GY, "gz")),
        check_vma=False,
    )
```

```python
import jax
import jax.numpy as jnp
from jax import lax
from jax.experimental import pallas as pl
from jax.experimental.pallas import tpu as pltpu
from jax.sharding import Mesh
from jax.sharding import PartitionSpec as P

ITERS = 3
HALO = ITERS
GX = ("gx_0", "gx_1")
GY = ("gy_0", "gy_1")
ALL = GX + GY + ("gz",)

step_length = 0.5
tv_weight = 0.2
dual_step = 0.28
primal_step = 0.28

VMEM = pl.BlockSpec(memory_space=pltpu.VMEM)
SMEM = pl.BlockSpec(memory_space=pltpu.SMEM)
HBM = pl.BlockSpec(memory_space=pltpu.HBM)
PARAMS = pltpu.CompilerParams(vmem_limit_bytes=16 * 1024 * 1024)
F32 = jnp.float32


def swap(blocks, axis, spare):
    size, width = lax.axis_size(axis), lax.axis_size(spare)
    pairs = [(i, i ^ 1) for i in range(size)]
    axes = axis if isinstance(axis, tuple) else (axis,)
    ahead = ALL.index(spare) < ALL.index(axes[0])

    def at(i, k):
        return k * size + i if ahead else i * width + k

    others = []
    for i in range(size):
        j = ((i + 1) ^ 1) - 1
        for k in range(width):
            others.append((at(i, k), at(j, k) if 0 <= j < size else at(i, k ^ 1)))
    both = (spare, *axes) if ahead else (*axes, spare)
    return lax.ppermute(blocks[0], axis, pairs), lax.ppermute(blocks[1], both, others)


def struct(*shape):
    return jax.ShapeDtypeStruct(shape, F32)


def in_hbm(array):
    return pltpu.with_memory_space_constraint(array, pltpu.HBM)


def presum(device, partials, code_bits, group_map, sizes, chunks):
    slots, nx, by, bz = partials.shape
    rows = nx // chunks

    def kernel(dev_ref, map_hbm, bits_hbm, part_ref, out_ref, buf, map_ref, bits_ref, sems):
        map_copy = pltpu.make_async_copy(map_hbm, map_ref, sems.at[chunks])
        bits_copy = pltpu.make_async_copy(bits_hbm, bits_ref, sems.at[chunks + 1])
        map_copy.start()
        bits_copy.start()

        def copy(c):
            part = pl.ds(c * rows, rows)
            return pltpu.make_async_copy(part_ref.at[:, part], buf.at[:, part], sems.at[c])

        for c in range(chunks):
            copy(c).start()
        map_copy.wait()
        bits_copy.wait()
        base = position(dev_ref, sizes)[0] * slots
        groups = [map_ref[base + s] for s in range(slots)]
        for c in range(chunks):
            copy(c).wait()

            def row(i, carry):
                x = c * rows + i
                total = None
                for s in range(slots):
                    sign = (2 * bits_ref[groups[s], x] - 1).astype(F32)
                    term = sign * buf[s, x]
                    total = term if total is None else total + term
                out_ref[x] = total
                return carry

            lax.fori_loop(0, rows, row, 0, unroll=4)

    return pl.pallas_call(
        kernel,
        name="presum",
        compiler_params=PARAMS,
        out_shape=struct(nx, by, bz),
        in_specs=[SMEM, HBM, HBM, HBM],
        out_specs=VMEM,
        scratch_shapes=[
            pltpu.VMEM(partials.shape, F32),
            pltpu.SMEM(group_map.shape, jnp.int32),
            pltpu.SMEM(code_bits.shape, jnp.int32),
            pltpu.SemaphoreType.DMA((chunks + 2,)),
        ],
    )(device, in_hbm(group_map), in_hbm(code_bits), in_hbm(partials))


def position(dev_ref, sizes):
    _, size_y, size_z = sizes
    dev = dev_ref[0]
    return dev // (size_y * size_z), (dev // size_z) % size_y, dev % size_z


def is_even(index):
    return index % 2 == 0


def reduce_pack(device, parts, velocity, sizes):
    bx, by, bz = velocity.shape
    members = sizes[0]

    def kernel(dev_ref, part_ref, v_ref, g_ref, near_ref, other_ref, square_ref):
        even = is_even(position(dev_ref, sizes)[0])
        squares = jnp.zeros((by, bz), F32)
        for i in range(bx):
            total = part_ref[i]
            for m in range(1, members):
                total = total + part_ref[m * bx + i]
            g_ref[i] = total
            squares = squares + total * total
        for i in range(HALO):
            for k, ref in enumerate((g_ref, v_ref)):
                first, last = ref[i], ref[bx - HALO + i]
                near_ref[k * HALO + i] = jnp.where(even, last, first)
                other_ref[k * HALO + i] = jnp.where(even, first, last)
        square_ref[...] = jnp.broadcast_to(jnp.sum(squares, axis=0, keepdims=True), (8, bz))

    edge = struct(2 * HALO, by, bz)
    return pl.pallas_call(
        kernel,
        name="reduce_pack",
        compiler_params=PARAMS,
        out_shape=(struct(bx, by, bz), edge, edge, struct(8, bz)),
        in_specs=[SMEM, VMEM, VMEM],
        out_specs=(VMEM,) * 4,
    )(device, parts, velocity)


def plane_of(main_ref, near_ref, other_ref, even, field, p):
    bx = main_ref.shape[0]
    if p < HALO:
        at = field * HALO + p
        return jnp.where(even, other_ref[at], near_ref[at])
    if p < HALO + bx:
        return main_ref[p - HALO]
    at = field * HALO + p - HALO - bx
    return jnp.where(even, near_ref[at], other_ref[at])


def sublane(shape):
    return lax.broadcasted_iota(jnp.int32, shape, len(shape) - 2)


def lane(shape):
    return lax.broadcasted_iota(jnp.int32, shape, len(shape) - 1)


def pack_y(device, gradient, velocity, halo_x, sizes):
    bx, by, bz = velocity.shape
    pairs = (bx + 2 * HALO) // 2

    def kernel(dev_ref, g_ref, v_ref, nx_ref, ox_ref, near_ref, other_ref):
        even_x, even_y = (is_even(i) for i in position(dev_ref, sizes)[:2])
        low = sublane((8, bz)) < 4
        for field, main in enumerate((g_ref, v_ref)):
            for q in range(pairs):
                left = plane_of(main, nx_ref, ox_ref, even_x, field, 2 * q)
                right = plane_of(main, nx_ref, ox_ref, even_x, field, 2 * q + 1)
                first = jnp.where(low, left[:8], pltpu.roll(right[:8], 4, 0))
                last = jnp.where(low, pltpu.roll(left[by - 8 :], 4, 0), right[by - 8 :])
                near_ref[field * pairs + q] = jnp.where(even_y, last, first)
                other_ref[field * pairs + q] = jnp.where(even_y, first, last)

    edge = struct(2 * pairs, 8, bz)
    return pl.pallas_call(
        kernel,
        name="pack_y",
        compiler_params=PARAMS,
        out_shape=(edge, edge),
        in_specs=[SMEM] + [VMEM] * 4,
        out_specs=(VMEM,) * 2,
    )(device, gradient, velocity, *halo_x)


def rows_of(near_ref, other_ref, even, field, p, pairs):
    near = near_ref[field * pairs + p // 2]
    other = other_ref[field * pairs + p // 2]
    low = sublane(near.shape) < 4
    after = jnp.where(even, near, other)
    before = jnp.where(even, other, near)
    if p % 2 == 0:
        return jnp.where(low, after, pltpu.roll(before, 4, 0))
    return jnp.where(low, pltpu.roll(after, 4, 0), before)


def pack_z(device, gradient, velocity, halo_x, halo_y, sizes):
    bx, by, bz = velocity.shape
    planes = bx + 2 * HALO
    pairs = planes // 2
    groups = bz // 4
    tall = by + 8

    def kernel(dev_ref, g_ref, v_ref, nx_ref, ox_ref, ny_ref, oy_ref, near_ref, other_ref):
        even_x, even_y, even_z = (is_even(i) for i in position(dev_ref, sizes))
        group = lane((tall, bz)) // 4
        for field, main in enumerate((g_ref, v_ref)):
            first = jnp.zeros((tall, bz), F32)
            last = jnp.zeros((tall, bz), F32)
            for p in range(planes):
                own = plane_of(main, nx_ref, ox_ref, even_x, field, p)
                extra = rows_of(ny_ref, oy_ref, even_y, field, p, pairs)
                plane = jnp.concatenate([own, extra], 0)
                turned = pltpu.roll(plane, 4 * p, 1) if p else plane
                first = jnp.where(group == p, turned, first)
                last = jnp.where(group == (p - 1) % groups, turned, last)
            near_ref[pl.ds(field * tall, tall)] = jnp.where(even_z, last, first)
            other_ref[pl.ds(field * tall, tall)] = jnp.where(even_z, first, last)

    edge = struct(2 * tall, bz)
    return pl.pallas_call(
        kernel,
        name="pack_z",
        compiler_params=PARAMS,
        out_shape=(edge, edge),
        in_specs=[SMEM] + [VMEM] * 6,
        out_specs=(VMEM,) * 2,
    )(device, gradient, velocity, *halo_x, *halo_y)


def proximal(device, gradient, velocity, halos, squares, sizes):
    bx, by, bz = velocity.shape
    planes = bx + 2 * HALO
    pairs = planes // 2
    tall = by + 8
    wide = 2 * bz
    size_x, size_y, size_z = sizes
    cells = size_x * bx * size_y * by * size_z * bz

    def kernel(
        dev_ref,
        g_ref,
        v_ref,
        nx_ref,
        ox_ref,
        ny_ref,
        oy_ref,
        nz_ref,
        oz_ref,
        sq_ref,
        gradient_ref,
        model_ref,
        target,
        current,
        extra,
        dual_x,
        dual_y,
        dual_z,
        model,
        sems,
    ):
        gradient_copy = pltpu.make_async_copy(g_ref, gradient_ref, sems.at[0])
        gradient_copy.start()
        pos_x, pos_y, pos_z = position(dev_ref, sizes)
        even_x, even_y, even_z = (is_even(i) for i in (pos_x, pos_y, pos_z))

        total = jnp.sum(jnp.sum(sq_ref[...], axis=0), axis=1, keepdims=True)
        scale = step_length * lax.rsqrt(total / cells + 1.0)
        scale = jnp.broadcast_to(scale, (1, bz))

        side_lane = lane((tall, bz)) < bz // 2
        near_z = nz_ref[pl.ds(tall, tall)] - scale * nz_ref[pl.ds(0, tall)]
        other_z = oz_ref[pl.ds(tall, tall)] - scale * oz_ref[pl.ds(0, tall)]
        before_z = jnp.where(even_z, other_z, near_z)
        after_z = jnp.where(even_z, near_z, other_z)
        for p in range(planes):
            own, rows = (
                [
                    plane_of(main, nx_ref, ox_ref, even_x, field, p),
                    rows_of(ny_ref, oy_ref, even_y, field, p, pairs),
                ]
                for field, main in ((1, v_ref), (0, g_ref))
            )
            own, rows = (own[0] - scale * rows[0], own[1] - scale * rows[1])
            back = (bz - 4 * p) % bz
            after = pltpu.roll(after_z, back, 1) if back else after_z
            before = pltpu.roll(before_z, back, 1) if back else before_z
            target[p, pl.ds(0, by), pl.ds(0, bz)] = own
            target[p, pl.ds(by, 8), pl.ds(0, bz)] = rows
            target[p, :, pl.ds(bz, bz)] = jnp.where(side_lane, after, before)

        def factor(index, limit):
            return jnp.where((index >= 0) & (index < limit - 1), dual_step, 0.0).astype(F32)

        row = sublane((tall, 1))
        row = jnp.where(row < by + 4, row, row - tall) + pos_y * by
        factor_y = factor(row, size_y * by)
        col = lane((1, wide))
        col = jnp.where(col < bz + bz // 2, col, col - wide) + pos_z * bz
        factor_z = factor(col, size_z * bz)
        shrink = 1.0 / (1.0 + primal_step)
        gain = primal_step / (1.0 + primal_step)

        for iteration in range(ITERS):
            first = iteration == 0
            final = iteration == ITERS - 1
            here_ref = target if first else extra
            ahead = here_ref[iteration]
            before_x = None
            for p in range(iteration, planes - 1 - iteration):
                here = ahead
                ahead = here_ref[p + 1]
                index = pos_x * bx + (p - HALO)
                factor_x = factor(index, size_x * bx)
                dx = factor_x * (ahead - here)
                dy = factor_y * (pltpu.roll(here, tall - 1, 0) - here)
                dz = factor_z * (pltpu.roll(here, wide - 1, 1) - here)
                if not first:
                    dx = dual_x[p] + dx
                    dy = dual_y[p] + dy
                    dz = dual_z[p] + dz
                norm = dx * dx + dy * dy + dz * dz
                ratio = jnp.minimum(1.0, tv_weight * lax.rsqrt(norm))
                dx = dx * ratio
                dy = dy * ratio
                dz = dz * ratio
                if not final:
                    dual_x[p] = dx
                    dual_y[p] = dy
                    dual_z[p] = dz
                if p > iteration:
                    if final:
                        spread = dx[:by, :bz] - before_x
                        spread += dy[:by, :bz] - pltpu.roll(dy[:, :bz], 1, 0)[:by]
                        spread += dz[:by, :bz] - pltpu.roll(dz[:by], 1, 1)[:, :bz]
                        goal = target[p, pl.ds(0, by), pl.ds(0, bz)]
                        old = current[p, pl.ds(0, by), pl.ds(0, bz)]
                        model[p - HALO] = shrink * old + gain * (spread + goal)
                    else:
                        spread = dx - before_x
                        spread += dy - pltpu.roll(dy, 1, 0)
                        spread += dz - pltpu.roll(dz, 1, 1)
                        if first:
                            new = here + gain * spread
                            old = here
                        else:
                            old = current[p]
                            new = shrink * old + gain * (spread + target[p])
                        current[p] = new
                        extra[p] = 2.0 * new - old
                before_x = dx[:by, :bz] if final else dx
        model_copy = pltpu.make_async_copy(model, model_ref, sems.at[1])
        model_copy.start()
        gradient_copy.wait()
        model_copy.wait()

    field = pltpu.VMEM((planes, tall, wide), F32)
    return pl.pallas_call(
        kernel,
        name="proximal",
        compiler_params=PARAMS,
        out_shape=(struct(bx, by, bz),) * 2,
        in_specs=[SMEM] + [VMEM] * 9,
        out_specs=(HBM,) * 2,
        scratch_shapes=[field] * 6 + [pltpu.VMEM((bx, by, bz), F32), pltpu.SemaphoreType.DMA((2,))],
    )(device, gradient, velocity, *halos, squares)


def shards(partials, code_bits, group_map, velocity):
    sizes = tuple(lax.axis_size(axis) for axis in (GX, GY, "gz"))
    device = lax.axis_index(ALL).astype(jnp.int32).reshape(1)

    local = presum(device, partials, code_bits, group_map, sizes, 8)
    parts = lax.all_to_all(local, GX, split_axis=0, concat_axis=0, tiled=True)
    gradient, *send_x, squares = reduce_pack(device, parts, velocity, sizes)
    halo_x = swap(send_x, GX, GY[1])
    table = jnp.broadcast_to(
        squares[:1][None], (sizes[0] * sizes[1] * sizes[2], 1, squares.shape[1])
    )
    table = lax.all_to_all(table, ALL, split_axis=0, concat_axis=0, tiled=True)
    send_y = pack_y(device, gradient, velocity, halo_x, sizes)
    halo_y = swap(send_y, GY, "gz")
    send_z = pack_z(device, gradient, velocity, halo_x, halo_y, sizes)
    halo_z = swap(send_z, "gz", GY[1])
    halos = (*halo_x, *halo_y, *halo_z)
    return proximal(device, gradient, velocity, halos, table, sizes)


def solution(mesh):
    torus = Mesh(
        mesh.devices.reshape(4, 2, 4, 2, mesh.shape["gz"]), ("gx_0", "gx_1", "gy_0", "gy_1", "gz")
    )
    placed = (P(GX, None, GY, "gz"), P(), P(), P(GX, GY, "gz"))
    return jax.shard_map(
        shards,
        mesh=torus,
        in_specs=placed,
        out_specs=(P(GX, GY, "gz"), P(GX, GY, "gz")),
        check_vma=False,
    )
```

```python
import jax
import jax.numpy as jnp
from jax import lax
from jax.experimental import pallas as pl
from jax.experimental.pallas import tpu as pltpu
from jax.sharding import Mesh
from jax.sharding import PartitionSpec as P

ITERS = 3
HALO = ITERS
GX = ("gx_0", "gx_1")
GY = ("gy_0", "gy_1")
ALL = GX + GY + ("gz",)
XZ = GX + ("gz",)

step_length = 0.5
tv_weight = 0.2
dual_step = 0.28
primal_step = 0.28

VMEM = pl.BlockSpec(memory_space=pltpu.VMEM)
SMEM = pl.BlockSpec(memory_space=pltpu.SMEM)
HBM = pl.BlockSpec(memory_space=pltpu.HBM)
PARAMS = pltpu.CompilerParams(vmem_limit_bytes=16 * 1024 * 1024)
F32 = jnp.float32


def swap(blocks, axis, spare):
    size, width = lax.axis_size(axis), lax.axis_size(spare)
    pairs = [(i, i ^ 1) for i in range(size)]
    axes = axis if isinstance(axis, tuple) else (axis,)
    ahead = ALL.index(spare) < ALL.index(axes[0])

    def at(i, k):
        return k * size + i if ahead else i * width + k

    others = []
    for i in range(size):
        j = ((i + 1) ^ 1) - 1
        for k in range(width):
            others.append((at(i, k), at(j, k) if 0 <= j < size else at(i, k ^ 1)))
    both = (spare, *axes) if ahead else (*axes, spare)
    return lax.ppermute(blocks[0], axis, pairs), lax.ppermute(blocks[1], both, others)


def add_pairs(row, axis, partner):
    size = lax.axis_size(axis)
    return row + lax.ppermute(row, axis, [(i, partner(i, size)) for i in range(size)])


def struct(*shape):
    return jax.ShapeDtypeStruct(shape, F32)


def in_hbm(array):
    return pltpu.with_memory_space_constraint(array, pltpu.HBM)


def presum(device, partials, code_bits, group_map, sizes, chunks):
    slots, nx, by, bz = partials.shape
    rows = nx // chunks

    def kernel(dev_ref, map_hbm, bits_hbm, part_ref, out_ref, buf, map_ref, bits_ref, sems):
        map_copy = pltpu.make_async_copy(map_hbm, map_ref, sems.at[chunks])
        bits_copy = pltpu.make_async_copy(bits_hbm, bits_ref, sems.at[chunks + 1])
        map_copy.start()
        bits_copy.start()

        def copy(c):
            part = pl.ds(c * rows, rows)
            return pltpu.make_async_copy(part_ref.at[:, part], buf.at[:, part], sems.at[c])

        for c in range(chunks):
            copy(c).start()
        map_copy.wait()
        bits_copy.wait()
        base = position(dev_ref, sizes)[0] * slots
        groups = [map_ref[base + s] for s in range(slots)]
        for c in range(chunks):
            copy(c).wait()

            def row(i, carry):
                x = c * rows + i
                total = None
                for s in range(slots):
                    sign = (2 * bits_ref[groups[s], x] - 1).astype(F32)
                    term = sign * buf[s, x]
                    total = term if total is None else total + term
                out_ref[x] = total
                return carry

            lax.fori_loop(0, rows, row, 0, unroll=4)

    return pl.pallas_call(
        kernel,
        name="presum",
        compiler_params=PARAMS,
        out_shape=struct(nx, by, bz),
        in_specs=[SMEM, HBM, HBM, HBM],
        out_specs=VMEM,
        scratch_shapes=[
            pltpu.VMEM(partials.shape, F32),
            pltpu.SMEM(group_map.shape, jnp.int32),
            pltpu.SMEM(code_bits.shape, jnp.int32),
            pltpu.SemaphoreType.DMA((chunks + 2,)),
        ],
    )(device, in_hbm(group_map), in_hbm(code_bits), in_hbm(partials))


def position(dev_ref, sizes):
    _, size_y, size_z = sizes
    dev = dev_ref[0]
    return dev // (size_y * size_z), (dev // size_z) % size_y, dev % size_z


def is_even(index):
    return index % 2 == 0


def reduce_pack(device, parts, velocity, sizes):
    bx, by, bz = velocity.shape
    members = sizes[0]

    def kernel(dev_ref, part_ref, v_ref, g_ref, near_ref, other_ref, square_ref):
        even = is_even(position(dev_ref, sizes)[0])
        squares = jnp.zeros((by, bz), F32)
        for i in range(bx):
            total = part_ref[i]
            for m in range(1, members):
                total = total + part_ref[m * bx + i]
            g_ref[i] = total
            squares = squares + total * total
        for i in range(HALO):
            for k, ref in enumerate((g_ref, v_ref)):
                first, last = ref[i], ref[bx - HALO + i]
                near_ref[k * HALO + i] = jnp.where(even, last, first)
                other_ref[k * HALO + i] = jnp.where(even, first, last)
        square_ref[...] = jnp.broadcast_to(jnp.sum(squares, axis=0, keepdims=True), (8, bz))

    edge = struct(2 * HALO, by, bz)
    return pl.pallas_call(
        kernel,
        name="reduce_pack",
        compiler_params=PARAMS,
        out_shape=(struct(bx, by, bz), edge, edge, struct(8, bz)),
        in_specs=[SMEM, VMEM, VMEM],
        out_specs=(VMEM,) * 4,
    )(device, parts, velocity)


def plane_of(main_ref, near_ref, other_ref, even, field, p):
    bx = main_ref.shape[0]
    if p < HALO:
        at = field * HALO + p
        return jnp.where(even, other_ref[at], near_ref[at])
    if p < HALO + bx:
        return main_ref[p - HALO]
    at = field * HALO + p - HALO - bx
    return jnp.where(even, near_ref[at], other_ref[at])


def sublane(shape):
    return lax.broadcasted_iota(jnp.int32, shape, len(shape) - 2)


def lane(shape):
    return lax.broadcasted_iota(jnp.int32, shape, len(shape) - 1)


def pack_y(device, gradient, velocity, halo_x, sizes):
    bx, by, bz = velocity.shape
    pairs = (bx + 2 * HALO) // 2

    def kernel(dev_ref, g_ref, v_ref, nx_ref, ox_ref, near_ref, other_ref):
        even_x, even_y = (is_even(i) for i in position(dev_ref, sizes)[:2])
        low = sublane((8, bz)) < 4
        for field, main in enumerate((g_ref, v_ref)):
            for q in range(pairs):
                left = plane_of(main, nx_ref, ox_ref, even_x, field, 2 * q)
                right = plane_of(main, nx_ref, ox_ref, even_x, field, 2 * q + 1)
                first = jnp.where(low, left[:8], pltpu.roll(right[:8], 4, 0))
                last = jnp.where(low, pltpu.roll(left[by - 8 :], 4, 0), right[by - 8 :])
                near_ref[field * pairs + q] = jnp.where(even_y, last, first)
                other_ref[field * pairs + q] = jnp.where(even_y, first, last)

    edge = struct(2 * pairs, 8, bz)
    return pl.pallas_call(
        kernel,
        name="pack_y",
        compiler_params=PARAMS,
        out_shape=(edge, edge),
        in_specs=[SMEM] + [VMEM] * 4,
        out_specs=(VMEM,) * 2,
    )(device, gradient, velocity, *halo_x)


def rows_of(near_ref, other_ref, even, field, p, pairs):
    near = near_ref[field * pairs + p // 2]
    other = other_ref[field * pairs + p // 2]
    low = sublane(near.shape) < 4
    after = jnp.where(even, near, other)
    before = jnp.where(even, other, near)
    if p % 2 == 0:
        return jnp.where(low, after, pltpu.roll(before, 4, 0))
    return jnp.where(low, pltpu.roll(after, 4, 0), before)


def pack_z(device, gradient, velocity, halo_x, halo_y, sizes):
    bx, by, bz = velocity.shape
    planes = bx + 2 * HALO
    pairs = planes // 2
    groups = bz // 4
    tall = by + 8

    def kernel(dev_ref, g_ref, v_ref, nx_ref, ox_ref, ny_ref, oy_ref, near_ref, other_ref):
        even_x, even_y, even_z = (is_even(i) for i in position(dev_ref, sizes))
        group = lane((tall, bz)) // 4
        for field, main in enumerate((g_ref, v_ref)):
            first = jnp.zeros((tall, bz), F32)
            last = jnp.zeros((tall, bz), F32)
            for p in range(planes):
                own = plane_of(main, nx_ref, ox_ref, even_x, field, p)
                extra = rows_of(ny_ref, oy_ref, even_y, field, p, pairs)
                plane = jnp.concatenate([own, extra], 0)
                turned = pltpu.roll(plane, 4 * p, 1) if p else plane
                first = jnp.where(group == p, turned, first)
                last = jnp.where(group == (p - 1) % groups, turned, last)
            near_ref[pl.ds(field * tall, tall)] = jnp.where(even_z, last, first)
            other_ref[pl.ds(field * tall, tall)] = jnp.where(even_z, first, last)

    edge = struct(2 * tall, bz)
    return pl.pallas_call(
        kernel,
        name="pack_z",
        compiler_params=PARAMS,
        out_shape=(edge, edge),
        in_specs=[SMEM] + [VMEM] * 6,
        out_specs=(VMEM,) * 2,
    )(device, gradient, velocity, *halo_x, *halo_y)


def proximal(device, gradient, velocity, halos, squares, sizes):
    bx, by, bz = velocity.shape
    planes = bx + 2 * HALO
    pairs = planes // 2
    tall = by + 8
    wide = 2 * bz
    size_x, size_y, size_z = sizes
    cells = size_x * bx * size_y * by * size_z * bz

    def kernel(
        dev_ref,
        g_ref,
        v_ref,
        nx_ref,
        ox_ref,
        ny_ref,
        oy_ref,
        nz_ref,
        oz_ref,
        sq_ref,
        gradient_ref,
        model_ref,
        target,
        current,
        extra,
        dual_x,
        dual_y,
        dual_z,
        model,
        sems,
    ):
        gradient_copy = pltpu.make_async_copy(g_ref, gradient_ref, sems.at[0])
        gradient_copy.start()
        pos_x, pos_y, pos_z = position(dev_ref, sizes)
        even_x, even_y, even_z = (is_even(i) for i in (pos_x, pos_y, pos_z))

        total = jnp.sum(sq_ref[0:1], axis=1, keepdims=True)
        scale = step_length * lax.rsqrt(total / cells + 1.0)
        scale = jnp.broadcast_to(scale, (1, bz))

        side_lane = lane((tall, bz)) < bz // 2
        near_z = nz_ref[pl.ds(tall, tall)] - scale * nz_ref[pl.ds(0, tall)]
        other_z = oz_ref[pl.ds(tall, tall)] - scale * oz_ref[pl.ds(0, tall)]
        before_z = jnp.where(even_z, other_z, near_z)
        after_z = jnp.where(even_z, near_z, other_z)
        for p in range(planes):
            own, rows = (
                [
                    plane_of(main, nx_ref, ox_ref, even_x, field, p),
                    rows_of(ny_ref, oy_ref, even_y, field, p, pairs),
                ]
                for field, main in ((1, v_ref), (0, g_ref))
            )
            own, rows = (own[0] - scale * rows[0], own[1] - scale * rows[1])
            back = (bz - 4 * p) % bz
            after = pltpu.roll(after_z, back, 1) if back else after_z
            before = pltpu.roll(before_z, back, 1) if back else before_z
            target[p, pl.ds(0, by), pl.ds(0, bz)] = own
            target[p, pl.ds(by, 8), pl.ds(0, bz)] = rows
            target[p, :, pl.ds(bz, bz)] = jnp.where(side_lane, after, before)

        def factor(index, limit):
            return jnp.where((index >= 0) & (index < limit - 1), dual_step, 0.0).astype(F32)

        row = sublane((tall, 1))
        row = jnp.where(row < by + 4, row, row - tall) + pos_y * by
        factor_y = factor(row, size_y * by)
        col = lane((1, wide))
        col = jnp.where(col < bz + bz // 2, col, col - wide) + pos_z * bz
        factor_z = factor(col, size_z * bz)
        shrink = 1.0 / (1.0 + primal_step)
        gain = primal_step / (1.0 + primal_step)

        for iteration in range(ITERS):
            first = iteration == 0
            final = iteration == ITERS - 1
            here_ref = target if first else extra

            def plane(p, here, before_x, first=first, final=final, here_ref=here_ref):
                ahead = here_ref[p + 1]
                factor_x = factor(pos_x * bx + (p - HALO), size_x * bx)
                dx = factor_x * (ahead - here)
                dy = factor_y * (pltpu.roll(here, tall - 1, 0) - here)
                dz = factor_z * (pltpu.roll(here, wide - 1, 1) - here)
                if not first:
                    dx = dual_x[p] + dx
                    dy = dual_y[p] + dy
                    dz = dual_z[p] + dz
                norm = dx * dx + dy * dy + dz * dz
                ratio = jnp.minimum(1.0, tv_weight * lax.rsqrt(norm))
                dx = dx * ratio
                dy = dy * ratio
                dz = dz * ratio
                if not final:
                    dual_x[p] = dx
                    dual_y[p] = dy
                    dual_z[p] = dz
                if final:
                    if before_x is not None:
                        spread = dx[:by, :bz] - before_x
                        spread += dy[:by, :bz] - pltpu.roll(dy[:, :bz], 1, 0)[:by]
                        spread += dz[:by, :bz] - pltpu.roll(dz[:by], 1, 1)[:, :bz]
                        goal = target[p, pl.ds(0, by), pl.ds(0, bz)]
                        old = current[p, pl.ds(0, by), pl.ds(0, bz)]
                        model[p - HALO] = shrink * old + gain * (spread + goal)
                    return ahead, dx[:by, :bz]
                if before_x is not None:
                    spread = dx - before_x
                    spread += dy - pltpu.roll(dy, 1, 0)
                    spread += dz - pltpu.roll(dz, 1, 1)
                    if first:
                        new = here + gain * spread
                        old = here
                    else:
                        old = current[p]
                        new = shrink * old + gain * (spread + target[p])
                    current[p] = new
                    extra[p] = 2.0 * new - old
                return ahead, dx

            carry = plane(iteration, here_ref[iteration], None)
            rest = planes - 2 - 2 * iteration
            unroll = next(u for u in (5, 6, 4, 2, 1) if rest % u == 0)

            def several(j, carry, plane=plane, start=iteration + 1, unroll=unroll):
                for k in range(unroll):
                    carry = plane(start + j * unroll + k, *carry)
                return carry

            lax.fori_loop(0, rest // unroll, several, carry)
        model_copy = pltpu.make_async_copy(model, model_ref, sems.at[1])
        model_copy.start()
        gradient_copy.wait()
        model_copy.wait()

    field = pltpu.VMEM((planes, tall, wide), F32)
    return pl.pallas_call(
        kernel,
        name="proximal",
        compiler_params=PARAMS,
        out_shape=(struct(bx, by, bz),) * 2,
        in_specs=[SMEM] + [VMEM] * 9,
        out_specs=(HBM,) * 2,
        scratch_shapes=[field] * 6 + [pltpu.VMEM((bx, by, bz), F32), pltpu.SemaphoreType.DMA((2,))],
    )(device, gradient, velocity, *halos, squares)


def shards(partials, code_bits, group_map, velocity):
    sizes = tuple(lax.axis_size(axis) for axis in (GX, GY, "gz"))
    device = lax.axis_index(ALL).astype(jnp.int32).reshape(1)

    local = presum(device, partials, code_bits, group_map, sizes, 8)
    parts = lax.all_to_all(local, GX, split_axis=0, concat_axis=0, tiled=True)
    gradient, *send_x, squares = reduce_pack(device, parts, velocity, sizes)
    halo_x = swap(send_x, GX, GY[1])
    table = jnp.broadcast_to(squares[:1][None], (sizes[0] * sizes[2], 1, squares.shape[1]))
    table = lax.all_to_all(table, XZ, split_axis=0, concat_axis=0, tiled=True)
    send_y = pack_y(device, gradient, velocity, halo_x, sizes)
    halo_y = swap(send_y, GY, "gz")
    column = jnp.broadcast_to(jnp.sum(table, axis=0), squares.shape)
    column = add_pairs(column, GY[1], lambda i, n: i ^ 1)
    column = add_pairs(column, GY[0], lambda i, n: i ^ 1)
    send_z = pack_z(device, gradient, velocity, halo_x, halo_y, sizes)
    halo_z = swap(send_z, "gz", GY[1])
    if lax.axis_size(GY[0]) > 2:
        column = add_pairs(column, GY[0], lambda i, n: n - 1 - i)

    halos = (*halo_x, *halo_y, *halo_z)
    return proximal(device, gradient, velocity, halos, column, sizes)


def solution(mesh):
    torus = Mesh(
        mesh.devices.reshape(4, 2, 4, 2, mesh.shape["gz"]), ("gx_0", "gx_1", "gy_0", "gy_1", "gz")
    )
    placed = (P(GX, None, GY, "gz"), P(), P(), P(GX, GY, "gz"))
    return jax.shard_map(
        shards,
        mesh=torus,
        in_specs=placed,
        out_specs=(P(GX, GY, "gz"), P(GX, GY, "gz")),
        check_vma=False,
    )
```

```python
import jax
import jax.numpy as jnp
from jax import lax
from jax.experimental import pallas as pl
from jax.experimental.pallas import tpu as pltpu
from jax.sharding import Mesh
from jax.sharding import PartitionSpec as P

ITERS = 3
HALO = ITERS
GX = ("gx_0", "gx_1")
GY = ("gy_0", "gy_1")
ALL = GX + GY + ("gz",)

step_length = 0.5
tv_weight = 0.2
dual_step = 0.28
primal_step = 0.28

VMEM = pl.BlockSpec(memory_space=pltpu.VMEM)
SMEM = pl.BlockSpec(memory_space=pltpu.SMEM)
HBM = pl.BlockSpec(memory_space=pltpu.HBM)
PARAMS = pltpu.CompilerParams(vmem_limit_bytes=16 * 1024 * 1024)
F32 = jnp.float32


def swap(blocks, axis, spare):
    size, width = lax.axis_size(axis), lax.axis_size(spare)
    pairs = [(i, i ^ 1) for i in range(size)]
    axes = axis if isinstance(axis, tuple) else (axis,)
    ahead = ALL.index(spare) < ALL.index(axes[0])

    def at(i, k):
        return k * size + i if ahead else i * width + k

    others = []
    for i in range(size):
        j = ((i + 1) ^ 1) - 1
        for k in range(width):
            others.append((at(i, k), at(j, k) if 0 <= j < size else at(i, k ^ 1)))
    both = (spare, *axes) if ahead else (*axes, spare)
    return lax.ppermute(blocks[0], axis, pairs), lax.ppermute(blocks[1], both, others)


def corner_swap(block, odd_y, odd_z):
    axes = (GX[1], *GY, "gz")
    sides, size_y, size_z = (lax.axis_size(axis) for axis in (GX[1], GY, "gz"))

    def partner(i, size, odd):
        j = ((i + 1) ^ 1) - 1 if odd else i ^ 1
        return j if 0 <= j < size else None

    route = []
    for s in range(sides):
        for y in range(size_y):
            for z in range(size_z):
                to_y, to_z = partner(y, size_y, odd_y), partner(z, size_z, odd_z)
                to_s = s ^ 1 if to_y is None and to_z is None else s
                to_y, to_z = (y if to_y is None else to_y), (z if to_z is None else to_z)
                route.append(
                    ((s * size_y + y) * size_z + z, (to_s * size_y + to_y) * size_z + to_z)
                )
    return lax.ppermute(block, axes, route)


def struct(*shape):
    return jax.ShapeDtypeStruct(shape, F32)


def in_hbm(array):
    return pltpu.with_memory_space_constraint(array, pltpu.HBM)


def presum(device, partials, code_bits, group_map, sizes, chunks):
    slots, nx, by, bz = partials.shape
    rows = nx // chunks

    def kernel(dev_ref, map_hbm, bits_hbm, part_ref, out_ref, buf, map_ref, bits_ref, sems):
        map_copy = pltpu.make_async_copy(map_hbm, map_ref, sems.at[chunks])
        bits_copy = pltpu.make_async_copy(bits_hbm, bits_ref, sems.at[chunks + 1])
        map_copy.start()
        bits_copy.start()

        def copy(c):
            part = pl.ds(c * rows, rows)
            return pltpu.make_async_copy(part_ref.at[:, part], buf.at[:, part], sems.at[c])

        for c in range(chunks):
            copy(c).start()
        map_copy.wait()
        bits_copy.wait()
        base = position(dev_ref, sizes)[0] * slots
        groups = [map_ref[base + s] for s in range(slots)]
        for c in range(chunks):
            copy(c).wait()

            def row(i, carry):
                x = c * rows + i
                total = None
                for s in range(slots):
                    sign = (2 * bits_ref[groups[s], x] - 1).astype(F32)
                    term = sign * buf[s, x]
                    total = term if total is None else total + term
                out_ref[x] = total
                return carry

            lax.fori_loop(0, rows, row, 0, unroll=4)

    return pl.pallas_call(
        kernel,
        name="presum",
        compiler_params=PARAMS,
        out_shape=struct(nx, by, bz),
        in_specs=[SMEM, HBM, HBM, HBM],
        out_specs=VMEM,
        scratch_shapes=[
            pltpu.VMEM(partials.shape, F32),
            pltpu.SMEM(group_map.shape, jnp.int32),
            pltpu.SMEM(code_bits.shape, jnp.int32),
            pltpu.SemaphoreType.DMA((chunks + 2,)),
        ],
    )(device, in_hbm(group_map), in_hbm(code_bits), in_hbm(partials))


def position(dev_ref, sizes):
    _, size_y, size_z = sizes
    dev = dev_ref[0]
    return dev // (size_y * size_z), (dev // size_z) % size_y, dev % size_z


def is_even(index):
    return index % 2 == 0


def reduce_pack(device, parts, velocity, sizes):
    bx, by, bz = velocity.shape
    members = sizes[0]

    def kernel(dev_ref, part_ref, v_ref, g_ref, near_ref, other_ref, square_ref):
        even = is_even(position(dev_ref, sizes)[0])
        squares = jnp.zeros((by, bz), F32)
        for i in range(bx):
            total = part_ref[i]
            for m in range(1, members):
                total = total + part_ref[m * bx + i]
            g_ref[i] = total
            squares = squares + total * total
        for i in range(HALO):
            for k, ref in enumerate((g_ref, v_ref)):
                first, last = ref[i], ref[bx - HALO + i]
                near_ref[k * HALO + i] = jnp.where(even, last, first)
                other_ref[k * HALO + i] = jnp.where(even, first, last)
        square_ref[...] = jnp.broadcast_to(jnp.sum(squares, axis=0, keepdims=True), (8, bz))

    edge = struct(2 * HALO, by, bz)
    return pl.pallas_call(
        kernel,
        name="reduce_pack",
        compiler_params=PARAMS,
        out_shape=(struct(bx, by, bz), edge, edge, struct(8, bz)),
        in_specs=[SMEM, VMEM, VMEM],
        out_specs=(VMEM,) * 4,
    )(device, parts, velocity)


def plane_of(main_ref, near_ref, other_ref, even, field, p):
    bx = main_ref.shape[0]
    if p < HALO:
        at = field * HALO + p
        return jnp.where(even, other_ref[at], near_ref[at])
    if p < HALO + bx:
        return main_ref[p - HALO]
    at = field * HALO + p - HALO - bx
    return jnp.where(even, near_ref[at], other_ref[at])


def sublane(shape):
    return lax.broadcasted_iota(jnp.int32, shape, len(shape) - 2)


def lane(shape):
    return lax.broadcasted_iota(jnp.int32, shape, len(shape) - 1)


def pack_y(device, gradient, velocity, halo_x, sizes):
    bx, by, bz = velocity.shape
    pairs = (bx + 2 * HALO) // 2

    def kernel(dev_ref, g_ref, v_ref, nx_ref, ox_ref, near_ref, other_ref):
        even_x, even_y = (is_even(i) for i in position(dev_ref, sizes)[:2])
        low = sublane((8, bz)) < 4
        for field, main in enumerate((g_ref, v_ref)):
            for q in range(pairs):
                left = plane_of(main, nx_ref, ox_ref, even_x, field, 2 * q)
                right = plane_of(main, nx_ref, ox_ref, even_x, field, 2 * q + 1)
                first = jnp.where(low, left[:8], pltpu.roll(right[:8], 4, 0))
                last = jnp.where(low, pltpu.roll(left[by - 8 :], 4, 0), right[by - 8 :])
                near_ref[field * pairs + q] = jnp.where(even_y, last, first)
                other_ref[field * pairs + q] = jnp.where(even_y, first, last)

    edge = struct(2 * pairs, 8, bz)
    return pl.pallas_call(
        kernel,
        name="pack_y",
        compiler_params=PARAMS,
        out_shape=(edge, edge),
        in_specs=[SMEM] + [VMEM] * 4,
        out_specs=(VMEM,) * 2,
    )(device, gradient, velocity, *halo_x)


def rows_of(near_ref, other_ref, even, field, p, pairs):
    near = near_ref[field * pairs + p // 2]
    other = other_ref[field * pairs + p // 2]
    low = sublane(near.shape) < 4
    after = jnp.where(even, near, other)
    before = jnp.where(even, other, near)
    if p % 2 == 0:
        return jnp.where(low, after, pltpu.roll(before, 4, 0))
    return jnp.where(low, pltpu.roll(after, 4, 0), before)


def pack_z(device, gradient, velocity, halo_x, sizes):
    bx, by, bz = velocity.shape
    planes = bx + 2 * HALO
    groups = bz // 4

    def kernel(dev_ref, g_ref, v_ref, nx_ref, ox_ref, near_ref, other_ref, *corner_refs):
        even_x, even_y, even_z = (is_even(i) for i in position(dev_ref, sizes))
        group = lane((by, bz)) // 4
        for field, main in enumerate((g_ref, v_ref)):
            first = jnp.zeros((by, bz), F32)
            last = jnp.zeros((by, bz), F32)
            for p in range(planes):
                plane = plane_of(main, nx_ref, ox_ref, even_x, field, p)
                turned = pltpu.roll(plane, 4 * p, 1) if p else plane
                first = jnp.where(group == p, turned, first)
                last = jnp.where(group == (p - 1) % groups, turned, last)
            near = jnp.where(even_z, last, first)
            other = jnp.where(even_z, first, last)
            near_ref[pl.ds(field * by, by)] = near
            other_ref[pl.ds(field * by, by)] = other
            for k, side in enumerate((near, other)):
                top, bottom = side[:8], side[by - 8 :]
                corner_refs[k][pl.ds(field * 8, 8)] = jnp.where(even_y, bottom, top)
                corner_refs[2 + k][pl.ds(field * 8, 8)] = jnp.where(even_y, top, bottom)

    edge = struct(2 * by, bz)
    return pl.pallas_call(
        kernel,
        name="pack_z",
        compiler_params=PARAMS,
        out_shape=(edge,) * 2 + (struct(16, bz),) * 4,
        in_specs=[SMEM] + [VMEM] * 4,
        out_specs=(VMEM,) * 6,
    )(device, gradient, velocity, *halo_x)


def proximal(device, gradient, velocity, halos, squares, sizes):
    bx, by, bz = velocity.shape
    planes = bx + 2 * HALO
    pairs = planes // 2
    tall = by + 8
    wide = 2 * bz
    size_x, size_y, size_z = sizes
    cells = size_x * bx * size_y * by * size_z * bz

    def kernel(
        dev_ref,
        g_ref,
        v_ref,
        nx_ref,
        ox_ref,
        ny_ref,
        oy_ref,
        nz_ref,
        oz_ref,
        c00_ref,
        c01_ref,
        c10_ref,
        c11_ref,
        sq_ref,
        gradient_ref,
        model_ref,
        target,
        current,
        extra,
        dual_x,
        dual_y,
        dual_z,
        model,
        sems,
    ):
        gradient_copy = pltpu.make_async_copy(g_ref, gradient_ref, sems.at[0])
        gradient_copy.start()
        pos_x, pos_y, pos_z = position(dev_ref, sizes)
        even_x, even_y, even_z = (is_even(i) for i in (pos_x, pos_y, pos_z))

        total = jnp.sum(jnp.sum(sq_ref[...], axis=0), axis=1, keepdims=True)
        scale = step_length * lax.rsqrt(total / cells + 1.0)
        scale = jnp.broadcast_to(scale, (1, bz))

        side_lane = lane((tall, bz)) < bz // 2

        def scaled(ref, rows):
            return ref[pl.ds(rows, rows)] - scale * ref[pl.ds(0, rows)]

        def tall_edge(ref, near_corner, other_corner):
            near, other = scaled(near_corner, 8), scaled(other_corner, 8)
            after = jnp.where(even_y, near, other)
            before = jnp.where(even_y, other, near)
            extra = jnp.where(sublane((8, bz)) < 4, after, before)
            return jnp.concatenate([scaled(ref, by), extra], 0)

        near_z = tall_edge(nz_ref, c00_ref, c10_ref)
        other_z = tall_edge(oz_ref, c01_ref, c11_ref)
        before_z = jnp.where(even_z, other_z, near_z)
        after_z = jnp.where(even_z, near_z, other_z)
        for p in range(planes):
            own, rows = (
                [
                    plane_of(main, nx_ref, ox_ref, even_x, field, p),
                    rows_of(ny_ref, oy_ref, even_y, field, p, pairs),
                ]
                for field, main in ((1, v_ref), (0, g_ref))
            )
            own, rows = (own[0] - scale * rows[0], own[1] - scale * rows[1])
            back = (bz - 4 * p) % bz
            after = pltpu.roll(after_z, back, 1) if back else after_z
            before = pltpu.roll(before_z, back, 1) if back else before_z
            target[p, pl.ds(0, by), pl.ds(0, bz)] = own
            target[p, pl.ds(by, 8), pl.ds(0, bz)] = rows
            target[p, :, pl.ds(bz, bz)] = jnp.where(side_lane, after, before)

        def factor(index, limit):
            return jnp.where((index >= 0) & (index < limit - 1), dual_step, 0.0).astype(F32)

        row = sublane((tall, 1))
        row = jnp.where(row < by + 4, row, row - tall) + pos_y * by
        factor_y = factor(row, size_y * by)
        col = lane((1, wide))
        col = jnp.where(col < bz + bz // 2, col, col - wide) + pos_z * bz
        factor_z = factor(col, size_z * bz)
        shrink = 1.0 / (1.0 + primal_step)
        gain = primal_step / (1.0 + primal_step)

        for iteration in range(ITERS):
            first = iteration == 0
            final = iteration == ITERS - 1
            here_ref = target if first else extra
            ahead = here_ref[iteration]
            before_x = None
            for p in range(iteration, planes - 1 - iteration):
                here = ahead
                ahead = here_ref[p + 1]
                index = pos_x * bx + (p - HALO)
                factor_x = factor(index, size_x * bx)
                dx = factor_x * (ahead - here)
                dy = factor_y * (pltpu.roll(here, tall - 1, 0) - here)
                dz = factor_z * (pltpu.roll(here, wide - 1, 1) - here)
                if not first:
                    dx = dual_x[p] + dx
                    dy = dual_y[p] + dy
                    dz = dual_z[p] + dz
                norm = dx * dx + dy * dy + dz * dz
                ratio = jnp.minimum(1.0, tv_weight * lax.rsqrt(norm))
                dx = dx * ratio
                dy = dy * ratio
                dz = dz * ratio
                if not final:
                    dual_x[p] = dx
                    dual_y[p] = dy
                    dual_z[p] = dz
                if p > iteration:
                    if final:
                        spread = dx[:by, :bz] - before_x
                        spread += dy[:by, :bz] - pltpu.roll(dy[:, :bz], 1, 0)[:by]
                        spread += dz[:by, :bz] - pltpu.roll(dz[:by], 1, 1)[:, :bz]
                        goal = target[p, pl.ds(0, by), pl.ds(0, bz)]
                        old = current[p, pl.ds(0, by), pl.ds(0, bz)]
                        model[p - HALO] = shrink * old + gain * (spread + goal)
                    else:
                        spread = dx - before_x
                        spread += dy - pltpu.roll(dy, 1, 0)
                        spread += dz - pltpu.roll(dz, 1, 1)
                        if first:
                            new = here + gain * spread
                            old = here
                        else:
                            old = current[p]
                            new = shrink * old + gain * (spread + target[p])
                        current[p] = new
                        extra[p] = 2.0 * new - old
                before_x = dx[:by, :bz] if final else dx
        model_copy = pltpu.make_async_copy(model, model_ref, sems.at[1])
        model_copy.start()
        gradient_copy.wait()
        model_copy.wait()

    field = pltpu.VMEM((planes, tall, wide), F32)
    return pl.pallas_call(
        kernel,
        name="proximal",
        compiler_params=PARAMS,
        out_shape=(struct(bx, by, bz),) * 2,
        in_specs=[SMEM] + [VMEM] * 13,
        out_specs=(HBM,) * 2,
        scratch_shapes=[field] * 6 + [pltpu.VMEM((bx, by, bz), F32), pltpu.SemaphoreType.DMA((2,))],
    )(device, gradient, velocity, *halos, squares)


def shards(partials, code_bits, group_map, velocity):
    sizes = tuple(lax.axis_size(axis) for axis in (GX, GY, "gz"))
    device = lax.axis_index(ALL).astype(jnp.int32).reshape(1)

    local = presum(device, partials, code_bits, group_map, sizes, 8)
    parts = lax.all_to_all(local, GX, split_axis=0, concat_axis=0, tiled=True)
    gradient, *send_x, squares = reduce_pack(device, parts, velocity, sizes)
    halo_x = swap(send_x, GX, GY[1])
    table = jnp.broadcast_to(
        squares[:1][None], (sizes[0] * sizes[1] * sizes[2], 1, squares.shape[1])
    )
    table = lax.all_to_all(table, ALL, split_axis=0, concat_axis=0, tiled=True)
    send_y = pack_y(device, gradient, velocity, halo_x, sizes)
    halo_y = swap(send_y, GY, "gz")
    *send_z, c00, c01, c10, c11 = pack_z(device, gradient, velocity, halo_x, sizes)
    halo_z = swap(send_z, "gz", GY[1])
    corners = (
        corner_swap(c00, False, False),
        corner_swap(c01, False, True),
        corner_swap(c10, True, False),
        corner_swap(c11, True, True),
    )

    halos = (*halo_x, *halo_y, *halo_z, *corners)
    return proximal(device, gradient, velocity, halos, table, sizes)


def solution(mesh):
    torus = Mesh(
        mesh.devices.reshape(4, 2, 4, 2, mesh.shape["gz"]), ("gx_0", "gx_1", "gy_0", "gy_1", "gz")
    )
    placed = (P(GX, None, GY, "gz"), P(), P(), P(GX, GY, "gz"))
    return jax.shard_map(
        shards,
        mesh=torus,
        in_specs=placed,
        out_specs=(P(GX, GY, "gz"), P(GX, GY, "gz")),
        check_vma=False,
    )
```

```python
import jax
import jax.numpy as jnp
from jax import lax
from jax.experimental import pallas as pl
from jax.experimental.pallas import tpu as pltpu
from jax.sharding import Mesh
from jax.sharding import PartitionSpec as P

ITERS = 3
HALO = ITERS
GX = ("gx_0", "gx_1")
GY = ("gy_0", "gy_1")
ALL = GX + GY + ("gz",)

step_length = 0.5
tv_weight = 0.2
dual_step = 0.28
primal_step = 0.28

VMEM = pl.BlockSpec(memory_space=pltpu.VMEM)
SMEM = pl.BlockSpec(memory_space=pltpu.SMEM)
HBM = pl.BlockSpec(memory_space=pltpu.HBM)
PARAMS = pltpu.CompilerParams(vmem_limit_bytes=16 * 1024 * 1024)
F32 = jnp.float32


def swap(blocks, axis, spare):
    size, width = lax.axis_size(axis), lax.axis_size(spare)
    pairs = [(i, i ^ 1) for i in range(size)]
    axes = axis if isinstance(axis, tuple) else (axis,)
    ahead = ALL.index(spare) < ALL.index(axes[0])

    def at(i, k):
        return k * size + i if ahead else i * width + k

    others = []
    for i in range(size):
        j = ((i + 1) ^ 1) - 1
        for k in range(width):
            others.append((at(i, k), at(j, k) if 0 <= j < size else at(i, k ^ 1)))
    both = (spare, *axes) if ahead else (*axes, spare)
    return lax.ppermute(blocks[0], axis, pairs), lax.ppermute(blocks[1], both, others)


def struct(*shape):
    return jax.ShapeDtypeStruct(shape, F32)


def in_hbm(array):
    return pltpu.with_memory_space_constraint(array, pltpu.HBM)


def presum(device, partials, code_bits, group_map, sizes, chunks):
    slots, nx, by, bz = partials.shape
    rows = nx // chunks

    def kernel(dev_ref, map_hbm, bits_hbm, part_ref, out_ref, buf, map_ref, bits_ref, sems):
        map_copy = pltpu.make_async_copy(map_hbm, map_ref, sems.at[chunks])
        bits_copy = pltpu.make_async_copy(bits_hbm, bits_ref, sems.at[chunks + 1])
        map_copy.start()
        bits_copy.start()

        def copy(c):
            part = pl.ds(c * rows, rows)
            return pltpu.make_async_copy(part_ref.at[:, part], buf.at[:, part], sems.at[c])

        for c in range(chunks):
            copy(c).start()
        map_copy.wait()
        bits_copy.wait()
        base = position(dev_ref, sizes)[0] * slots
        groups = [map_ref[base + s] for s in range(slots)]
        for c in range(chunks):
            copy(c).wait()

            def row(i, carry):
                x = c * rows + i
                total = None
                for s in range(slots):
                    sign = (2 * bits_ref[groups[s], x] - 1).astype(F32)
                    term = sign * buf[s, x]
                    total = term if total is None else total + term
                out_ref[x] = total
                return carry

            lax.fori_loop(0, rows, row, 0, unroll=4)

    return pl.pallas_call(
        kernel,
        name="presum",
        compiler_params=PARAMS,
        out_shape=struct(nx, by, bz),
        in_specs=[SMEM, HBM, HBM, HBM],
        out_specs=VMEM,
        scratch_shapes=[
            pltpu.VMEM(partials.shape, F32),
            pltpu.SMEM(group_map.shape, jnp.int32),
            pltpu.SMEM(code_bits.shape, jnp.int32),
            pltpu.SemaphoreType.DMA((chunks + 2,)),
        ],
    )(device, in_hbm(group_map), in_hbm(code_bits), in_hbm(partials))


def position(dev_ref, sizes):
    _, size_y, size_z = sizes
    dev = dev_ref[0]
    return dev // (size_y * size_z), (dev // size_z) % size_y, dev % size_z


def is_even(index):
    return index % 2 == 0


def reduce_pack(device, parts, velocity, sizes):
    bx, by, bz = velocity.shape
    members = sizes[0]

    def kernel(dev_ref, part_ref, v_ref, g_ref, near_ref, other_ref, square_ref):
        even = is_even(position(dev_ref, sizes)[0])
        squares = jnp.zeros((by, bz), F32)
        for i in range(bx):
            total = part_ref[i]
            for m in range(1, members):
                total = total + part_ref[m * bx + i]
            g_ref[i] = total
            squares = squares + total * total
        for i in range(HALO):
            for k, ref in enumerate((g_ref, v_ref)):
                first, last = ref[i], ref[bx - HALO + i]
                near_ref[k * HALO + i] = jnp.where(even, last, first)
                other_ref[k * HALO + i] = jnp.where(even, first, last)
        square_ref[...] = jnp.broadcast_to(jnp.sum(squares, axis=0, keepdims=True), (8, bz))

    edge = struct(2 * HALO, by, bz)
    return pl.pallas_call(
        kernel,
        name="reduce_pack",
        compiler_params=PARAMS,
        out_shape=(struct(bx, by, bz), edge, edge, struct(8, bz)),
        in_specs=[SMEM, VMEM, VMEM],
        out_specs=(VMEM,) * 4,
    )(device, parts, velocity)


def plane_of(main_ref, near_ref, other_ref, even, field, p):
    bx = main_ref.shape[0]
    if p < HALO:
        at = field * HALO + p
        return jnp.where(even, other_ref[at], near_ref[at])
    if p < HALO + bx:
        return main_ref[p - HALO]
    at = field * HALO + p - HALO - bx
    return jnp.where(even, near_ref[at], other_ref[at])


def sublane(shape):
    return lax.broadcasted_iota(jnp.int32, shape, len(shape) - 2)


def lane(shape):
    return lax.broadcasted_iota(jnp.int32, shape, len(shape) - 1)


def pack_y(device, gradient, velocity, halo_x, sizes):
    bx, by, bz = velocity.shape
    pairs = (bx + 2 * HALO) // 2

    def kernel(dev_ref, g_ref, v_ref, nx_ref, ox_ref, near_ref, other_ref):
        even_x, even_y = (is_even(i) for i in position(dev_ref, sizes)[:2])
        low = sublane((8, bz)) < 4
        for field, main in enumerate((g_ref, v_ref)):
            for q in range(pairs):
                left = plane_of(main, nx_ref, ox_ref, even_x, field, 2 * q)
                right = plane_of(main, nx_ref, ox_ref, even_x, field, 2 * q + 1)
                first = jnp.where(low, left[:8], pltpu.roll(right[:8], 4, 0))
                last = jnp.where(low, pltpu.roll(left[by - 8 :], 4, 0), right[by - 8 :])
                near_ref[field * pairs + q] = jnp.where(even_y, last, first)
                other_ref[field * pairs + q] = jnp.where(even_y, first, last)

    edge = struct(2 * pairs, 8, bz)
    return pl.pallas_call(
        kernel,
        name="pack_y",
        compiler_params=PARAMS,
        out_shape=(edge, edge),
        in_specs=[SMEM] + [VMEM] * 4,
        out_specs=(VMEM,) * 2,
    )(device, gradient, velocity, *halo_x)


def rows_of(near_ref, other_ref, even, field, p, pairs):
    near = near_ref[field * pairs + p // 2]
    other = other_ref[field * pairs + p // 2]
    low = sublane(near.shape) < 4
    after = jnp.where(even, near, other)
    before = jnp.where(even, other, near)
    if p % 2 == 0:
        return jnp.where(low, after, pltpu.roll(before, 4, 0))
    return jnp.where(low, pltpu.roll(after, 4, 0), before)


def pack_lanes(device, gradient, velocity, halo_x, sizes):
    bx, by, bz = velocity.shape
    planes = bx + 2 * HALO
    groups = bz // 4

    def kernel(dev_ref, g_ref, v_ref, nx_ref, ox_ref, first_ref, last_ref, near_ref, other_ref):
        even_x, even_y = (is_even(i) for i in position(dev_ref, sizes)[:2])
        group = lane((by, bz)) // 4
        for field, main in enumerate((g_ref, v_ref)):
            first = jnp.zeros((by, bz), F32)
            last = jnp.zeros((by, bz), F32)
            for p in range(planes):
                plane = plane_of(main, nx_ref, ox_ref, even_x, field, p)
                turned = pltpu.roll(plane, 4 * p, 1) if p else plane
                first = jnp.where(group == p, turned, first)
                last = jnp.where(group == (p - 1) % groups, turned, last)
            first_ref[pl.ds(field * by, by)] = first
            last_ref[pl.ds(field * by, by)] = last
            for k, packed in enumerate((first, last)):
                top, bottom = packed[:8], packed[by - 8 :]
                near_ref[2 * field + k] = jnp.where(even_y, bottom, top)
                other_ref[2 * field + k] = jnp.where(even_y, top, bottom)

    own = struct(2 * by, bz)
    edge = struct(4, 8, bz)
    return pl.pallas_call(
        kernel,
        name="pack_lanes",
        compiler_params=PARAMS,
        out_shape=(own, own, edge, edge),
        in_specs=[SMEM] + [VMEM] * 4,
        out_specs=(VMEM,) * 4,
    )(device, gradient, velocity, *halo_x)


def pack_z(device, first, last, corners, sizes):
    rows, bz = first.shape
    by = rows // 2
    tall = by + 8

    def kernel(dev_ref, first_ref, last_ref, nc_ref, oc_ref, near_ref, other_ref):
        even_y, even_z = (is_even(i) for i in position(dev_ref, sizes)[1:])
        low = sublane((8, bz)) < 4
        for field in range(2):
            both = []
            for k, ref in enumerate((first_ref, last_ref)):
                near, other = nc_ref[2 * field + k], oc_ref[2 * field + k]
                after = jnp.where(even_y, near, other)
                before = jnp.where(even_y, other, near)
                extra = jnp.where(low, after, before)
                both.append(jnp.concatenate([ref[pl.ds(field * by, by)], extra], 0))
            near_ref[pl.ds(field * tall, tall)] = jnp.where(even_z, both[1], both[0])
            other_ref[pl.ds(field * tall, tall)] = jnp.where(even_z, both[0], both[1])

    edge = struct(2 * tall, bz)
    return pl.pallas_call(
        kernel,
        name="pack_z",
        compiler_params=PARAMS,
        out_shape=(edge, edge),
        in_specs=[SMEM] + [VMEM] * 4,
        out_specs=(VMEM,) * 2,
    )(device, first, last, *corners)


def proximal(device, gradient, velocity, halos, squares, sizes):
    bx, by, bz = velocity.shape
    planes = bx + 2 * HALO
    pairs = planes // 2
    tall = by + 8
    wide = 2 * bz
    size_x, size_y, size_z = sizes
    cells = size_x * bx * size_y * by * size_z * bz

    def kernel(
        dev_ref,
        g_ref,
        v_ref,
        nx_ref,
        ox_ref,
        ny_ref,
        oy_ref,
        nz_ref,
        oz_ref,
        sq_ref,
        gradient_ref,
        model_ref,
        target,
        current,
        extra,
        dual_x,
        dual_y,
        dual_z,
        model,
        sems,
    ):
        gradient_copy = pltpu.make_async_copy(g_ref, gradient_ref, sems.at[0])
        gradient_copy.start()
        pos_x, pos_y, pos_z = position(dev_ref, sizes)
        even_x, even_y, even_z = (is_even(i) for i in (pos_x, pos_y, pos_z))

        total = jnp.sum(jnp.sum(sq_ref[...], axis=0), axis=1, keepdims=True)
        scale = step_length * lax.rsqrt(total / cells + 1.0)
        scale = jnp.broadcast_to(scale, (1, bz))

        side_lane = lane((tall, bz)) < bz // 2
        near_z = nz_ref[pl.ds(tall, tall)] - scale * nz_ref[pl.ds(0, tall)]
        other_z = oz_ref[pl.ds(tall, tall)] - scale * oz_ref[pl.ds(0, tall)]
        before_z = jnp.where(even_z, other_z, near_z)
        after_z = jnp.where(even_z, near_z, other_z)
        for p in range(planes):
            own, rows = (
                [
                    plane_of(main, nx_ref, ox_ref, even_x, field, p),
                    rows_of(ny_ref, oy_ref, even_y, field, p, pairs),
                ]
                for field, main in ((1, v_ref), (0, g_ref))
            )
            own, rows = (own[0] - scale * rows[0], own[1] - scale * rows[1])
            back = (bz - 4 * p) % bz
            after = pltpu.roll(after_z, back, 1) if back else after_z
            before = pltpu.roll(before_z, back, 1) if back else before_z
            target[p, pl.ds(0, by), pl.ds(0, bz)] = own
            target[p, pl.ds(by, 8), pl.ds(0, bz)] = rows
            target[p, :, pl.ds(bz, bz)] = jnp.where(side_lane, after, before)

        def factor(index, limit):
            return jnp.where((index >= 0) & (index < limit - 1), dual_step, 0.0).astype(F32)

        row = sublane((tall, 1))
        row = jnp.where(row < by + 4, row, row - tall) + pos_y * by
        factor_y = factor(row, size_y * by)
        col = lane((1, wide))
        col = jnp.where(col < bz + bz // 2, col, col - wide) + pos_z * bz
        factor_z = factor(col, size_z * bz)
        shrink = 1.0 / (1.0 + primal_step)
        gain = primal_step / (1.0 + primal_step)

        for iteration in range(ITERS):
            first = iteration == 0
            final = iteration == ITERS - 1
            here_ref = target if first else extra

            def plane(p, here, before_x, first=first, final=final, here_ref=here_ref):
                ahead = here_ref[p + 1]
                factor_x = factor(pos_x * bx + (p - HALO), size_x * bx)
                dx = factor_x * (ahead - here)
                dy = factor_y * (pltpu.roll(here, tall - 1, 0) - here)
                dz = factor_z * (pltpu.roll(here, wide - 1, 1) - here)
                if not first:
                    dx = dual_x[p] + dx
                    dy = dual_y[p] + dy
                    dz = dual_z[p] + dz
                norm = dx * dx + dy * dy + dz * dz
                ratio = jnp.minimum(1.0, tv_weight * lax.rsqrt(norm))
                dx = dx * ratio
                dy = dy * ratio
                dz = dz * ratio
                if not final:
                    dual_x[p] = dx
                    dual_y[p] = dy
                    dual_z[p] = dz
                if final:
                    if before_x is not None:
                        spread = dx[:by, :bz] - before_x
                        spread += dy[:by, :bz] - pltpu.roll(dy[:, :bz], 1, 0)[:by]
                        spread += dz[:by, :bz] - pltpu.roll(dz[:by], 1, 1)[:, :bz]
                        goal = target[p, pl.ds(0, by), pl.ds(0, bz)]
                        old = current[p, pl.ds(0, by), pl.ds(0, bz)]
                        model[p - HALO] = shrink * old + gain * (spread + goal)
                    return ahead, dx[:by, :bz]
                if before_x is not None:
                    spread = dx - before_x
                    spread += dy - pltpu.roll(dy, 1, 0)
                    spread += dz - pltpu.roll(dz, 1, 1)
                    if first:
                        new = here + gain * spread
                        old = here
                    else:
                        old = current[p]
                        new = shrink * old + gain * (spread + target[p])
                    current[p] = new
                    extra[p] = 2.0 * new - old
                return ahead, dx

            carry = plane(iteration, here_ref[iteration], None)
            rest = planes - 2 - 2 * iteration
            unroll = next(u for u in (5, 6, 4, 2, 1) if rest % u == 0)

            def several(j, carry, plane=plane, start=iteration + 1, unroll=unroll):
                for k in range(unroll):
                    carry = plane(start + j * unroll + k, *carry)
                return carry

            lax.fori_loop(0, rest // unroll, several, carry)
        model_copy = pltpu.make_async_copy(model, model_ref, sems.at[1])
        model_copy.start()
        gradient_copy.wait()
        model_copy.wait()

    field = pltpu.VMEM((planes, tall, wide), F32)
    return pl.pallas_call(
        kernel,
        name="proximal",
        compiler_params=PARAMS,
        out_shape=(struct(bx, by, bz),) * 2,
        in_specs=[SMEM] + [VMEM] * 9,
        out_specs=(HBM,) * 2,
        scratch_shapes=[field] * 6 + [pltpu.VMEM((bx, by, bz), F32), pltpu.SemaphoreType.DMA((2,))],
    )(device, gradient, velocity, *halos, squares)


def shards(partials, code_bits, group_map, velocity):
    sizes = tuple(lax.axis_size(axis) for axis in (GX, GY, "gz"))
    device = lax.axis_index(ALL).astype(jnp.int32).reshape(1)

    local = presum(device, partials, code_bits, group_map, sizes, 16)
    parts = lax.all_to_all(local, GX, split_axis=0, concat_axis=0, tiled=True)
    gradient, *send_x, squares = reduce_pack(device, parts, velocity, sizes)
    halo_x = swap(send_x, GX, GY[1])
    table = jnp.broadcast_to(
        squares[:1][None], (sizes[0] * sizes[1] * sizes[2], 1, squares.shape[1])
    )
    table = lax.all_to_all(table, ALL, split_axis=0, concat_axis=0, tiled=True)
    first, last, *send_corners = pack_lanes(device, gradient, velocity, halo_x, sizes)
    corners = swap(send_corners, GY, "gz")
    send_y = pack_y(device, gradient, velocity, halo_x, sizes)
    halo_y = swap(send_y, GY, "gz")

    send_z = pack_z(device, first, last, corners, sizes)
    halo_z = swap(send_z, "gz", GY[1])

    halos = (*halo_x, *halo_y, *halo_z)
    return proximal(device, gradient, velocity, halos, table, sizes)


def solution(mesh):
    torus = Mesh(
        mesh.devices.reshape(4, 2, 4, 2, mesh.shape["gz"]), ("gx_0", "gx_1", "gy_0", "gy_1", "gz")
    )
    placed = (P(GX, None, GY, "gz"), P(), P(), P(GX, GY, "gz"))
    return jax.shard_map(
        shards,
        mesh=torus,
        in_specs=placed,
        out_specs=(P(GX, GY, "gz"), P(GX, GY, "gz")),
        check_vma=False,
    )
```

```python
import jax
import jax.numpy as jnp
from jax import lax
from jax.experimental import pallas as pl
from jax.experimental.pallas import tpu as pltpu
from jax.sharding import Mesh
from jax.sharding import PartitionSpec as P

ITERS = 3
HALO = ITERS
GX = ("gx_0", "gx_1")
GY = ("gy_0", "gy_1")
ALL = GX + GY + ("gz",)

step_length = 0.5
tv_weight = 0.2
dual_step = 0.28
primal_step = 0.28

VMEM = pl.BlockSpec(memory_space=pltpu.VMEM)
SMEM = pl.BlockSpec(memory_space=pltpu.SMEM)
HBM = pl.BlockSpec(memory_space=pltpu.HBM)
PARAMS = pltpu.CompilerParams(vmem_limit_bytes=16 * 1024 * 1024)
F32 = jnp.float32


def swap(blocks, axis, spare):
    size, width = lax.axis_size(axis), lax.axis_size(spare)
    pairs = [(i, i ^ 1) for i in range(size)]
    axes = axis if isinstance(axis, tuple) else (axis,)
    ahead = ALL.index(spare) < ALL.index(axes[0])

    def at(i, k):
        return k * size + i if ahead else i * width + k

    others = []
    for i in range(size):
        j = ((i + 1) ^ 1) - 1
        for k in range(width):
            others.append((at(i, k), at(j, k) if 0 <= j < size else at(i, k ^ 1)))
    both = (spare, *axes) if ahead else (*axes, spare)
    near = lax.ppermute(blocks[0], axis, pairs)
    other = lax.ppermute(blocks[1], both, others)
    return near, other


def struct(*shape):
    return jax.ShapeDtypeStruct(shape, F32)


def in_hbm(array):
    return pltpu.with_memory_space_constraint(array, pltpu.HBM)


def presum(device, partials, code_bits, group_map, sizes, chunks):
    slots, nx, by, bz = partials.shape
    rows = nx // chunks

    def kernel(dev_ref, map_hbm, bits_hbm, part_ref, out_ref, buf, map_ref, bits_ref, sems):
        map_copy = pltpu.make_async_copy(map_hbm, map_ref, sems.at[chunks])
        bits_copy = pltpu.make_async_copy(bits_hbm, bits_ref, sems.at[chunks + 1])
        map_copy.start()
        bits_copy.start()

        def copy(c):
            part = pl.ds(c * rows, rows)
            return pltpu.make_async_copy(part_ref.at[:, part], buf.at[:, part], sems.at[c])

        for c in range(chunks):
            copy(c).start()
        map_copy.wait()
        bits_copy.wait()
        base = position(dev_ref, sizes)[0] * slots
        groups = [map_ref[base + s] for s in range(slots)]
        for c in range(chunks):
            copy(c).wait()

            def row(i, carry):
                x = c * rows + i
                total = None
                for s in range(slots):
                    sign = (2 * bits_ref[groups[s], x] - 1).astype(F32)
                    term = sign * buf[s, x]
                    total = term if total is None else total + term
                out_ref[x] = total
                return carry

            lax.fori_loop(0, rows, row, 0, unroll=4)

    return pl.pallas_call(
        kernel,
        name="presum",
        compiler_params=PARAMS,
        out_shape=struct(nx, by, bz),
        in_specs=[SMEM, HBM, HBM, HBM],
        out_specs=VMEM,
        scratch_shapes=[
            pltpu.VMEM(partials.shape, F32),
            pltpu.SMEM(group_map.shape, jnp.int32),
            pltpu.SMEM(code_bits.shape, jnp.int32),
            pltpu.SemaphoreType.DMA((chunks + 2,)),
        ],
    )(device, in_hbm(group_map), in_hbm(code_bits), in_hbm(partials))


def position(dev_ref, sizes):
    _, size_y, size_z = sizes
    dev = dev_ref[0]
    return dev // (size_y * size_z), (dev // size_z) % size_y, dev % size_z


def is_even(index):
    return index % 2 == 0


def reduce_pack(device, parts, velocity, sizes):
    bx, by, bz = velocity.shape
    members = sizes[0]

    def kernel(dev_ref, part_ref, v_ref, g_ref, near_ref, other_ref, square_ref):
        even = is_even(position(dev_ref, sizes)[0])
        squares = jnp.zeros((by, bz), F32)
        for i in range(bx):
            total = part_ref[i]
            for m in range(1, members):
                total = total + part_ref[m * bx + i]
            g_ref[i] = total
            squares = squares + total * total
        for i in range(HALO):
            for k, ref in enumerate((g_ref, v_ref)):
                first, last = ref[i], ref[bx - HALO + i]
                near_ref[k * HALO + i] = jnp.where(even, last, first)
                other_ref[k * HALO + i] = jnp.where(even, first, last)
        square_ref[...] = jnp.broadcast_to(jnp.sum(squares, axis=0, keepdims=True), (8, bz))

    edge = struct(2 * HALO, by, bz)
    return pl.pallas_call(
        kernel,
        name="reduce_pack",
        compiler_params=PARAMS,
        out_shape=(struct(bx, by, bz), edge, edge, struct(8, bz)),
        in_specs=[SMEM, VMEM, VMEM],
        out_specs=(VMEM,) * 4,
    )(device, parts, velocity)


def plane_of(main_ref, near_ref, other_ref, even, field, p):
    bx = main_ref.shape[0]
    if p < HALO:
        at = field * HALO + p
        return jnp.where(even, other_ref[at], near_ref[at])
    if p < HALO + bx:
        return main_ref[p - HALO]
    at = field * HALO + p - HALO - bx
    return jnp.where(even, near_ref[at], other_ref[at])


def sublane(shape):
    return lax.broadcasted_iota(jnp.int32, shape, len(shape) - 2)


def lane(shape):
    return lax.broadcasted_iota(jnp.int32, shape, len(shape) - 1)


def pack_y(device, gradient, velocity, halo_x, sizes):
    bx, by, bz = velocity.shape
    pairs = (bx + 2 * HALO) // 2

    def kernel(dev_ref, g_ref, v_ref, nx_ref, ox_ref, near_ref, other_ref):
        even_x, even_y = (is_even(i) for i in position(dev_ref, sizes)[:2])
        low = sublane((8, bz)) < 4
        for field, main in enumerate((g_ref, v_ref)):
            for q in range(pairs):
                left = plane_of(main, nx_ref, ox_ref, even_x, field, 2 * q)
                right = plane_of(main, nx_ref, ox_ref, even_x, field, 2 * q + 1)
                first = jnp.where(low, left[:8], pltpu.roll(right[:8], 4, 0))
                last = jnp.where(low, pltpu.roll(left[by - 8 :], 4, 0), right[by - 8 :])
                near_ref[field * pairs + q] = jnp.where(even_y, last, first)
                other_ref[field * pairs + q] = jnp.where(even_y, first, last)

    edge = struct(2 * pairs, 8, bz)
    return pl.pallas_call(
        kernel,
        name="pack_y",
        compiler_params=PARAMS,
        out_shape=(edge, edge),
        in_specs=[SMEM] + [VMEM] * 4,
        out_specs=(VMEM,) * 2,
    )(device, gradient, velocity, *halo_x)


def rows_of(near_ref, other_ref, even, field, p, pairs):
    near = near_ref[field * pairs + p // 2]
    other = other_ref[field * pairs + p // 2]
    low = sublane(near.shape) < 4
    after = jnp.where(even, near, other)
    before = jnp.where(even, other, near)
    if p % 2 == 0:
        return jnp.where(low, after, pltpu.roll(before, 4, 0))
    return jnp.where(low, pltpu.roll(after, 4, 0), before)


def pack_lanes(device, gradient, velocity, halo_x, sizes):
    bx, by, bz = velocity.shape
    planes = bx + 2 * HALO
    groups = bz // 4

    def kernel(dev_ref, g_ref, v_ref, nx_ref, ox_ref, first_ref, last_ref, near_ref, other_ref):
        even_x, even_y = (is_even(i) for i in position(dev_ref, sizes)[:2])
        group = lane((by, bz)) // 4
        for field, main in enumerate((g_ref, v_ref)):
            first = jnp.zeros((by, bz), F32)
            last = jnp.zeros((by, bz), F32)
            for p in range(planes):
                plane = plane_of(main, nx_ref, ox_ref, even_x, field, p)
                turned = pltpu.roll(plane, 4 * p, 1) if p else plane
                first = jnp.where(group == p, turned, first)
                last = jnp.where(group == (p - 1) % groups, turned, last)
            first_ref[pl.ds(field * by, by)] = first
            last_ref[pl.ds(field * by, by)] = last
            for k, packed in enumerate((first, last)):
                top, bottom = packed[:8], packed[by - 8 :]
                near_ref[2 * field + k] = jnp.where(even_y, bottom, top)
                other_ref[2 * field + k] = jnp.where(even_y, top, bottom)

    own = struct(2 * by, bz)
    edge = struct(4, 8, bz)
    return pl.pallas_call(
        kernel,
        name="pack_lanes",
        compiler_params=PARAMS,
        out_shape=(own, own, edge, edge),
        in_specs=[SMEM] + [VMEM] * 4,
        out_specs=(VMEM,) * 4,
    )(device, gradient, velocity, *halo_x)


def pack_z(device, first, last, corners, sizes):
    rows, bz = first.shape
    by = rows // 2
    tall = by + 8

    def kernel(dev_ref, first_ref, last_ref, nc_ref, oc_ref, near_ref, other_ref):
        even_y, even_z = (is_even(i) for i in position(dev_ref, sizes)[1:])
        low = sublane((8, bz)) < 4
        for field in range(2):
            both = []
            for k, ref in enumerate((first_ref, last_ref)):
                near, other = nc_ref[2 * field + k], oc_ref[2 * field + k]
                after = jnp.where(even_y, near, other)
                before = jnp.where(even_y, other, near)
                extra = jnp.where(low, after, before)
                both.append(jnp.concatenate([ref[pl.ds(field * by, by)], extra], 0))
            near_ref[pl.ds(field * tall, tall)] = jnp.where(even_z, both[1], both[0])
            other_ref[pl.ds(field * tall, tall)] = jnp.where(even_z, both[0], both[1])

    edge = struct(2 * tall, bz)
    return pl.pallas_call(
        kernel,
        name="pack_z",
        compiler_params=PARAMS,
        out_shape=(edge, edge),
        in_specs=[SMEM] + [VMEM] * 4,
        out_specs=(VMEM,) * 2,
    )(device, first, last, *corners)


def proximal(device, gradient, velocity, halos, squares, sizes):
    bx, by, bz = velocity.shape
    planes = bx + 2 * HALO
    pairs = planes // 2
    tall = by + 8
    wide = 2 * bz
    size_x, size_y, size_z = sizes
    cells = size_x * bx * size_y * by * size_z * bz

    def kernel(
        dev_ref,
        g_ref,
        v_ref,
        nx_ref,
        ox_ref,
        ny_ref,
        oy_ref,
        nz_ref,
        oz_ref,
        sq_ref,
        gradient_ref,
        model_ref,
        target,
        current,
        extra,
        dual_x,
        dual_y,
        dual_z,
        model,
        sems,
    ):
        gradient_copy = pltpu.make_async_copy(g_ref, gradient_ref, sems.at[0])
        gradient_copy.start()
        pos_x, pos_y, pos_z = position(dev_ref, sizes)
        even_x, even_y, even_z = (is_even(i) for i in (pos_x, pos_y, pos_z))

        total = jnp.sum(jnp.sum(sq_ref[...], axis=0), axis=1, keepdims=True)
        scale = step_length * lax.rsqrt(total / cells + 1.0)
        scale = jnp.broadcast_to(scale, (1, bz))

        side_lane = lane((tall, bz)) < bz // 2
        near_z = nz_ref[pl.ds(tall, tall)] - scale * nz_ref[pl.ds(0, tall)]
        other_z = oz_ref[pl.ds(tall, tall)] - scale * oz_ref[pl.ds(0, tall)]
        before_z = jnp.where(even_z, other_z, near_z)
        after_z = jnp.where(even_z, near_z, other_z)
        for p in range(planes):
            own, rows = (
                [
                    plane_of(main, nx_ref, ox_ref, even_x, field, p),
                    rows_of(ny_ref, oy_ref, even_y, field, p, pairs),
                ]
                for field, main in ((1, v_ref), (0, g_ref))
            )
            own, rows = (own[0] - scale * rows[0], own[1] - scale * rows[1])
            back = (bz - 4 * p) % bz
            after = pltpu.roll(after_z, back, 1) if back else after_z
            before = pltpu.roll(before_z, back, 1) if back else before_z
            target[p, pl.ds(0, by), pl.ds(0, bz)] = own
            target[p, pl.ds(by, 8), pl.ds(0, bz)] = rows
            target[p, :, pl.ds(bz, bz)] = jnp.where(side_lane, after, before)

        def factor(index, limit):
            return jnp.where((index >= 0) & (index < limit - 1), dual_step, 0.0).astype(F32)

        row = sublane((tall, 1))
        row = jnp.where(row < by + 4, row, row - tall) + pos_y * by
        factor_y = factor(row, size_y * by)
        col = lane((1, wide))
        col = jnp.where(col < bz + bz // 2, col, col - wide) + pos_z * bz
        factor_z = factor(col, size_z * bz)
        shrink = 1.0 / (1.0 + primal_step)
        gain = primal_step / (1.0 + primal_step)

        for iteration in range(ITERS):
            first = iteration == 0
            final = iteration == ITERS - 1
            here_ref = target if first else extra
            ahead = here_ref[iteration]
            before_x = None
            for p in range(iteration, planes - 1 - iteration):
                here = ahead
                ahead = here_ref[p + 1]
                index = pos_x * bx + (p - HALO)
                factor_x = factor(index, size_x * bx)
                dx = factor_x * (ahead - here)
                dy = factor_y * (pltpu.roll(here, tall - 1, 0) - here)
                dz = factor_z * (pltpu.roll(here, wide - 1, 1) - here)
                if not first:
                    dx = dual_x[p] + dx
                    dy = dual_y[p] + dy
                    dz = dual_z[p] + dz
                norm = dx * dx + dy * dy + dz * dz
                ratio = jnp.minimum(1.0, tv_weight * lax.rsqrt(norm))
                dx = dx * ratio
                dy = dy * ratio
                dz = dz * ratio
                if not final:
                    dual_x[p] = dx
                    dual_y[p] = dy
                    dual_z[p] = dz
                if p > iteration:
                    if final:
                        spread = dx[:by, :bz] - before_x
                        spread += dy[:by, :bz] - pltpu.roll(dy[:, :bz], 1, 0)[:by]
                        spread += dz[:by, :bz] - pltpu.roll(dz[:by], 1, 1)[:, :bz]
                        goal = target[p, pl.ds(0, by), pl.ds(0, bz)]
                        old = current[p, pl.ds(0, by), pl.ds(0, bz)]
                        model[p - HALO] = shrink * old + gain * (spread + goal)
                    else:
                        spread = dx - before_x
                        spread += dy - pltpu.roll(dy, 1, 0)
                        spread += dz - pltpu.roll(dz, 1, 1)
                        if first:
                            new = here + gain * spread
                            old = here
                        else:
                            old = current[p]
                            new = shrink * old + gain * (spread + target[p])
                        current[p] = new
                        extra[p] = 2.0 * new - old
                before_x = dx[:by, :bz] if final else dx
        model_copy = pltpu.make_async_copy(model, model_ref, sems.at[1])
        model_copy.start()
        gradient_copy.wait()
        model_copy.wait()

    field = pltpu.VMEM((planes, tall, wide), F32)
    return pl.pallas_call(
        kernel,
        name="proximal",
        compiler_params=PARAMS,
        out_shape=(struct(bx, by, bz),) * 2,
        in_specs=[SMEM] + [VMEM] * 9,
        out_specs=(HBM,) * 2,
        scratch_shapes=[field] * 6 + [pltpu.VMEM((bx, by, bz), F32), pltpu.SemaphoreType.DMA((2,))],
    )(device, gradient, velocity, *halos, squares)


def shards(partials, code_bits, group_map, velocity):
    sizes = tuple(lax.axis_size(axis) for axis in (GX, GY, "gz"))
    device = lax.axis_index(ALL).astype(jnp.int32).reshape(1)

    local = presum(device, partials, code_bits, group_map, sizes, 8)
    parts = lax.all_to_all(local, GX, split_axis=0, concat_axis=0, tiled=True)
    gradient, *send_x, squares = reduce_pack(device, parts, velocity, sizes)
    halo_x = swap(send_x, GX, GY[1])
    table = jnp.broadcast_to(
        squares[:1][None], (sizes[0] * sizes[1] * sizes[2], 1, squares.shape[1])
    )
    table = lax.all_to_all(table, ALL, split_axis=0, concat_axis=0, tiled=True)
    first, last, *send_corners = pack_lanes(device, gradient, velocity, halo_x, sizes)
    corners = swap(send_corners, GY, "gz")
    send_y = pack_y(device, gradient, velocity, halo_x, sizes)
    halo_y = swap(send_y, GY, "gz")

    send_z = pack_z(device, first, last, corners, sizes)
    halo_z = swap(send_z, "gz", GY[1])

    halos = (*halo_x, *halo_y, *halo_z)
    return proximal(device, gradient, velocity, halos, table, sizes)


def solution(mesh):
    torus = Mesh(
        mesh.devices.reshape(4, 2, 4, 2, mesh.shape["gz"]), ("gx_0", "gx_1", "gy_0", "gy_1", "gz")
    )
    placed = (P(GX, None, GY, "gz"), P(), P(), P(GX, GY, "gz"))
    return jax.shard_map(
        shards,
        mesh=torus,
        in_specs=placed,
        out_specs=(P(GX, GY, "gz"), P(GX, GY, "gz")),
        check_vma=False,
    )
```

```python
import jax
import jax.numpy as jnp
from jax import lax
from jax.experimental import pallas as pl
from jax.experimental.pallas import tpu as pltpu
from jax.sharding import Mesh
from jax.sharding import PartitionSpec as P

ITERS = 3
HALO = ITERS
GX = ("gx_0", "gx_1")
GY = ("gy_0", "gy_1")
ALL = GX + GY + ("gz",)

step_length = 0.5
tv_weight = 0.2
dual_step = 0.28
primal_step = 0.28

VMEM = pl.BlockSpec(memory_space=pltpu.VMEM)
SMEM = pl.BlockSpec(memory_space=pltpu.SMEM)
HBM = pl.BlockSpec(memory_space=pltpu.HBM)
PARAMS = pltpu.CompilerParams(vmem_limit_bytes=16 * 1024 * 1024)
F32 = jnp.float32


def swap(blocks, axis, spare):
    size, width = lax.axis_size(axis), lax.axis_size(spare)
    pairs = [(i, i ^ 1) for i in range(size)]
    axes = axis if isinstance(axis, tuple) else (axis,)
    ahead = ALL.index(spare) < ALL.index(axes[0])

    def at(i, k):
        return k * size + i if ahead else i * width + k

    others = []
    for i in range(size):
        j = ((i + 1) ^ 1) - 1
        for k in range(width):
            others.append((at(i, k), at(j, k) if 0 <= j < size else at(i, k ^ 1)))
    both = (spare, *axes) if ahead else (*axes, spare)
    return lax.ppermute(blocks[0], axis, pairs), lax.ppermute(blocks[1], both, others)


def struct(*shape):
    return jax.ShapeDtypeStruct(shape, F32)


def in_hbm(array):
    return pltpu.with_memory_space_constraint(array, pltpu.HBM)


def presum(device, partials, code_bits, group_map, sizes, chunks):
    slots, nx, by, bz = partials.shape
    rows = nx // chunks

    def kernel(dev_ref, map_hbm, bits_hbm, part_ref, out_ref, buf, map_ref, bits_ref, sems):
        map_copy = pltpu.make_async_copy(map_hbm, map_ref, sems.at[chunks])
        bits_copy = pltpu.make_async_copy(bits_hbm, bits_ref, sems.at[chunks + 1])
        map_copy.start()
        bits_copy.start()

        def copy(c):
            part = pl.ds(c * rows, rows)
            return pltpu.make_async_copy(part_ref.at[:, part], buf.at[:, part], sems.at[c])

        for c in range(chunks):
            copy(c).start()
        map_copy.wait()
        bits_copy.wait()
        base = position(dev_ref, sizes)[0] * slots
        groups = [map_ref[base + s] for s in range(slots)]
        for c in range(chunks):
            copy(c).wait()

            def row(i, carry):
                x = c * rows + i
                total = None
                for s in range(slots):
                    sign = (2 * bits_ref[groups[s], x] - 1).astype(F32)
                    term = sign * buf[s, x]
                    total = term if total is None else total + term
                out_ref[x] = total
                return carry

            lax.fori_loop(0, rows, row, 0, unroll=8)

    return pl.pallas_call(
        kernel,
        name="presum",
        compiler_params=PARAMS,
        out_shape=struct(nx, by, bz),
        in_specs=[SMEM, HBM, HBM, HBM],
        out_specs=VMEM,
        scratch_shapes=[
            pltpu.VMEM(partials.shape, F32),
            pltpu.SMEM(group_map.shape, jnp.int32),
            pltpu.SMEM(code_bits.shape, jnp.int32),
            pltpu.SemaphoreType.DMA((chunks + 2,)),
        ],
    )(device, in_hbm(group_map), in_hbm(code_bits), in_hbm(partials))


def position(dev_ref, sizes):
    _, size_y, size_z = sizes
    dev = dev_ref[0]
    return dev // (size_y * size_z), (dev // size_z) % size_y, dev % size_z


def is_even(index):
    return index % 2 == 0


def reduce_pack(device, parts, velocity, sizes):
    bx, by, bz = velocity.shape
    members = sizes[0]

    def kernel(dev_ref, part_ref, v_ref, g_ref, near_ref, other_ref, square_ref):
        even = is_even(position(dev_ref, sizes)[0])
        squares = jnp.zeros((by, bz), F32)
        for i in range(bx):
            total = part_ref[i]
            for m in range(1, members):
                total = total + part_ref[m * bx + i]
            g_ref[i] = total
            squares = squares + total * total
        for i in range(HALO):
            for k, ref in enumerate((g_ref, v_ref)):
                first, last = ref[i], ref[bx - HALO + i]
                near_ref[k * HALO + i] = jnp.where(even, last, first)
                other_ref[k * HALO + i] = jnp.where(even, first, last)
        square_ref[...] = jnp.broadcast_to(jnp.sum(squares, axis=0, keepdims=True), (8, bz))

    edge = struct(2 * HALO, by, bz)
    return pl.pallas_call(
        kernel,
        name="reduce_pack",
        compiler_params=PARAMS,
        out_shape=(struct(bx, by, bz), edge, edge, struct(8, bz)),
        in_specs=[SMEM, VMEM, VMEM],
        out_specs=(VMEM,) * 4,
    )(device, parts, velocity)


def plane_of(main_ref, near_ref, other_ref, even, field, p):
    bx = main_ref.shape[0]
    if p < HALO:
        at = field * HALO + p
        return jnp.where(even, other_ref[at], near_ref[at])
    if p < HALO + bx:
        return main_ref[p - HALO]
    at = field * HALO + p - HALO - bx
    return jnp.where(even, near_ref[at], other_ref[at])


def sublane(shape):
    return lax.broadcasted_iota(jnp.int32, shape, len(shape) - 2)


def lane(shape):
    return lax.broadcasted_iota(jnp.int32, shape, len(shape) - 1)


def pack_y(device, gradient, velocity, halo_x, sizes):
    bx, by, bz = velocity.shape
    pairs = (bx + 2 * HALO) // 2

    def kernel(dev_ref, g_ref, v_ref, nx_ref, ox_ref, near_ref, other_ref):
        even_x, even_y = (is_even(i) for i in position(dev_ref, sizes)[:2])
        low = sublane((8, bz)) < 4
        for field, main in enumerate((g_ref, v_ref)):
            for q in range(pairs):
                left = plane_of(main, nx_ref, ox_ref, even_x, field, 2 * q)
                right = plane_of(main, nx_ref, ox_ref, even_x, field, 2 * q + 1)
                first = jnp.where(low, left[:8], pltpu.roll(right[:8], 4, 0))
                last = jnp.where(low, pltpu.roll(left[by - 8 :], 4, 0), right[by - 8 :])
                near_ref[field * pairs + q] = jnp.where(even_y, last, first)
                other_ref[field * pairs + q] = jnp.where(even_y, first, last)

    edge = struct(2 * pairs, 8, bz)
    return pl.pallas_call(
        kernel,
        name="pack_y",
        compiler_params=PARAMS,
        out_shape=(edge, edge),
        in_specs=[SMEM] + [VMEM] * 4,
        out_specs=(VMEM,) * 2,
    )(device, gradient, velocity, *halo_x)


def rows_of(near_ref, other_ref, even, field, p, pairs):
    near = near_ref[field * pairs + p // 2]
    other = other_ref[field * pairs + p // 2]
    low = sublane(near.shape) < 4
    after = jnp.where(even, near, other)
    before = jnp.where(even, other, near)
    if p % 2 == 0:
        return jnp.where(low, after, pltpu.roll(before, 4, 0))
    return jnp.where(low, pltpu.roll(after, 4, 0), before)


def pack_lanes(device, gradient, velocity, halo_x, sizes):
    bx, by, bz = velocity.shape
    planes = bx + 2 * HALO
    groups = bz // 4

    def kernel(dev_ref, g_ref, v_ref, nx_ref, ox_ref, first_ref, last_ref, near_ref, other_ref):
        even_x, even_y = (is_even(i) for i in position(dev_ref, sizes)[:2])
        group = lane((by, bz)) // 4
        for field, main in enumerate((g_ref, v_ref)):
            first = jnp.zeros((by, bz), F32)
            last = jnp.zeros((by, bz), F32)
            for p in range(planes):
                plane = plane_of(main, nx_ref, ox_ref, even_x, field, p)
                turned = pltpu.roll(plane, 4 * p, 1) if p else plane
                first = jnp.where(group == p, turned, first)
                last = jnp.where(group == (p - 1) % groups, turned, last)
            first_ref[pl.ds(field * by, by)] = first
            last_ref[pl.ds(field * by, by)] = last
            for k, packed in enumerate((first, last)):
                top, bottom = packed[:8], packed[by - 8 :]
                near_ref[2 * field + k] = jnp.where(even_y, bottom, top)
                other_ref[2 * field + k] = jnp.where(even_y, top, bottom)

    own = struct(2 * by, bz)
    edge = struct(4, 8, bz)
    return pl.pallas_call(
        kernel,
        name="pack_lanes",
        compiler_params=PARAMS,
        out_shape=(own, own, edge, edge),
        in_specs=[SMEM] + [VMEM] * 4,
        out_specs=(VMEM,) * 4,
    )(device, gradient, velocity, *halo_x)


def pack_z(device, first, last, corners, sizes):
    rows, bz = first.shape
    by = rows // 2
    tall = by + 8

    def kernel(dev_ref, first_ref, last_ref, nc_ref, oc_ref, near_ref, other_ref):
        even_y, even_z = (is_even(i) for i in position(dev_ref, sizes)[1:])
        low = sublane((8, bz)) < 4
        for field in range(2):
            both = []
            for k, ref in enumerate((first_ref, last_ref)):
                near, other = nc_ref[2 * field + k], oc_ref[2 * field + k]
                after = jnp.where(even_y, near, other)
                before = jnp.where(even_y, other, near)
                extra = jnp.where(low, after, before)
                both.append(jnp.concatenate([ref[pl.ds(field * by, by)], extra], 0))
            near_ref[pl.ds(field * tall, tall)] = jnp.where(even_z, both[1], both[0])
            other_ref[pl.ds(field * tall, tall)] = jnp.where(even_z, both[0], both[1])

    edge = struct(2 * tall, bz)
    return pl.pallas_call(
        kernel,
        name="pack_z",
        compiler_params=PARAMS,
        out_shape=(edge, edge),
        in_specs=[SMEM] + [VMEM] * 4,
        out_specs=(VMEM,) * 2,
    )(device, first, last, *corners)


def proximal(device, gradient, velocity, halos, squares, sizes):
    bx, by, bz = velocity.shape
    planes = bx + 2 * HALO
    pairs = planes // 2
    tall = by + 8
    wide = 2 * bz
    size_x, size_y, size_z = sizes
    cells = size_x * bx * size_y * by * size_z * bz

    def kernel(
        dev_ref,
        g_ref,
        v_ref,
        nx_ref,
        ox_ref,
        ny_ref,
        oy_ref,
        nz_ref,
        oz_ref,
        sq_ref,
        gradient_ref,
        model_ref,
        target,
        current,
        extra,
        dual_x,
        dual_y,
        dual_z,
        model,
        sems,
    ):
        gradient_copy = pltpu.make_async_copy(g_ref, gradient_ref, sems.at[0])
        gradient_copy.start()
        pos_x, pos_y, pos_z = position(dev_ref, sizes)
        even_x, even_y, even_z = (is_even(i) for i in (pos_x, pos_y, pos_z))

        total = jnp.sum(jnp.sum(sq_ref[...], axis=0), axis=1, keepdims=True)
        scale = step_length * lax.rsqrt(total / cells + 1.0)
        scale = jnp.broadcast_to(scale, (1, bz))

        side_lane = lane((tall, bz)) < bz // 2
        near_z = nz_ref[pl.ds(tall, tall)] - scale * nz_ref[pl.ds(0, tall)]
        other_z = oz_ref[pl.ds(tall, tall)] - scale * oz_ref[pl.ds(0, tall)]
        before_z = jnp.where(even_z, other_z, near_z)
        after_z = jnp.where(even_z, near_z, other_z)
        for p in range(planes):
            own, rows = (
                [
                    plane_of(main, nx_ref, ox_ref, even_x, field, p),
                    rows_of(ny_ref, oy_ref, even_y, field, p, pairs),
                ]
                for field, main in ((1, v_ref), (0, g_ref))
            )
            own, rows = (own[0] - scale * rows[0], own[1] - scale * rows[1])
            back = (bz - 4 * p) % bz
            after = pltpu.roll(after_z, back, 1) if back else after_z
            before = pltpu.roll(before_z, back, 1) if back else before_z
            target[p, pl.ds(0, by), pl.ds(0, bz)] = own
            target[p, pl.ds(by, 8), pl.ds(0, bz)] = rows
            target[p, :, pl.ds(bz, bz)] = jnp.where(side_lane, after, before)

        def factor(index, limit):
            return jnp.where((index >= 0) & (index < limit - 1), dual_step, 0.0).astype(F32)

        row = sublane((tall, 1))
        row = jnp.where(row < by + 4, row, row - tall) + pos_y * by
        factor_y = factor(row, size_y * by)
        col = lane((1, wide))
        col = jnp.where(col < bz + bz // 2, col, col - wide) + pos_z * bz
        factor_z = factor(col, size_z * bz)
        shrink = 1.0 / (1.0 + primal_step)
        gain = primal_step / (1.0 + primal_step)

        for iteration in range(ITERS):
            first = iteration == 0
            final = iteration == ITERS - 1
            here_ref = target if first else extra
            ahead = here_ref[iteration]
            before_x = None
            for p in range(iteration, planes - 1 - iteration):
                here = ahead
                ahead = here_ref[p + 1]
                index = pos_x * bx + (p - HALO)
                factor_x = factor(index, size_x * bx)
                dx = factor_x * (ahead - here)
                dy = factor_y * (pltpu.roll(here, tall - 1, 0) - here)
                dz = factor_z * (pltpu.roll(here, wide - 1, 1) - here)
                if not first:
                    dx = dual_x[p] + dx
                    dy = dual_y[p] + dy
                    dz = dual_z[p] + dz
                norm = dx * dx + dy * dy + dz * dz
                ratio = jnp.minimum(1.0, tv_weight * lax.rsqrt(norm))
                dx = dx * ratio
                dy = dy * ratio
                dz = dz * ratio
                if not final:
                    dual_x[p] = dx
                    dual_y[p] = dy
                    dual_z[p] = dz
                if p > iteration:
                    if final:
                        spread = dx[:by, :bz] - before_x
                        spread += dy[:by, :bz] - pltpu.roll(dy[:, :bz], 1, 0)[:by]
                        spread += dz[:by, :bz] - pltpu.roll(dz[:by], 1, 1)[:, :bz]
                        goal = target[p, pl.ds(0, by), pl.ds(0, bz)]
                        old = current[p, pl.ds(0, by), pl.ds(0, bz)]
                        model[p - HALO] = shrink * old + gain * (spread + goal)
                    else:
                        spread = dx - before_x
                        spread += dy - pltpu.roll(dy, 1, 0)
                        spread += dz - pltpu.roll(dz, 1, 1)
                        if first:
                            new = here + gain * spread
                            old = here
                        else:
                            old = current[p]
                            new = shrink * old + gain * (spread + target[p])
                        current[p] = new
                        extra[p] = 2.0 * new - old
                before_x = dx[:by, :bz] if final else dx
        model_copy = pltpu.make_async_copy(model, model_ref, sems.at[1])
        model_copy.start()
        gradient_copy.wait()
        model_copy.wait()

    field = pltpu.VMEM((planes, tall, wide), F32)
    return pl.pallas_call(
        kernel,
        name="proximal",
        compiler_params=PARAMS,
        out_shape=(struct(bx, by, bz),) * 2,
        in_specs=[SMEM] + [VMEM] * 9,
        out_specs=(HBM,) * 2,
        scratch_shapes=[field] * 6 + [pltpu.VMEM((bx, by, bz), F32), pltpu.SemaphoreType.DMA((2,))],
    )(device, gradient, velocity, *halos, squares)


def shards(partials, code_bits, group_map, velocity):
    sizes = tuple(lax.axis_size(axis) for axis in (GX, GY, "gz"))
    device = lax.axis_index(ALL).astype(jnp.int32).reshape(1)

    local = presum(device, partials, code_bits, group_map, sizes, 8)
    parts = lax.all_to_all(local, GX, split_axis=0, concat_axis=0, tiled=True)
    gradient, *send_x, squares = reduce_pack(device, parts, velocity, sizes)
    halo_x = swap(send_x, GX, GY[1])
    table = jnp.broadcast_to(
        squares[:1][None], (sizes[0] * sizes[1] * sizes[2], 1, squares.shape[1])
    )
    table = lax.all_to_all(table, ALL, split_axis=0, concat_axis=0, tiled=True)
    first, last, *send_corners = pack_lanes(device, gradient, velocity, halo_x, sizes)
    corners = swap(send_corners, GY, "gz")
    send_y = pack_y(device, gradient, velocity, halo_x, sizes)
    halo_y = swap(send_y, GY, "gz")

    send_z = pack_z(device, first, last, corners, sizes)
    halo_z = swap(send_z, "gz", GY[1])

    halos = (*halo_x, *halo_y, *halo_z)
    return proximal(device, gradient, velocity, halos, table, sizes)


def solution(mesh):
    torus = Mesh(
        mesh.devices.reshape(4, 2, 4, 2, mesh.shape["gz"]), ("gx_0", "gx_1", "gy_0", "gy_1", "gz")
    )
    placed = (P(GX, None, GY, "gz"), P(), P(), P(GX, GY, "gz"))
    return jax.shard_map(
        shards,
        mesh=torus,
        in_specs=placed,
        out_specs=(P(GX, GY, "gz"), P(GX, GY, "gz")),
        check_vma=False,
    )
```
